32 devices in a mesh: fsdp: 4 (over x, core), context: 2 (over y), tensor: 4 (over z).
Axes of the slice: x: 2, y: 2, z: 4, core: 2. Of those that a mesh axis runs over, the one named last changes fastest.
Arguments:
- tokens: bfloat16 [8, 1024, 2560], P('fsdp', 'context'), may hold values from -6 to 6
- norm_one: bfloat16 [2560], P(('fsdp', 'context')), may hold values from 0.099609375 to 1.8984375
- q_weight: bfloat16 [2560, 2560], P(('fsdp', 'context'), 'tensor'), may hold values from -0.125 to 0.125
- k_weight: bfloat16 [2560, 640], P(('fsdp', 'context'), 'tensor'), may hold values from -0.125 to 0.125
- v_weight: bfloat16 [2560, 640], P(('fsdp', 'context'), 'tensor'), may hold values from -0.125 to 0.125
- o_weight: bfloat16 [2560, 2560], P('tensor', ('fsdp', 'context')), may hold values from -0.5 to 0.5
- norm_two: bfloat16 [2560], P(('fsdp', 'context')), may hold values from 0.099609375 to 1.8984375
- gate_weight: bfloat16 [2560, 6912], P(('fsdp', 'context'), 'tensor'), may hold values from -0.125 to 0.125
- up_weight: bfloat16 [2560, 6912], P(('fsdp', 'context'), 'tensor'), may hold values from -0.125 to 0.125
- down_weight: bfloat16 [6912, 2560], P('tensor', ('fsdp', 'context')), may hold values from -0.15625 to 0.15625
- segment_ids: int32 [8, 1024], P('fsdp'), may hold values from 0 to 12, as said below
- parent_ids: int32 [8, 1024], P('fsdp'), may hold values from 0 to 4, as said below
- path_pos: int32 [8, 1024], P('fsdp'), may hold values from 0 to 607, as said below
- cotangent: bfloat16 [8, 1024, 2560], P('fsdp', 'context'), may hold values from -6 to 6
Outputs:
- layer_out: bfloat16 [8, 1024, 2560], P('fsdp', ('context', 'tensor'))
- tokens_grad: bfloat16 [8, 1024, 2560], P('fsdp', ('context', 'tensor'))
- norm_one_grad: float32 [2560], P(('fsdp', 'context'))
- q_grad: float32 [2560, 2560], P(('fsdp', 'context'), 'tensor')
- k_grad: float32 [2560, 640], P(('fsdp', 'context'), 'tensor')
- v_grad: float32 [2560, 640], P(('fsdp', 'context'), 'tensor')
- o_grad: float32 [2560, 2560], P('tensor', ('fsdp', 'context'))
- norm_two_grad: float32 [2560], P(('fsdp', 'context'))
- gate_grad: float32 [2560, 6912], P(('fsdp', 'context'), 'tensor')
- up_grad: float32 [2560, 6912], P(('fsdp', 'context'), 'tensor')
- down_grad: float32 [6912, 2560], P('tensor', ('fsdp', 'context'))
The draws below stay inside these ranges and needn't reach their ends.
Inputs may be any that keep to these rules, and one draw needn't show every extreme that they name: `segment_ids`: in each tree, tokens 0 to 511 are segment 0, the trunk; the other tokens form 4 branches (segments 1 to 4, 64 tokens each) and 2 leaves per branch (32 tokens each, segments above 4); each segment is contiguous and each leaf comes after its branch. `parent_ids`: 0 for tokens of the trunk and of branches; for a leaf's tokens, the leaf's branch. `path_pos`: the trunk counts 0 upward; a branch continues from 512, a leaf from 576, each token one more than the one before it in its segment.
All inputs are finite; a program needn't handle non-finite values.
Results may differ from the reference program's by a relative error of at most 0.02.
Values may be sent and summed in bfloat16 or wider, within the bound.
A program may use at most 320 MiB of HBM per device.

```python
import jax
import jax.numpy as jnp
from jax import lax

D = 2560
HEADS = 32
KV_HEADS = 8
HEAD = 80
FF = 6912
TRUNK = 512
BRANCH = 64
LEAF = 32
BRANCHES = 4
LEAVES = 2
TREE_LEN = 1024
TREES_ALL = 8


def tree_layout(key):
    layout_key = jax.random.fold_in(key, 11)
    seg_count = BRANCHES * (1 + LEAVES)
    order_index = jnp.arange(seg_count)
    owner_branch = jnp.where(order_index < BRANCHES, order_index, (order_index - BRANCHES) // LEAVES)
    is_leaf = order_index >= BRANCHES
    raw_scores = jax.random.randint(layout_key, (TREES_ALL, seg_count), 0, 64)
    parent_scores = jnp.take(raw_scores, owner_branch, axis=1)
    leaf_scores = jnp.maximum(raw_scores, parent_scores) + 1
    scores = jnp.where(is_leaf[None, :], leaf_scores, raw_scores) * 64 + order_index[None, :]
    seg_order = jnp.argsort(scores, axis=1, stable=True).astype(jnp.int32)
    seg_lengths = jnp.where(seg_order >= BRANCHES, LEAF, BRANCH)
    seg_starts = TRUNK + jnp.cumsum(seg_lengths, axis=1) - seg_lengths
    token_index = jnp.arange(TREE_LEN)
    slot_hits = (token_index[None, :, None] >= seg_starts[:, None, :]).astype(jnp.int32)
    slot_index = jnp.sum(slot_hits, axis=2) - 1
    one_hot = (slot_index[:, :, None] == order_index[None, None, :]).astype(jnp.int32)
    seg_here = jnp.sum(one_hot * seg_order[:, None, :], axis=2)
    start_here = jnp.sum(one_hot * seg_starts[:, None, :], axis=2)
    in_trunk = slot_index < 0
    leaf_here = seg_here >= BRANCHES
    segment = jnp.where(in_trunk, 0, seg_here + 1)
    parent = jnp.where(in_trunk | jnp.logical_not(leaf_here), 0, 1 + (seg_here - BRANCHES) // LEAVES)
    position = jnp.where(in_trunk, token_index[None, :], TRUNK + jnp.where(leaf_here, BRANCH, 0) + token_index[None, :] - start_here)
    return (segment.astype(jnp.int32), parent.astype(jnp.int32), position.astype(jnp.int32))


def draw_segment_ids(key, part):
    return tree_layout(key)[0]


def draw_parent_ids(key, part):
    return tree_layout(key)[1]


def draw_path_pos(key, part):
    return tree_layout(key)[2]


def shard_levels(key, extent, shards, smallest, largest):
    def one(dim, shards_of):
        heights = jax.random.uniform(jax.random.fold_in(jax.random.fold_in(key, 6), dim), (shards_of,), jnp.float32, smallest / len(shards), largest / len(shards))
        return jnp.repeat(jnp.exp(heights), extent[dim] // shards_of).reshape((-1,) + (1,) * (len(extent) - dim - 1))

    factor_of = one(*shards[0])
    for cut in shards[1:]:
        factor_of = factor_of * one(*cut)
    return factor_of


def noise(own_key, dims, width, bound, split=(), kind=jnp.bfloat16):
    array = width * jax.random.normal(own_key, dims, jnp.float32)
    if split:
        array = array * shard_levels(own_key, dims, split, -0.22, 0.18)
    return jnp.clip(array, -bound, bound).astype(kind)


def setup_inputs(seed: int = 0) -> dict:
    streams_of = jax.random.split(jax.random.key(seed), 15)
    return {
        "tokens": noise(streams_of[0], (TREES_ALL, TREE_LEN, D), 1.0, 6.0, ((0, 4), (1, 2))),
        "norm_one": jnp.clip(1.0 + 0.18 * jax.random.normal(streams_of[1], (D,), jnp.float32), 0.099609375, 1.8984375).astype(jnp.bfloat16),
        "q_weight": noise(streams_of[2], (D, HEADS * HEAD), D ** -0.5, 0.125, ((0, 8), (1, 4))),
        "k_weight": noise(streams_of[3], (D, KV_HEADS * HEAD), D ** -0.5, 0.125, ((0, 8), (1, 4))),
        "v_weight": noise(streams_of[4], (D, KV_HEADS * HEAD), D ** -0.5, 0.125, ((0, 8), (1, 4))),
        "o_weight": noise(streams_of[5], (HEADS * HEAD, D), (HEADS * HEAD // 16) ** -0.5, 0.5, ((0, 4), (1, 8))),
        "norm_two": jnp.clip(1.0 + 0.18 * jax.random.normal(streams_of[6], (D,), jnp.float32), 0.099609375, 1.8984375).astype(jnp.bfloat16),
        "gate_weight": noise(streams_of[7], (D, FF), D ** -0.5, 0.125, ((0, 8), (1, 4))),
        "up_weight": noise(streams_of[8], (D, FF), D ** -0.5, 0.125, ((0, 8), (1, 4))),
        "down_weight": noise(streams_of[9], (FF, D), (FF // 4) ** -0.5, 0.15625, ((0, 4), (1, 8))),
        "segment_ids": draw_segment_ids(jax.random.fold_in(streams_of[14], 71), 0),
        "parent_ids": draw_parent_ids(jax.random.fold_in(streams_of[14], 71), 0),
        "path_pos": draw_path_pos(jax.random.fold_in(streams_of[14], 71), 0),
        "cotangent": noise(streams_of[13], (TREES_ALL, TREE_LEN, D), 1.0, 6.0, ((0, 4), (1, 2))),
    }


@jax.custom_vjp
def low(v):
    return lax.optimization_barrier(v.astype(jnp.bfloat16)).astype(jnp.float32)

@jax.custom_vjp
def low_back(v):
    return v

def low_keep(v):
    return (low(v), None)

def low_pass(kept, grad):
    return (grad,)

def back_keep(v):
    return (v, None)

def back_low(kept, grad):
    return (low(grad),)
low.defvjp(low_keep, low_pass)
low_back.defvjp(back_keep, back_low)
EPS = 1e-05
THETA = 10000.0
NEG = -1000000000.0

def matmul(left, right):
    return jnp.dot(left, right, precision=lax.Precision.HIGHEST, preferred_element_type=jnp.float32)

def scaled_norm(values, gain):
    return values * lax.rsqrt(lax.optimization_barrier(jnp.mean(values * values, axis=-1, keepdims=True)) + EPS) * gain

def angle_tables(positions):
    half_width = HEAD // 2
    frequency = THETA ** (-(jnp.arange(half_width, dtype=jnp.float32) * 2.0 / HEAD))
    angles = positions.astype(jnp.float32)[:, None] * frequency[None, :]
    return (jnp.cos(angles), jnp.sin(angles))

def rotate(values, cosine, sine_part):
    half_width = values.shape[-1] // 2
    low_half = values[..., :half_width]
    high_half = values[..., half_width:]
    cos_rows = cosine[:, None, :]
    sin_rows = sine_part[:, None, :]
    return jnp.concatenate([low_half * cos_rows - high_half * sin_rows, high_half * cos_rows + low_half * sin_rows], axis=-1)

def tree_layer(params, tree_inputs):
    norm_gain_one, wq_all, wk_all, wv_all, wo_all, norm_gain_two, wg_all, wu_all, wd_all = params
    hidden_in, seg_tree, parent_tree, pos_tree = tree_inputs
    length = hidden_in.shape[0]
    normed = low(scaled_norm(hidden_in, norm_gain_one))
    queries = low_back(matmul(normed, wq_all)).reshape(length, HEADS, HEAD)
    key_rows = low_back(matmul(normed, wk_all)).reshape(length, KV_HEADS, HEAD)
    value_rows = low(low_back(matmul(normed, wv_all))).reshape(length, KV_HEADS, HEAD)
    cosine, sine_part = angle_tables(pos_tree)
    queries = low(low_back(rotate(queries, cosine, sine_part)))
    key_rows = low(low_back(rotate(key_rows, cosine, sine_part)))
    group_size = HEADS // KV_HEADS
    key_rows = jnp.repeat(key_rows, group_size, axis=1)
    value_rows = jnp.repeat(value_rows, group_size, axis=1)
    same_path = (seg_tree[None, :] == seg_tree[:, None]) | (seg_tree[None, :] == parent_tree[:, None]) | (seg_tree[None, :] == 0)
    allowed = same_path & (pos_tree[None, :] <= pos_tree[:, None])
    scores = jnp.einsum('qhd,khd->hqk', queries, key_rows, precision=lax.Precision.HIGHEST) * HEAD ** (-0.5)
    scores = low_back(jnp.where(allowed[None], scores, NEG))
    probs_low = low(jax.nn.softmax(scores, axis=-1))
    attended = jnp.einsum('hqk,khd->qhd', probs_low, value_rows, precision=lax.Precision.HIGHEST)
    attended = low(low_back(attended)).reshape(length, HEADS * HEAD)
    branch = low_back(matmul(attended, wo_all))
    middle = hidden_in + branch
    normed_two = low(scaled_norm(middle, norm_gain_two))
    gate_rows = low_back(matmul(normed_two, wg_all))
    upward = low_back(matmul(normed_two, wu_all))
    mixed_rows = low(jax.nn.silu(gate_rows) * upward)
    return middle + low_back(matmul(mixed_rows, wd_all))

def reference(tokens, norm_one, q_weight, k_weight, v_weight, o_weight, norm_two, gate_weight, up_weight, down_weight, segment_ids, parent_ids, path_pos, cotangent):
    params = (norm_one.astype(jnp.float32), q_weight.astype(jnp.float32), k_weight.astype(jnp.float32), v_weight.astype(jnp.float32), o_weight.astype(jnp.float32), norm_two.astype(jnp.float32), gate_weight.astype(jnp.float32), up_weight.astype(jnp.float32), down_weight.astype(jnp.float32))
    hidden = tokens.astype(jnp.float32)

    def forward(params_in, hidden_in):

        def one_tree(tree_inputs):
            return tree_layer(params_in, tree_inputs)
        return lax.map(jax.checkpoint(one_tree), (hidden_in, segment_ids, parent_ids, path_pos))
    layer_out, pullback = jax.vjp(forward, params, hidden)
    weight_grads, hidden_grad = pullback(cotangent.astype(jnp.float32))
    return (layer_out.astype(jnp.bfloat16), hidden_grad.astype(jnp.bfloat16), weight_grads[0], weight_grads[1], weight_grads[2], weight_grads[3], weight_grads[4], weight_grads[5], weight_grads[6], weight_grads[7], weight_grads[8])
```

```python
import functools

import jax
import jax.numpy as jnp
import numpy as np
from jax import lax
from jax.experimental import pallas as pl
from jax.experimental.pallas import tpu as pltpu
from jax.sharding import PartitionSpec as P

HEADS = 32
KV_HEADS = 8
HEAD = 80
HALF = HEAD // 2
LANES = 128
MICRO = 2
EPS = 1e-05
THETA = 10000.0
NEG = -1000000000.0
TRUNK = 512
WEIGHT_AXES = ("fsdp", "context")
BF16 = jnp.bfloat16
F32 = jnp.float32


def round_up(value, unit):
    return (value + unit - 1) // unit * unit


def mm(left, right):
    return lax.dot_general(left, right, (((1,), (0,)), ((), ())), preferred_element_type=F32)


def mm_nt(left, right):
    return lax.dot_general(left, right, (((1,), (1,)), ((), ())), preferred_element_type=F32)


def mm_tn(left, right):
    return lax.dot_general(left, right, (((0,), (0,)), ((), ())), preferred_element_type=F32)


def rotated(values, cos_table, sin_table):
    lane = lax.broadcasted_iota(jnp.int32, values.shape, 1)
    swapped = jnp.where(
        lane < HALF, pltpu.roll(values, LANES - HALF, 1), pltpu.roll(values, HALF, 1)
    )
    return values * cos_table + swapped * sin_table


def window_of(head):
    start = head * HEAD
    base = start // LANES * LANES
    return base, start - base


def split_kernel(q_heads, kv_heads, x_ref, cos_ref, sin_ref, q_ref, kv_ref):
    cos_table = cos_ref[...]
    sin_table = sin_ref[...]
    for head in range(q_heads + 2 * kv_heads):
        base, shift = window_of(head)
        window = x_ref[:, base : base + 2 * LANES]
        if shift:
            window = pltpu.roll(window, 2 * LANES - shift, 1)
        values = window[:, :LANES]
        if head < q_heads + kv_heads:
            result = rotated(values, cos_table, sin_table)
        else:
            lane = lax.broadcasted_iota(jnp.int32, values.shape, 1)
            result = jnp.where(lane < HEAD, values, 0.0)
        result = result.astype(BF16)
        if head < q_heads:
            q_ref[:, head * LANES : (head + 1) * LANES] = result
        else:
            at = (head - q_heads) * LANES
            kv_ref[:, at : at + LANES] = result


def split_heads(packed, cos_table, sin_table, q_heads, kv_heads, rows):
    total, width = packed.shape
    q_wide = q_heads * LANES
    kv_wide = 2 * kv_heads * LANES
    return pl.pallas_call(
        functools.partial(split_kernel, q_heads, kv_heads),
        grid=(total // rows,),
        in_specs=[
            pl.BlockSpec((rows, width), lambda b: (b, 0)),
            pl.BlockSpec((rows, LANES), lambda b: (b, 0)),
            pl.BlockSpec((rows, LANES), lambda b: (b, 0)),
        ],
        out_specs=[
            pl.BlockSpec((rows, q_wide), lambda b: (b, 0)),
            pl.BlockSpec((rows, kv_wide), lambda b: (b, 0)),
        ],
        out_shape=[
            jax.ShapeDtypeStruct((total, q_wide), BF16),
            jax.ShapeDtypeStruct((total, kv_wide), BF16),
        ],
        cost_estimate=pl.CostEstimate(
            flops=10 * total * width, bytes_accessed=7 * total * width, transcendentals=0
        ),
        name="split_heads",
    )(packed, cos_table, sin_table)


def pack_kernel(q_heads, kv_heads, dq_ref, dkv_ref, cos_ref, sin_ref, out_ref, sum_ref):
    cos_table = cos_ref[...]
    sin_table = -sin_ref[...]
    sum_ref[...] = jnp.zeros_like(sum_ref)
    for head in range(q_heads + 2 * kv_heads):
        base, shift = window_of(head)
        if head < q_heads:
            values = dq_ref[:, head * LANES : (head + 1) * LANES].astype(F32)
        else:
            at = (head - q_heads) * LANES
            values = dkv_ref[:, at : at + LANES].astype(BF16).astype(F32)
        if head < q_heads + kv_heads:
            values = rotated(values, cos_table, sin_table)
        wide = jnp.concatenate([values, jnp.zeros_like(values)], axis=1)
        if shift:
            wide = pltpu.roll(wide, shift, 1)
        sum_ref[:, base : base + 2 * LANES] += wide
    out_ref[...] = sum_ref[...].astype(BF16)


def pack_heads(dq_wide, dkv, cos_table, sin_table, q_heads, kv_heads, width, rows):
    total = dq_wide.shape[0]
    return pl.pallas_call(
        functools.partial(pack_kernel, q_heads, kv_heads),
        grid=(total // rows,),
        in_specs=[
            pl.BlockSpec((rows, dq_wide.shape[1]), lambda b: (b, 0)),
            pl.BlockSpec((rows, dkv.shape[1]), lambda b: (b, 0)),
            pl.BlockSpec((rows, LANES), lambda b: (b, 0)),
            pl.BlockSpec((rows, LANES), lambda b: (b, 0)),
        ],
        out_specs=pl.BlockSpec((rows, width), lambda b: (b, 0)),
        out_shape=jax.ShapeDtypeStruct((total, width), BF16),
        scratch_shapes=[pltpu.VMEM((rows, width), F32)],
        cost_estimate=pl.CostEstimate(
            flops=10 * total * width, bytes_accessed=7 * total * width, transcendentals=0
        ),
        name="pack_heads",
    )(dq_wide, dkv, cos_table, sin_table)


def fill_bias(seg_q, par_q, pos_q, seg_k, pos_k, bias_ref):
    same = (seg_k == seg_q) | (seg_k == par_q) | (seg_k == 0)
    bias_ref[...] = jnp.where(same & (pos_k <= pos_q), 0.0, NEG)


def probabilities(q_block, keys, bias):
    scores = mm_nt(q_block, keys) * HEAD ** (-0.5) + bias
    top = jnp.max(scores, axis=1, keepdims=True)
    raised = jnp.exp(scores - top)
    return raised * (1.0 / jnp.sum(raised, axis=1, keepdims=True))


def forward_kernel(
    rows, tree_len, block,
    ctx_ref, q_ref, k_ref, v_ref, seg_q, par_q, pos_q, seg_k, pos_k, out_ref, bias_ref,
):
    @pl.when(pl.program_id(1) == 0)
    def _():
        fill_bias(seg_q[0], par_q[0], pos_q[0], seg_k[0], pos_k[0], bias_ref)

    in_trunk = (ctx_ref[0] + 1) * rows <= TRUNK

    def run(keys):
        @pl.loop(0, rows // block)
        def _(step):
            at = pl.ds(pl.multiple_of(step * block, block), block)
            probs = probabilities(q_ref[at, :], k_ref[0, :keys, :], bias_ref[at, :keys])
            out_ref[at, :] = mm(probs.astype(BF16), v_ref[0, :keys, :]).astype(BF16)

    pl.when(in_trunk)(lambda: run(min(TRUNK, tree_len)))
    pl.when(jnp.logical_not(in_trunk))(lambda: run(tree_len))


def backward_kernel(
    rows, tree_len, block, group,
    ctx_ref, q_ref, k_ref, v_ref, do_ref, seg_q, par_q, pos_q, seg_k, pos_k,
    dq_ref, dk_ref, dv_ref, bias_ref,
):
    head = pl.program_id(1)

    @pl.when(head == 0)
    def _():
        fill_bias(seg_q[0], par_q[0], pos_q[0], seg_k[0], pos_k[0], bias_ref)

    @pl.when(lax.rem(head, group) == 0)
    def _():
        dk_ref[...] = jnp.zeros_like(dk_ref)
        dv_ref[...] = jnp.zeros_like(dv_ref)

    in_trunk = (ctx_ref[0] + 1) * rows <= TRUNK
    scale = HEAD ** (-0.5)

    def run(keys):
        @pl.loop(0, rows // block)
        def _(step):
            at = pl.ds(pl.multiple_of(step * block, block), block)
            q_block = q_ref[at, :]
            do_block = do_ref[at, :]
            k_all = k_ref[0, :keys, :]
            probs = probabilities(q_block, k_all, bias_ref[at, :keys])
            dprobs = mm_nt(do_block, v_ref[0, :keys, :])
            delta = jnp.sum(probs * dprobs, axis=1, keepdims=True)
            dscores = (probs * (dprobs - delta)).astype(BF16)
            dq_ref[at, :] = (mm(dscores, k_all) * scale).astype(BF16)
            dk_ref[0, :keys, :] += mm_tn(dscores, q_block) * scale
            dv_ref[0, :keys, :] += mm_tn(probs.astype(BF16), do_block)

    pl.when(in_trunk)(lambda: run(min(TRUNK, tree_len)))
    pl.when(jnp.logical_not(in_trunk))(lambda: run(tree_len))


def attention_specs(rows, tree_len, group, kv_heads):
    return [
        pl.BlockSpec((rows, LANES), lambda b, h, c: (b, h)),
        pl.BlockSpec((1, tree_len, LANES), lambda b, h, c: (b, 0, h // group)),
        pl.BlockSpec((1, tree_len, LANES), lambda b, h, c: (b, 0, kv_heads + h // group)),
    ], [
        pl.BlockSpec((1, rows, 1), lambda b, h, c: (b, 0, 0)),
        pl.BlockSpec((1, rows, 1), lambda b, h, c: (b, 0, 0)),
        pl.BlockSpec((1, rows, 1), lambda b, h, c: (b, 0, 0)),
        pl.BlockSpec((1, 1, tree_len), lambda b, h, c: (b, 0, 0)),
        pl.BlockSpec((1, 1, tree_len), lambda b, h, c: (b, 0, 0)),
    ]


def attend_forward(ctx, q_wide, kv_full, ids, q_heads, kv_heads, rows):
    trees, tree_len, _ = kv_full.shape
    group = q_heads // kv_heads
    first, last = attention_specs(rows, tree_len, group, kv_heads)
    block = min(rows, 256)
    work = trees * q_heads * rows * tree_len
    return pl.pallas_call(
        functools.partial(forward_kernel, rows, tree_len, block),
        grid_spec=pltpu.PrefetchScalarGridSpec(
            num_scalar_prefetch=1,
            grid=(trees, q_heads),
            in_specs=first + last,
            out_specs=pl.BlockSpec((rows, LANES), lambda b, h, c: (b, h)),
            scratch_shapes=[pltpu.VMEM((rows, tree_len), F32)],
        ),
        out_shape=jax.ShapeDtypeStruct(q_wide.shape, BF16),
        cost_estimate=pl.CostEstimate(
            flops=4 * LANES * work, bytes_accessed=8 * q_wide.size, transcendentals=work
        ),
        name="attend_forward",
    )(ctx, q_wide, kv_full, kv_full, *ids)


def attend_backward(ctx, q_wide, kv_full, do_wide, ids, q_heads, kv_heads, rows):
    trees, tree_len, _ = kv_full.shape
    group = q_heads // kv_heads
    first, last = attention_specs(rows, tree_len, group, kv_heads)
    block = min(rows, 256)
    work = trees * q_heads * rows * tree_len
    grad_spec = pl.BlockSpec((1, tree_len, LANES), lambda b, h, c: (b, 0, h // group))
    grad_shape = jax.ShapeDtypeStruct((trees, tree_len, kv_heads * LANES), F32)
    return pl.pallas_call(
        functools.partial(backward_kernel, rows, tree_len, block, group),
        grid_spec=pltpu.PrefetchScalarGridSpec(
            num_scalar_prefetch=1,
            grid=(trees, q_heads),
            in_specs=first + [first[0]] + last,
            out_specs=[first[0], grad_spec, grad_spec],
            scratch_shapes=[pltpu.VMEM((rows, tree_len), F32)],
        ),
        out_shape=[jax.ShapeDtypeStruct(q_wide.shape, BF16), grad_shape, grad_shape],
        cost_estimate=pl.CostEstimate(
            flops=10 * LANES * work, bytes_accessed=12 * q_wide.size, transcendentals=work
        ),
        name="attend_backward",
    )(ctx, q_wide, kv_full, kv_full, do_wide, *ids)


def piece(values, index, size):
    return lax.dynamic_slice_in_dim(values, index * size, size, 1)


def line_reduce_scatter(partial_rows, size, axis):
    count = lax.axis_size(axis)
    here = lax.axis_index(axis)
    from_left = None
    from_right = None
    for step in range(1, count):
        index = jnp.clip(count - step + here, 0, count - 1)
        value = piece(partial_rows, index, size)
        if from_left is not None:
            value = value + from_left.astype(F32)
        pairs = [(i, i + 1) for i in range(step)]
        next_left = lax.ppermute(value.astype(BF16), axis, pairs)
        index = jnp.clip(here - (count - step), 0, count - 1)
        value = piece(partial_rows, index, size)
        if from_right is not None:
            value = value + from_right.astype(F32)
        pairs = [(count - 1 - i, count - 2 - i) for i in range(step)]
        next_right = lax.ppermute(value.astype(BF16), axis, pairs)
        from_left, from_right = next_left, next_right
    total = piece(partial_rows, here, size)
    if from_left is not None:
        total = total + from_left.astype(F32) + from_right.astype(F32)
    return total


def line_all_gather(own, axis):
    count = lax.axis_size(axis)
    here = lax.axis_index(axis)
    trees, size, width = own.shape
    lefts = [own]
    rights = [own]
    for step in range(1, count):
        pairs = [(i, i + 1) for i in range(step - 1, count - 1)]
        lefts.append(lax.ppermute(lefts[-1], axis, pairs))
        pairs = [(i, i - 1) for i in range(count - step, 0, -1)]
        rights.append(lax.ppermute(rights[-1], axis, pairs))
    result = jnp.zeros((trees, count * size, width), own.dtype)
    result = lax.dynamic_update_slice_in_dim(result, own, here * size, 1)
    for step in range(1, count):
        value = jnp.where(here >= step, lefts[step], rights[count - step])
        slot = lax.rem(here - step + count, count)
        result = lax.dynamic_update_slice_in_dim(result, value, slot * size, 1)
    return result


def earlier_gather(own, axis):
    count = lax.axis_size(axis)
    here = lax.axis_index(axis)
    trees, rows, width = own.shape
    result = jnp.zeros((trees, count * rows, width), own.dtype)
    result = lax.dynamic_update_slice_in_dim(result, own, here * rows, 1)
    for step in range(1, count):
        other = lax.ppermute(own, axis, [(i, i + step) for i in range(count - step)])
        slot = lax.rem(here - step + count, count)
        result = lax.dynamic_update_slice_in_dim(result, other, slot * rows, 1)
    return result


def earlier_return(full, axis):
    count = lax.axis_size(axis)
    here = lax.axis_index(axis)
    rows = full.shape[1] // count
    total = piece(full, here, rows)
    for step in range(1, count):
        slot = lax.rem(here - step + count, count)
        other = lax.ppermute(
            piece(full, slot, rows).astype(BF16),
            axis,
            [(i + step, i) for i in range(count - step)],
        )
        total = total + other.astype(F32)
    return total


def small_sum(values, axis):
    count = lax.axis_size(axis)
    total = values
    for step in range(1, count):
        total = total + lax.ppermute(
            values, axis, [(i, (i + step) % count) for i in range(count)]
        )
    return total


def norm_back(grad, values, gain):
    root = lax.rsqrt(jnp.mean(values * values, axis=-1, keepdims=True) + EPS)
    weighted = grad * gain
    mean = jnp.mean(weighted * values, axis=-1, keepdims=True)
    return root * weighted - values * (root * root * root) * mean


def on_device(
    tokens, norm_one, q_weight, k_weight, v_weight, o_weight, norm_two,
    gate_weight, up_weight, down_weight, segment_ids, parent_ids, path_pos, cotangent,
):
    ctx = lax.axis_index("context")
    ctx_count = lax.axis_size("context")
    ten = lax.axis_index("tensor")
    ten_count = lax.axis_size("tensor")
    tree_count, rows, width = tokens.shape
    share = rows // ten_count
    trees = tree_count // MICRO
    flat = trees * rows
    part, q_width = q_weight.shape
    kv_width = k_weight.shape[1]
    q_heads = q_width // HEAD
    kv_heads = kv_width // HEAD
    used = q_width + 2 * kv_width
    packed_width = round_up(used + 2, LANES)
    tree_len = rows * ctx_count

    attention_block = jnp.concatenate(
        [
            q_weight, k_weight, v_weight, norm_one[:, None], norm_two[:, None],
            jnp.zeros((part, packed_width - used - 2), BF16),
        ],
        axis=1,
    )
    attention_full = lax.all_gather(attention_block, WEIGHT_AXES, axis=0, tiled=True)
    o_full = lax.all_gather(o_weight.T, WEIGHT_AXES, axis=0, tiled=True)
    down_full = lax.all_gather(down_weight.T, WEIGHT_AXES, axis=0, tiled=True)
    gate_full = lax.all_gather(gate_weight, WEIGHT_AXES, axis=0, tiled=True)
    up_full = lax.all_gather(up_weight, WEIGHT_AXES, axis=0, tiled=True)
    gain_one = attention_full[:, used].astype(F32)
    gain_two = attention_full[:, used + 1].astype(F32)

    lane = np.arange(q_heads * LANES)
    column = np.arange(q_width)
    select = jnp.asarray(
        (lane[:, None] // LANES == column[None, :] // HEAD)
        & (lane[:, None] % LANES == column[None, :] % HEAD),
        BF16,
    )
    frequency = THETA ** (-(jnp.arange(HALF, dtype=F32) * 2.0 / HEAD))
    pad = jnp.zeros((flat, LANES - HEAD), F32)
    ctx_ref = jnp.reshape(ctx, (1,)).astype(jnp.int32)

    state = []
    for micro in range(MICRO):
        pick = slice(micro * trees, (micro + 1) * trees)
        m = {}
        state.append(m)
        m["x"] = tokens[pick]
        m["dy"] = cotangent[pick]
        seg, par, pos = segment_ids[pick], parent_ids[pick], path_pos[pick]

        def here(ids):
            return lax.dynamic_slice_in_dim(ids, ctx * rows, rows, 1)

        m["ids"] = (
            here(seg)[:, :, None], here(par)[:, :, None], here(pos)[:, :, None],
            seg[:, None, :], pos[:, None, :],
        )
        angles = here(pos).reshape(flat).astype(F32)[:, None] * frequency[None, :]
        cosine, sine = jnp.cos(angles), jnp.sin(angles)
        m["cos"] = jnp.concatenate([cosine, cosine, pad], axis=1)
        m["sin"] = jnp.concatenate([-sine, sine, pad], axis=1)
        x = m["x"].reshape(flat, width).astype(F32)
        m["root_one"] = lax.rsqrt(jnp.mean(x * x, axis=-1, keepdims=True) + EPS)
        m["x_here"] = lax.dynamic_slice_in_dim(m["x"], ten * share, share, 1).astype(F32)
        m["dy_here"] = lax.dynamic_slice_in_dim(m["dy"], ten * share, share, 1).astype(F32)

    for m in state:
        x = m["x"].reshape(flat, width).astype(F32)
        m["normed"] = (x * m["root_one"] * gain_one).astype(BF16)
        packed = mm(m["normed"], attention_full)
        m["q"], kv = split_heads(packed, m["cos"], m["sin"], q_heads, kv_heads, rows)
        m["kv"] = earlier_gather(kv.reshape(trees, rows, -1), "context")
    for m in state:
        wide = attend_forward(ctx_ref, m["q"], m["kv"], m["ids"], q_heads, kv_heads, rows)
        m["attended"] = mm(wide, select).astype(BF16)
        product = mm_nt(m["attended"], o_full).reshape(trees, rows, width)
        m["middle"] = m["x_here"] + line_reduce_scatter(product, share, "tensor")
    for m in state:
        middle = m["middle"]
        root = lax.rsqrt(jnp.mean(middle * middle, axis=-1, keepdims=True) + EPS)
        m["root_two"] = root
        m["normed_two"] = line_all_gather((middle * root * gain_two).astype(BF16), "tensor")

    for m in state:
        m["dmixed"] = mm(m["dy"].reshape(flat, width), down_full)
    for m in state:
        normed_two = m["normed_two"].reshape(flat, width)
        gate = mm(normed_two, gate_full)
        up = mm(normed_two, up_full)
        sigmoid = 1.0 / (1.0 + jnp.exp(-gate))
        silu = gate * sigmoid
        m["mixed"] = (silu * up).astype(BF16)
        slope = sigmoid * (1.0 + gate * (1.0 - sigmoid))
        m["dgate"] = (m["dmixed"] * up * slope).astype(BF16)
        m["dup"] = (m["dmixed"] * silu).astype(BF16)
        dn2 = mm_nt(m["dgate"], gate_full) + mm_nt(m["dup"], up_full)
        m["dn2"] = line_reduce_scatter(dn2.reshape(trees, rows, width), share, "tensor")
    for m in state:
        middle, dn2 = m["middle"], m["dn2"]
        m["gain_two_grad"] = jnp.sum(dn2 * middle * m["root_two"], axis=(0, 1))
        m["dmiddle"] = m["dy_here"] + norm_back(dn2, middle, gain_two)
        m["dmb"] = line_all_gather(m["dmiddle"].astype(BF16), "tensor").reshape(flat, width)
    for m in state:
        out = mm_nt(m["mixed"], down_full).reshape(trees, rows, width)
        m["out"] = (m["middle"] + line_reduce_scatter(out, share, "tensor")).astype(BF16)

    def together(name):
        return jnp.concatenate([m[name].reshape(flat, -1) for m in state], axis=0)

    def scattered(grad):
        return lax.psum_scatter(grad.astype(BF16), WEIGHT_AXES, scatter_dimension=0, tiled=True)

    dy_all = cotangent.reshape(-1, width)
    normed_two_all = together("normed_two")
    down_grad = scattered(mm_tn(dy_all, together("mixed")))
    gate_grad = scattered(mm_tn(normed_two_all, together("dgate")))
    up_grad = scattered(mm_tn(normed_two_all, together("dup")))

    for m in state:
        dattended = mm(m["dmb"], o_full).astype(BF16)
        do_wide = mm_nt(dattended, select).astype(BF16)
        dq, dk, dv = attend_backward(
            ctx_ref, m["q"], m["kv"], do_wide, m["ids"], q_heads, kv_heads, rows
        )
        dkv = earlier_return(jnp.concatenate([dk, dv], axis=2), "context").reshape(flat, -1)
        m["dqkv"] = pack_heads(
            dq, dkv, m["cos"], m["sin"], q_heads, kv_heads, packed_width, rows
        )
        dn1 = mm_nt(m["dqkv"], attention_full)
        x = m["x"].reshape(flat, width).astype(F32)
        m["gain_one_grad"] = jnp.sum(dn1 * x * m["root_one"], axis=0)
        m["dn1"] = line_reduce_scatter(dn1.reshape(trees, rows, width), share, "tensor")
    o_grad = scattered(mm_tn(together("dmb"), together("attended")))
    for m in state:
        m["dx"] = (m["dmiddle"] + norm_back(m["dn1"], m["x_here"], gain_one)).astype(BF16)

    attention_grad = mm_tn(together("normed"), together("dqkv"))
    gains = [sum(m[name] for m in state) for name in ("gain_one_grad", "gain_two_grad")]
    columns = lax.broadcasted_iota(jnp.int32, attention_grad.shape, 1)
    attention_grad = jnp.where(
        columns == used,
        gains[0][:, None],
        jnp.where(columns == used + 1, gains[1][:, None], attention_grad),
    )
    attention_grad = scattered(attention_grad).astype(F32)
    gain_grads = small_sum(attention_grad[:, used : used + 2], "tensor")
    return (
        jnp.concatenate([m["out"] for m in state], axis=0),
        jnp.concatenate([m["dx"] for m in state], axis=0),
        gain_grads[:, 0],
        attention_grad[:, :q_width],
        attention_grad[:, q_width : q_width + kv_width],
        attention_grad[:, q_width + kv_width : used],
        o_grad.T.astype(F32),
        gain_grads[:, 1],
        gate_grad.astype(F32),
        up_grad.astype(F32),
        down_grad.T.astype(F32),
    )


def solution(mesh):
    weights = ("fsdp", "context")
    return jax.shard_map(
        on_device,
        mesh=mesh,
        in_specs=(
            P("fsdp", "context", None),
            P(weights),
            P(weights, "tensor"),
            P(weights, "tensor"),
            P(weights, "tensor"),
            P("tensor", weights),
            P(weights),
            P(weights, "tensor"),
            P(weights, "tensor"),
            P("tensor", weights),
            P("fsdp", None),
            P("fsdp", None),
            P("fsdp", None),
            P("fsdp", "context", None),
        ),
        out_specs=(
            P("fsdp", ("context", "tensor"), None),
            P("fsdp", ("context", "tensor"), None),
            P(weights),
            P(weights, "tensor"),
            P(weights, "tensor"),
            P(weights, "tensor"),
            P("tensor", weights),
            P(weights),
            P(weights, "tensor"),
            P(weights, "tensor"),
            P("tensor", weights),
        ),
        check_vma=False,
    )
```

```python
import functools

import jax
import jax.numpy as jnp
import numpy as np
from jax import lax
from jax.experimental import pallas as pl
from jax.experimental.pallas import tpu as pltpu
from jax.experimental.layout import Layout, with_layout_constraint
from jax.sharding import PartitionSpec as P

HEADS = 32
KV_HEADS = 8
HEAD = 80
HALF = HEAD // 2
LANES = 128
MICRO = 2
EPS = 1e-05
THETA = 10000.0
NEG = -1000000000.0
TRUNK = 512
WEIGHT_AXES = ("fsdp", "context")
BF16 = jnp.bfloat16
F32 = jnp.float32


def row_major(value):
    return with_layout_constraint(value, Layout(major_to_minor=(0, 1)))


def round_up(value, unit):
    return (value + unit - 1) // unit * unit


def mm(left, right):
    return lax.dot_general(left, right, (((1,), (0,)), ((), ())), preferred_element_type=F32)


def mm_nt(left, right):
    return lax.dot_general(left, right, (((1,), (1,)), ((), ())), preferred_element_type=F32)


def mm_tn(left, right):
    return lax.dot_general(left, right, (((0,), (0,)), ((), ())), preferred_element_type=F32)


def rotated(values, cos_table, sin_table):
    lane = lax.broadcasted_iota(jnp.int32, values.shape, 1)
    swapped = jnp.where(
        lane < HALF, pltpu.roll(values, LANES - HALF, 1), pltpu.roll(values, HALF, 1)
    )
    return values * cos_table + swapped * sin_table


def window_of(head):
    start = head * HEAD
    base = start // LANES * LANES
    return base, start - base


def split_kernel(q_heads, kv_heads, x_ref, cos_ref, sin_ref, q_ref, kv_ref):
    cos_table = cos_ref[...]
    sin_table = sin_ref[...]
    for head in range(q_heads + 2 * kv_heads):
        base, shift = window_of(head)
        window = x_ref[:, base : base + 2 * LANES]
        if shift:
            window = pltpu.roll(window, 2 * LANES - shift, 1)
        values = window[:, :LANES]
        if head < q_heads + kv_heads:
            result = rotated(values, cos_table, sin_table)
        else:
            lane = lax.broadcasted_iota(jnp.int32, values.shape, 1)
            result = jnp.where(lane < HEAD, values, 0.0)
        result = result.astype(BF16)
        if head < q_heads:
            q_ref[:, head * LANES : (head + 1) * LANES] = result
        else:
            at = (head - q_heads) * LANES
            kv_ref[:, at : at + LANES] = result


def split_heads(packed, cos_table, sin_table, q_heads, kv_heads, rows):
    total, width = packed.shape
    q_wide = q_heads * LANES
    kv_wide = 2 * kv_heads * LANES
    return pl.pallas_call(
        functools.partial(split_kernel, q_heads, kv_heads),
        grid=(total // rows,),
        in_specs=[
            pl.BlockSpec((rows, width), lambda b: (b, 0)),
            pl.BlockSpec((rows, LANES), lambda b: (b, 0)),
            pl.BlockSpec((rows, LANES), lambda b: (b, 0)),
        ],
        out_specs=[
            pl.BlockSpec((rows, q_wide), lambda b: (b, 0)),
            pl.BlockSpec((rows, kv_wide), lambda b: (b, 0)),
        ],
        out_shape=[
            jax.ShapeDtypeStruct((total, q_wide), BF16),
            jax.ShapeDtypeStruct((total, kv_wide), BF16),
        ],
        cost_estimate=pl.CostEstimate(
            flops=10 * total * width, bytes_accessed=7 * total * width, transcendentals=0
        ),
        name="split_heads",
    )(packed, cos_table, sin_table)


def pack_kernel(q_heads, kv_heads, dq_ref, dkv_ref, cos_ref, sin_ref, out_ref, sum_ref):
    cos_table = cos_ref[...]
    sin_table = -sin_ref[...]
    sum_ref[...] = jnp.zeros_like(sum_ref)
    for head in range(q_heads + 2 * kv_heads):
        base, shift = window_of(head)
        if head < q_heads:
            values = dq_ref[:, head * LANES : (head + 1) * LANES].astype(F32)
        else:
            at = (head - q_heads) * LANES
            values = dkv_ref[:, at : at + LANES].astype(BF16).astype(F32)
        if head < q_heads + kv_heads:
            values = rotated(values, cos_table, sin_table)
        wide = jnp.concatenate([values, jnp.zeros_like(values)], axis=1)
        if shift:
            wide = pltpu.roll(wide, shift, 1)
        sum_ref[:, base : base + 2 * LANES] += wide
    out_ref[...] = sum_ref[...].astype(BF16)


def pack_heads(dq_wide, dkv, cos_table, sin_table, q_heads, kv_heads, width, rows):
    total = dq_wide.shape[0]
    return pl.pallas_call(
        functools.partial(pack_kernel, q_heads, kv_heads),
        grid=(total // rows,),
        in_specs=[
            pl.BlockSpec((rows, dq_wide.shape[1]), lambda b: (b, 0)),
            pl.BlockSpec((rows, dkv.shape[1]), lambda b: (b, 0)),
            pl.BlockSpec((rows, LANES), lambda b: (b, 0)),
            pl.BlockSpec((rows, LANES), lambda b: (b, 0)),
        ],
        out_specs=pl.BlockSpec((rows, width), lambda b: (b, 0)),
        out_shape=jax.ShapeDtypeStruct((total, width), BF16),
        scratch_shapes=[pltpu.VMEM((rows, width), F32)],
        cost_estimate=pl.CostEstimate(
            flops=10 * total * width, bytes_accessed=7 * total * width, transcendentals=0
        ),
        name="pack_heads",
    )(dq_wide, dkv, cos_table, sin_table)


def fill_bias(seg_q, par_q, pos_q, seg_k, pos_k, bias_ref):
    same = (seg_k == seg_q) | (seg_k == par_q) | (seg_k == 0)
    bias_ref[...] = jnp.where(same & (pos_k <= pos_q), 0.0, NEG)


def probabilities(q_block, keys, bias):
    scores = mm_nt(q_block, keys) * HEAD ** (-0.5) + bias
    top = jnp.max(scores, axis=1, keepdims=True)
    raised = jnp.exp(scores - top)
    return raised * (1.0 / jnp.sum(raised, axis=1, keepdims=True))


def forward_kernel(
    rows, tree_len, block,
    ctx_ref, q_ref, k_ref, v_ref, seg_q, par_q, pos_q, seg_k, pos_k, out_ref, bias_ref,
):
    @pl.when(pl.program_id(1) == 0)
    def _():
        fill_bias(seg_q[0], par_q[0], pos_q[0], seg_k[0], pos_k[0], bias_ref)

    in_trunk = (ctx_ref[0] + 1) * rows <= TRUNK

    def run(keys):
        @pl.loop(0, rows // block)
        def _(step):
            at = pl.ds(pl.multiple_of(step * block, block), block)
            probs = probabilities(q_ref[at, :], k_ref[0, :keys, :], bias_ref[at, :keys])
            out_ref[at, :] = mm(probs.astype(BF16), v_ref[0, :keys, :]).astype(BF16)

    pl.when(in_trunk)(lambda: run(min(TRUNK, tree_len)))
    pl.when(jnp.logical_not(in_trunk))(lambda: run(tree_len))


def backward_kernel(
    rows, tree_len, block, group,
    ctx_ref, q_ref, k_ref, v_ref, do_ref, seg_q, par_q, pos_q, seg_k, pos_k,
    dq_ref, dk_ref, dv_ref, bias_ref,
):
    head = pl.program_id(1)

    @pl.when(head == 0)
    def _():
        fill_bias(seg_q[0], par_q[0], pos_q[0], seg_k[0], pos_k[0], bias_ref)

    @pl.when(lax.rem(head, group) == 0)
    def _():
        dk_ref[...] = jnp.zeros_like(dk_ref)
        dv_ref[...] = jnp.zeros_like(dv_ref)

    in_trunk = (ctx_ref[0] + 1) * rows <= TRUNK
    scale = HEAD ** (-0.5)

    def run(keys):
        @pl.loop(0, rows // block)
        def _(step):
            at = pl.ds(pl.multiple_of(step * block, block), block)
            q_block = q_ref[at, :]
            do_block = do_ref[at, :]
            k_all = k_ref[0, :keys, :]
            probs = probabilities(q_block, k_all, bias_ref[at, :keys])
            dprobs = mm_nt(do_block, v_ref[0, :keys, :])
            delta = jnp.sum(probs * dprobs, axis=1, keepdims=True)
            dscores = (probs * (dprobs - delta)).astype(BF16)
            dq_ref[at, :] = (mm(dscores, k_all) * scale).astype(BF16)
            dk_ref[0, :keys, :] += mm_tn(dscores, q_block) * scale
            dv_ref[0, :keys, :] += mm_tn(probs.astype(BF16), do_block)

    pl.when(in_trunk)(lambda: run(min(TRUNK, tree_len)))
    pl.when(jnp.logical_not(in_trunk))(lambda: run(tree_len))


def attention_specs(rows, tree_len, group, kv_heads):
    return [
        pl.BlockSpec((rows, LANES), lambda b, h, c: (b, h)),
        pl.BlockSpec((1, tree_len, LANES), lambda b, h, c: (b, 0, h // group)),
        pl.BlockSpec((1, tree_len, LANES), lambda b, h, c: (b, 0, kv_heads + h // group)),
    ], [
        pl.BlockSpec((1, rows, 1), lambda b, h, c: (b, 0, 0)),
        pl.BlockSpec((1, rows, 1), lambda b, h, c: (b, 0, 0)),
        pl.BlockSpec((1, rows, 1), lambda b, h, c: (b, 0, 0)),
        pl.BlockSpec((1, 1, tree_len), lambda b, h, c: (b, 0, 0)),
        pl.BlockSpec((1, 1, tree_len), lambda b, h, c: (b, 0, 0)),
    ]


def attend_forward(ctx, q_wide, kv_full, ids, q_heads, kv_heads, rows):
    trees, tree_len, _ = kv_full.shape
    group = q_heads // kv_heads
    first, last = attention_specs(rows, tree_len, group, kv_heads)
    block = min(rows, 256)
    work = trees * q_heads * rows * tree_len
    return pl.pallas_call(
        functools.partial(forward_kernel, rows, tree_len, block),
        grid_spec=pltpu.PrefetchScalarGridSpec(
            num_scalar_prefetch=1,
            grid=(trees, q_heads),
            in_specs=first + last,
            out_specs=pl.BlockSpec((rows, LANES), lambda b, h, c: (b, h)),
            scratch_shapes=[pltpu.VMEM((rows, tree_len), F32)],
        ),
        out_shape=jax.ShapeDtypeStruct(q_wide.shape, BF16),
        cost_estimate=pl.CostEstimate(
            flops=4 * LANES * work, bytes_accessed=8 * q_wide.size, transcendentals=work
        ),
        name="attend_forward",
    )(ctx, q_wide, kv_full, kv_full, *ids)


def attend_backward(ctx, q_wide, kv_full, do_wide, ids, q_heads, kv_heads, rows):
    trees, tree_len, _ = kv_full.shape
    group = q_heads // kv_heads
    first, last = attention_specs(rows, tree_len, group, kv_heads)
    block = min(rows, 256)
    work = trees * q_heads * rows * tree_len
    grad_spec = pl.BlockSpec((1, tree_len, LANES), lambda b, h, c: (b, 0, h // group))
    grad_shape = jax.ShapeDtypeStruct((trees, tree_len, kv_heads * LANES), F32)
    return pl.pallas_call(
        functools.partial(backward_kernel, rows, tree_len, block, group),
        grid_spec=pltpu.PrefetchScalarGridSpec(
            num_scalar_prefetch=1,
            grid=(trees, q_heads),
            in_specs=first + [first[0]] + last,
            out_specs=[first[0], grad_spec, grad_spec],
            scratch_shapes=[pltpu.VMEM((rows, tree_len), F32)],
        ),
        out_shape=[jax.ShapeDtypeStruct(q_wide.shape, BF16), grad_shape, grad_shape],
        cost_estimate=pl.CostEstimate(
            flops=10 * LANES * work, bytes_accessed=12 * q_wide.size, transcendentals=work
        ),
        name="attend_backward",
    )(ctx, q_wide, kv_full, kv_full, do_wide, *ids)


def piece(values, index, size):
    return lax.dynamic_slice_in_dim(values, index * size, size, 1)


class LineSum:
    def __init__(self, values, size, axis):
        self.values, self.size, self.axis = values, size, axis
        self.count = lax.axis_size(axis)
        self.here = lax.axis_index(axis)
        self.step = 0
        self.got = None

    def sends(self):
        self.step += 1
        step, count = self.step, self.count
        away = count - step
        rights = [(i, i + 1) for i in range(step)]
        lefts = [(count - 1 - i, count - 2 - i) for i in range(step)]
        found = []
        for side, pairs in ((0, rights), (1, lefts)):
            index = jnp.clip(self.here + (away, -away)[side], 0, count - 1)
            value = piece(self.values, index, self.size)
            if self.got is not None:
                value = value + self.got[side].astype(F32)
            found.append((value.astype(BF16), self.axis, pairs))
        return found

    def receive(self, results):
        self.got = results

    def result(self):
        assert self.step == self.count - 1
        total = piece(self.values, self.here, self.size)
        for other in self.got or ():
            total = total + other.astype(F32)
        return total


class LineGather:
    def __init__(self, own, axis):
        self.own, self.axis = own, axis
        self.count = lax.axis_size(axis)
        self.here = lax.axis_index(axis)
        self.lefts, self.rights = [own], [own]

    def sends(self):
        step, count = len(self.lefts), self.count
        return [
            (self.lefts[-1], self.axis, [(i, i + 1) for i in range(step - 1, count - 1)]),
            (self.rights[-1], self.axis, [(i, i - 1) for i in range(count - step, 0, -1)]),
        ]

    def receive(self, results):
        self.lefts.append(results[0])
        self.rights.append(results[1])

    def result(self):
        count, here, own = self.count, self.here, self.own
        assert len(self.lefts) == count
        trees, size, width = own.shape
        result = jnp.zeros((trees, count * size, width), own.dtype)
        result = lax.dynamic_update_slice_in_dim(result, own, here * size, 1)
        for step in range(1, count):
            value = jnp.where(here >= step, self.lefts[step], self.rights[count - step])
            slot = lax.rem(here - step + count, count)
            result = lax.dynamic_update_slice_in_dim(result, value, slot * size, 1)
        return result


class EarlierGather:
    def __init__(self, own, axis):
        self.own, self.axis = own, axis
        self.count = lax.axis_size(axis)

    def sends(self):
        count = self.count
        return [
            (self.own, self.axis, [(i, i + step) for i in range(count - step)])
            for step in range(1, count)
        ]

    def receive(self, results):
        self.others = results

    def result(self):
        count, own = self.count, self.own
        here = lax.axis_index(self.axis)
        trees, rows, width = own.shape
        result = jnp.zeros((trees, count * rows, width), own.dtype)
        result = lax.dynamic_update_slice_in_dim(result, own, here * rows, 1)
        for step, other in enumerate(self.others, 1):
            slot = lax.rem(here - step + count, count)
            result = lax.dynamic_update_slice_in_dim(result, other, slot * rows, 1)
        return result


class EarlierReturn:
    def __init__(self, full, axis):
        self.full, self.axis = full, axis
        self.count = lax.axis_size(axis)
        self.rows = full.shape[1] // self.count

    def sends(self):
        count = self.count
        here = lax.axis_index(self.axis)
        found = []
        for step in range(1, count):
            slot = lax.rem(here - step + count, count)
            value = piece(self.full, slot, self.rows).astype(BF16)
            found.append((value, self.axis, [(i + step, i) for i in range(count - step)]))
        return found

    def receive(self, results):
        self.others = results

    def result(self):
        total = piece(self.full, lax.axis_index(self.axis), self.rows)
        for other in self.others:
            total = total + other.astype(F32)
        return total


class Stages:
    def __init__(self):
        self.token = ()

    def wait_for(self, *values):
        self.token += values

    def __call__(self, transfers, compute=None, inputs=()):
        transfers = [t for t in transfers if getattr(t, "count", 2) > 1]
        groups = [t.sends() for t in transfers]
        values = [value for group in groups for value, _, _ in group]
        tied = lax.optimization_barrier((*values, *inputs, *self.token))
        token, at = [], 0
        for transfer, group in zip(transfers, groups):
            results = []
            for _, axis, pairs in group:
                results.append(lax.ppermute(tied[at], axis, pairs))
                at += 1
            transfer.receive(results)
            token += results
        outs = compute(*tied[at : at + len(inputs)]) if compute else ()
        token += [o for o in outs]
        self.token = tuple(token)
        return outs


def small_sum(values, axis):
    count = lax.axis_size(axis)
    total = values
    for step in range(1, count):
        total = total + lax.ppermute(
            values, axis, [(i, (i + step) % count) for i in range(count)]
        )
    return total


def norm_back(grad, values, gain):
    root = lax.rsqrt(jnp.mean(values * values, axis=-1, keepdims=True) + EPS)
    weighted = grad * gain
    mean = jnp.mean(weighted * values, axis=-1, keepdims=True)
    return root * weighted - values * (root * root * root) * mean


def on_device(
    tokens, norm_one, q_weight, k_weight, v_weight, o_weight, norm_two,
    gate_weight, up_weight, down_weight, segment_ids, parent_ids, path_pos, cotangent,
):
    ctx = lax.axis_index("context")
    ctx_count = lax.axis_size("context")
    ten = lax.axis_index("tensor")
    ten_count = lax.axis_size("tensor")
    tree_count, rows, width = tokens.shape
    share = rows // ten_count
    trees = tree_count // MICRO
    flat = trees * rows
    part, q_width = q_weight.shape
    kv_width = k_weight.shape[1]
    q_heads = q_width // HEAD
    kv_heads = kv_width // HEAD
    used = q_width + 2 * kv_width
    packed_width = round_up(used + 2, LANES)
    tree_len = rows * ctx_count

    attention_block = jnp.concatenate(
        [
            q_weight, k_weight, v_weight, norm_one[:, None], norm_two[:, None],
            jnp.zeros((part, packed_width - used - 2), BF16),
        ],
        axis=1,
    )
    attention_full = lax.all_gather(attention_block, WEIGHT_AXES, axis=0, tiled=True)
    o_full = lax.all_gather(o_weight.T, WEIGHT_AXES, axis=0, tiled=True)
    down_full = lax.all_gather(down_weight.T, WEIGHT_AXES, axis=0, tiled=True)
    gate_full = lax.all_gather(gate_weight, WEIGHT_AXES, axis=0, tiled=True)
    up_full = lax.all_gather(up_weight, WEIGHT_AXES, axis=0, tiled=True)
    gain_one = attention_full[:, used].astype(F32)
    gain_two = attention_full[:, used + 1].astype(F32)

    lane = np.arange(q_heads * LANES)
    column = np.arange(q_width)
    select = jnp.asarray(
        (lane[:, None] // LANES == column[None, :] // HEAD)
        & (lane[:, None] % LANES == column[None, :] % HEAD),
        BF16,
    )
    frequency = THETA ** (-(jnp.arange(HALF, dtype=F32) * 2.0 / HEAD))
    pad = jnp.zeros((flat, LANES - HEAD), F32)
    ctx_ref = jnp.reshape(ctx, (1,)).astype(jnp.int32)

    state = []
    for micro in range(MICRO):
        pick = slice(micro * trees, (micro + 1) * trees)
        m = {}
        state.append(m)
        m["x"] = tokens[pick]
        m["dy"] = cotangent[pick]
        seg, par, pos = segment_ids[pick], parent_ids[pick], path_pos[pick]

        def here(ids):
            return lax.dynamic_slice_in_dim(ids, ctx * rows, rows, 1)

        m["ids"] = (
            here(seg)[:, :, None], here(par)[:, :, None], here(pos)[:, :, None],
            seg[:, None, :], pos[:, None, :],
        )
        angles = here(pos).reshape(flat).astype(F32)[:, None] * frequency[None, :]
        cosine, sine = jnp.cos(angles), jnp.sin(angles)
        m["cos"] = jnp.concatenate([cosine, cosine, pad], axis=1)
        m["sin"] = jnp.concatenate([-sine, sine, pad], axis=1)
        x = m["x"].reshape(flat, width).astype(F32)
        m["root_one"] = lax.rsqrt(jnp.mean(x * x, axis=-1, keepdims=True) + EPS)
        m["x_here"] = lax.dynamic_slice_in_dim(m["x"], ten * share, share, 1).astype(F32)
        m["dy_here"] = lax.dynamic_slice_in_dim(m["dy"], ten * share, share, 1).astype(F32)

    def scattered(grad):
        return lax.psum_scatter(grad, WEIGHT_AXES, scatter_dimension=0, tiled=True)

    def together(name):
        return jnp.concatenate([m[name].reshape(flat, -1) for m in state], axis=0)

    def shaped(product):
        return product.reshape(trees, rows, width)

    stage = Stages()
    a, b = state

    def project(m):
        def run(root):
            x = m["x"].reshape(flat, width).astype(F32)
            m["normed"] = (x * root * gain_one).astype(BF16)
            packed = mm(m["normed"], attention_full)
            m["q"], kv = split_heads(packed, m["cos"], m["sin"], q_heads, kv_heads, rows)
            m["kv"] = EarlierGather(kv.reshape(trees, rows, -1), "context")
            return (m["q"],)
        return run

    def attend(m):
        def run(q):
            m["kv_full"] = m["kv"].result()
            wide = attend_forward(ctx_ref, q, m["kv_full"], m["ids"], q_heads, kv_heads, rows)
            m["attended"] = mm(wide, select).astype(BF16)
            product = mm_nt(m["attended"], o_full)
            m["sum1"] = LineSum(shaped(product), share, "tensor")
            return (product,)
        return run

    def mixed_back(m):
        def run(dy):
            m["dmixed"] = row_major(mm(dy.reshape(flat, width), down_full))
            return (m["dmixed"],)
        return run

    def norm_two_of(m):
        middle = m["x_here"] + m["sum1"].result()
        root = lax.rsqrt(jnp.mean(middle * middle, axis=-1, keepdims=True) + EPS)
        m["middle"], m["root_two"] = middle, root
        m["gather1"] = LineGather((middle * root * gain_two).astype(BF16), "tensor")

    def gate_of(m):
        def run(normed_two):
            m["normed_two"] = normed_two
            m["gate"] = row_major(mm(normed_two, gate_full))
            return (m["gate"],)
        return run

    def up_of(m):
        def run(gate):
            up = row_major(mm(m["normed_two"], up_full))
            sigmoid = 1.0 / (1.0 + jnp.exp(-gate))
            silu = gate * sigmoid
            slope = sigmoid * (1.0 + gate * (1.0 - sigmoid))
            m["mixed"] = row_major((silu * up).astype(BF16))
            m["dgate"] = row_major((m["dmixed"] * up * slope).astype(BF16))
            m["dup"] = row_major((m["dmixed"] * silu).astype(BF16))
            return (m["mixed"], m["dgate"], m["dup"])
        return run

    def back_of(m):
        def run(dgate):
            product = mm_nt(dgate, gate_full) + mm_nt(m["dup"], up_full)
            m["sum3"] = LineSum(shaped(product), share, "tensor")
            return (product,)
        return run

    def norm_two_back(m):
        middle, dn2 = m["middle"], m["sum3"].result()
        m["gain_two_grad"] = jnp.sum(dn2 * middle * m["root_two"], axis=(0, 1))
        m["dmiddle"] = m["dy_here"] + norm_back(dn2, middle, gain_two)
        m["gather2"] = LineGather(m["dmiddle"].astype(BF16), "tensor")

    def out_of(m):
        def run(mixed):
            product = mm_nt(mixed, down_full)
            m["sum2"] = LineSum(shaped(product), share, "tensor")
            return (product,)
        return run

    def attend_back(m):
        def run(dmb):
            m["dmb"] = dmb
            dattended = mm(dmb, o_full).astype(BF16)
            do_wide = mm_nt(dattended, select).astype(BF16)
            m["dq"], dk, dv = attend_backward(
                ctx_ref, m["q"], m["kv_full"], do_wide, m["ids"], q_heads, kv_heads, rows
            )
            m["dkv"] = EarlierReturn(jnp.concatenate([dk, dv], axis=2), "context")
            return (m["dq"],)
        return run

    def norm_one_back(m):
        def run(dq):
            dkv = m["dkv"].result().reshape(flat, -1)
            m["dqkv"] = pack_heads(
                dq, dkv, m["cos"], m["sin"], q_heads, kv_heads, packed_width, rows
            )
            dn1 = mm_nt(m["dqkv"], attention_full)
            x = m["x"].reshape(flat, width).astype(F32)
            m["gain_one_grad"] = jnp.sum(dn1 * x * m["root_one"], axis=0)
            m["sum4"] = LineSum(shaped(dn1), share, "tensor")
            return (dn1,)
        return run

    weight_grads = {}

    def weight_grad(name, left_of, right_of):
        def run(tied):
            left = tied if left_of is None else left_of()
            weight_grads[name] = row_major(mm_tn(left, right_of()).astype(BF16))
            return (weight_grads[name],)
        return run

    def both(*steps):
        def run(*values):
            return tuple(out for step, v in zip(steps, values) for out in step(v))
        return run

    stage([], project(a), [a["root_one"]])
    stage([a["kv"]], project(b), [b["root_one"]])
    stage([b["kv"]], attend(a), [a["q"]])
    stage([a["sum1"]], attend(b), [b["q"]])
    stage([a["sum1"], b["sum1"]])
    stage([a["sum1"], b["sum1"]])
    norm_two_of(a)
    stage([a["gather1"], b["sum1"]], mixed_back(a), [a["dy"]])
    norm_two_of(b)
    stage([a["gather1"], b["gather1"]], mixed_back(b), [b["dy"]])
    stage([a["gather1"], b["gather1"]])
    stage([b["gather1"]], gate_of(a), [a["gather1"].result().reshape(flat, width)])
    stage([], up_of(a), [a["gate"]])
    stage([], back_of(a), [a["dgate"]])
    stage([a["sum3"]], gate_of(b), [b["gather1"].result().reshape(flat, width)])
    stage([a["sum3"]], up_of(b), [b["gate"]])
    dy_all = cotangent.reshape(-1, width)
    stage(
        [a["sum3"]],
        both(back_of(b), weight_grad("down", lambda: dy_all, lambda: together("mixed"))),
        [b["dgate"], b["mixed"]],
    )
    down_grad = scattered(weight_grads["down"])
    norm_two_back(a)
    normed_two_all = together("normed_two")
    stage(
        [a["gather2"], b["sum3"]],
        weight_grad("gate", None, lambda: together("dgate")),
        [normed_two_all],
    )
    gate_grad = scattered(weight_grads["gate"])
    stage(
        [a["gather2"], b["sum3"]],
        weight_grad("up", None, lambda: together("dup")),
        [normed_two_all],
    )
    up_grad = scattered(weight_grads["up"])
    stage([a["gather2"], b["sum3"]], both(out_of(a), out_of(b)), [a["mixed"], b["mixed"]])
    norm_two_back(b)
    stage.wait_for(down_grad)
    stage([b["gather2"]], attend_back(a), [a["gather2"].result().reshape(flat, width)])
    stage([b["gather2"], a["dkv"]])
    stage([b["gather2"], a["sum2"]], norm_one_back(a), [a["dq"]])
    stage.wait_for(gate_grad)
    stage(
        [a["sum4"], a["sum2"]], attend_back(b), [b["gather2"].result().reshape(flat, width)]
    )
    stage(
        [a["sum4"], b["dkv"], b["sum2"]],
        weight_grad("o", None, lambda: together("attended")),
        [together("dmb")],
    )
    o_grad = scattered(weight_grads["o"])
    stage([a["sum4"], a["sum2"]], norm_one_back(b), [b["dq"]])

    def attention_weight_grad():
        grad = mm_tn(together("normed"), together("dqkv"))
        gains = [sum(m[name] for m in state) for name in ("gain_one_grad", "gain_two_grad")]
        columns = lax.broadcasted_iota(jnp.int32, grad.shape, 1)
        grad = jnp.where(
            columns == used,
            gains[0][:, None],
            jnp.where(columns == used + 1, gains[1][:, None], grad),
        )
        weight_grads["attention"] = grad.astype(BF16)
        return (weight_grads["attention"],)

    stage.wait_for(up_grad)
    stage([b["sum4"], b["sum2"]], attention_weight_grad)
    attention_grad = scattered(weight_grads["attention"]).astype(F32)
    stage([b["sum4"], b["sum2"]])
    stage.wait_for(o_grad)
    stage([b["sum4"]])
    for m in state:
        m["out"] = (m["middle"] + m["sum2"].result()).astype(BF16)
        m["dx"] = (m["dmiddle"] + norm_back(m["sum4"].result(), m["x_here"], gain_one)).astype(BF16)

    gain_grads = small_sum(attention_grad[:, used : used + 2], "tensor")
    return (
        jnp.concatenate([m["out"] for m in state], axis=0),
        jnp.concatenate([m["dx"] for m in state], axis=0),
        gain_grads[:, 0],
        attention_grad[:, :q_width],
        attention_grad[:, q_width : q_width + kv_width],
        attention_grad[:, q_width + kv_width : used],
        o_grad.T.astype(F32),
        gain_grads[:, 1],
        gate_grad.astype(F32),
        up_grad.astype(F32),
        down_grad.T.astype(F32),
    )


def solution(mesh):
    weights = ("fsdp", "context")
    return jax.shard_map(
        on_device,
        mesh=mesh,
        in_specs=(
            P("fsdp", "context", None),
            P(weights),
            P(weights, "tensor"),
            P(weights, "tensor"),
            P(weights, "tensor"),
            P("tensor", weights),
            P(weights),
            P(weights, "tensor"),
            P(weights, "tensor"),
            P("tensor", weights),
            P("fsdp", None),
            P("fsdp", None),
            P("fsdp", None),
            P("fsdp", "context", None),
        ),
        out_specs=(
            P("fsdp", ("context", "tensor"), None),
            P("fsdp", ("context", "tensor"), None),
            P(weights),
            P(weights, "tensor"),
            P(weights, "tensor"),
            P(weights, "tensor"),
            P("tensor", weights),
            P(weights),
            P(weights, "tensor"),
            P(weights, "tensor"),
            P("tensor", weights),
        ),
        check_vma=False,
    )
```

```python
import functools
from types import SimpleNamespace

import jax
import jax.numpy as jnp
import numpy as np
from jax import lax
from jax.experimental import pallas as pl
from jax.experimental.pallas import tpu as pltpu
from jax.experimental.layout import Layout, with_layout_constraint
from jax.sharding import PartitionSpec as P


HEAD = 80
HALF = HEAD // 2
LANES = 128
MICRO = 2
EPS = 1e-05
THETA = 10000.0
NEG = -1000000000.0
TRUNK = 512
WEIGHT_AXES = ("fsdp", "context")
BF16 = jnp.bfloat16
F32 = jnp.float32


def after(value, *others):
    return lax.optimization_barrier((value, *others))[0]


def row_major(value):
    return with_layout_constraint(value, Layout(major_to_minor=(0, 1)))


def round_up(value, unit):
    return (value + unit - 1) // unit * unit


def mm(left, right):
    return lax.dot_general(left, right, (((1,), (0,)), ((), ())), preferred_element_type=F32)


def mm_nt(left, right):
    return lax.dot_general(left, right, (((1,), (1,)), ((), ())), preferred_element_type=F32)


def mm_tn(left, right):
    return lax.dot_general(left, right, (((0,), (0,)), ((), ())), preferred_element_type=F32)


def rotated(values, cos_table, sin_table):
    lane = lax.broadcasted_iota(jnp.int32, values.shape, 1)
    swapped = jnp.where(
        lane < HALF, pltpu.roll(values, LANES - HALF, 1), pltpu.roll(values, HALF, 1)
    )
    return values * cos_table + swapped * sin_table


def window_of(head):
    start = head * HEAD
    base = start // LANES * LANES
    return base, start - base


def split_kernel(q_heads, kv_heads, x_ref, cos_ref, sin_ref, q_ref, kv_ref):
    cos_table = cos_ref[...]
    sin_table = sin_ref[...]
    for head in range(q_heads + 2 * kv_heads):
        base, shift = window_of(head)
        window = x_ref[:, base : base + 2 * LANES]
        if shift:
            window = pltpu.roll(window, 2 * LANES - shift, 1)
        values = window[:, :LANES]
        if head < q_heads + kv_heads:
            result = rotated(values, cos_table, sin_table)
        else:
            lane = lax.broadcasted_iota(jnp.int32, values.shape, 1)
            result = jnp.where(lane < HEAD, values, 0.0)
        result = result.astype(BF16)
        if head < q_heads:
            q_ref[:, head * LANES : (head + 1) * LANES] = result
        else:
            at = (head - q_heads) * LANES
            kv_ref[:, at : at + LANES] = result


def split_heads(packed, cos_table, sin_table, q_heads, kv_heads, rows):
    total, width = packed.shape
    q_wide = q_heads * LANES
    kv_wide = 2 * kv_heads * LANES
    return pl.pallas_call(
        functools.partial(split_kernel, q_heads, kv_heads),
        grid=(total // rows,),
        in_specs=[
            pl.BlockSpec((rows, width), lambda b: (b, 0)),
            pl.BlockSpec((rows, LANES), lambda b: (b, 0)),
            pl.BlockSpec((rows, LANES), lambda b: (b, 0)),
        ],
        out_specs=[
            pl.BlockSpec((rows, q_wide), lambda b: (b, 0)),
            pl.BlockSpec((rows, kv_wide), lambda b: (b, 0)),
        ],
        out_shape=[
            jax.ShapeDtypeStruct((total, q_wide), BF16),
            jax.ShapeDtypeStruct((total, kv_wide), BF16),
        ],
        cost_estimate=pl.CostEstimate(
            flops=10 * total * width, bytes_accessed=7 * total * width, transcendentals=0
        ),
        name="split_heads",
    )(packed, cos_table, sin_table)


def pack_kernel(q_heads, kv_heads, dq_ref, dkv_ref, cos_ref, sin_ref, out_ref, sum_ref):
    cos_table = cos_ref[...]
    sin_table = -sin_ref[...]
    sum_ref[...] = jnp.zeros_like(sum_ref)
    for head in range(q_heads + 2 * kv_heads):
        base, shift = window_of(head)
        if head < q_heads:
            values = dq_ref[:, head * LANES : (head + 1) * LANES].astype(F32)
        else:
            at = (head - q_heads) * LANES
            values = dkv_ref[:, at : at + LANES].astype(BF16).astype(F32)
        if head < q_heads + kv_heads:
            values = rotated(values, cos_table, sin_table)
        wide = jnp.concatenate([values, jnp.zeros_like(values)], axis=1)
        if shift:
            wide = pltpu.roll(wide, shift, 1)
        sum_ref[:, base : base + 2 * LANES] += wide
    out_ref[...] = sum_ref[...].astype(BF16)


def pack_heads(dq_wide, dkv, cos_table, sin_table, q_heads, kv_heads, width, rows):
    total = dq_wide.shape[0]
    return pl.pallas_call(
        functools.partial(pack_kernel, q_heads, kv_heads),
        grid=(total // rows,),
        in_specs=[
            pl.BlockSpec((rows, dq_wide.shape[1]), lambda b: (b, 0)),
            pl.BlockSpec((rows, dkv.shape[1]), lambda b: (b, 0)),
            pl.BlockSpec((rows, LANES), lambda b: (b, 0)),
            pl.BlockSpec((rows, LANES), lambda b: (b, 0)),
        ],
        out_specs=pl.BlockSpec((rows, width), lambda b: (b, 0)),
        out_shape=jax.ShapeDtypeStruct((total, width), BF16),
        scratch_shapes=[pltpu.VMEM((rows, width), F32)],
        cost_estimate=pl.CostEstimate(
            flops=10 * total * width, bytes_accessed=7 * total * width, transcendentals=0
        ),
        name="pack_heads",
    )(dq_wide, dkv, cos_table, sin_table)


def fill_bias(seg_q, par_q, pos_q, seg_k, pos_k, bias_ref):
    same = (seg_k == seg_q) | (seg_k == par_q) | (seg_k == 0)
    bias_ref[...] = jnp.where(same & (pos_k <= pos_q), 0.0, NEG)


def probabilities(q_block, keys, bias):
    scores = mm_nt(q_block, keys) * HEAD ** (-0.5) + bias
    top = jnp.max(scores, axis=1, keepdims=True)
    raised = jnp.exp(scores - top)
    return raised * (1.0 / jnp.sum(raised, axis=1, keepdims=True))


def forward_kernel(
    rows, tree_len, block,
    ctx_ref, q_ref, k_ref, v_ref, seg_q, par_q, pos_q, seg_k, pos_k, out_ref, bias_ref,
):
    @pl.when(pl.program_id(1) == 0)
    def _():
        fill_bias(seg_q[0], par_q[0], pos_q[0], seg_k[0], pos_k[0], bias_ref)

    in_trunk = (ctx_ref[0] + 1) * rows <= TRUNK

    def run(keys):
        @pl.loop(0, rows // block)
        def _(step):
            at = pl.ds(pl.multiple_of(step * block, block), block)
            probs = probabilities(q_ref[at, :], k_ref[0, :keys, :], bias_ref[at, :keys])
            out_ref[at, :] = mm(probs.astype(BF16), v_ref[0, :keys, :]).astype(BF16)

    pl.when(in_trunk)(lambda: run(min(TRUNK, tree_len)))
    pl.when(jnp.logical_not(in_trunk))(lambda: run(tree_len))


def backward_kernel(
    rows, tree_len, block, group,
    q_ref, k_ref, v_ref, do_ref, seg_q, par_q, pos_q, seg_k, pos_k,
    dq_ref, dk_ref, dv_ref, bias_ref,
):
    head = pl.program_id(1)

    @pl.when(head == 0)
    def _():
        fill_bias(seg_q[0], par_q[0], pos_q[0], seg_k[0], pos_k[0], bias_ref)

    @pl.when(lax.rem(head, group) == 0)
    def _():
        dk_ref[...] = jnp.zeros_like(dk_ref)
        dv_ref[...] = jnp.zeros_like(dv_ref)

    in_trunk = (lax.axis_index("context") + 1) * rows <= TRUNK
    scale = HEAD ** (-0.5)

    def run(keys):
        @pl.loop(0, rows // block)
        def _(step):
            at = pl.ds(pl.multiple_of(step * block, block), block)
            q_block = q_ref[at, :]
            do_block = do_ref[at, :]
            k_all = k_ref[0, :keys, :]
            probs = probabilities(q_block, k_all, bias_ref[at, :keys])
            dprobs = mm_nt(do_block, v_ref[0, :keys, :])
            delta = jnp.sum(probs * dprobs, axis=1, keepdims=True)
            dscores = (probs * (dprobs - delta)).astype(BF16)
            dq_ref[at, :] = (mm(dscores, k_all) * scale).astype(BF16)
            dk_ref[0, :keys, :] += mm_tn(dscores, q_block) * scale
            dv_ref[0, :keys, :] += mm_tn(probs.astype(BF16), do_block)

    pl.when(in_trunk)(lambda: run(min(TRUNK, tree_len)))
    pl.when(jnp.logical_not(in_trunk))(lambda: run(tree_len))


def attention_specs(rows, tree_len, group, kv_heads):
    def column(b, h, *c):
        return (b, h)

    def whole(b, h, *c):
        return (b, 0, 0)

    return [
        pl.BlockSpec((rows, LANES), column),
        pl.BlockSpec((1, tree_len, LANES), lambda b, h, *c: (b, 0, h // group)),
        pl.BlockSpec((1, tree_len, LANES), lambda b, h, *c: (b, 0, kv_heads + h // group)),
    ], [
        pl.BlockSpec((1, rows, 1), whole),
        pl.BlockSpec((1, rows, 1), whole),
        pl.BlockSpec((1, rows, 1), whole),
        pl.BlockSpec((1, 1, tree_len), whole),
        pl.BlockSpec((1, 1, tree_len), whole),
    ]


def attend_forward(ctx, q_wide, kv_full, ids, q_heads, kv_heads, rows):
    trees, tree_len, _ = kv_full.shape
    group = q_heads // kv_heads
    first, last = attention_specs(rows, tree_len, group, kv_heads)
    block = min(rows, 256)
    work = trees * q_heads * rows * tree_len
    return pl.pallas_call(
        functools.partial(forward_kernel, rows, tree_len, block),
        grid_spec=pltpu.PrefetchScalarGridSpec(
            num_scalar_prefetch=1,
            grid=(trees, q_heads),
            in_specs=first + last,
            out_specs=pl.BlockSpec((rows, LANES), lambda b, h, c: (b, h)),
            scratch_shapes=[pltpu.VMEM((rows, tree_len), F32)],
        ),
        out_shape=jax.ShapeDtypeStruct(q_wide.shape, BF16),
        cost_estimate=pl.CostEstimate(
            flops=4 * LANES * work, bytes_accessed=8 * q_wide.size, transcendentals=work
        ),
        name="attend_forward",
    )(ctx, q_wide, kv_full, kv_full, *ids)


HOP_AXIS = "tensor"


def with_hops(kernel, counts, sides, *refs):
    own_in, own_out, own_scratch = counts
    sends = len(sides)
    ends_at = []
    for size in (own_in, sends, own_out, sends, own_scratch):
        ends_at.append((ends_at[-1] if ends_at else 0) + size)
    ins, sent, outs, received, scratch = (
        refs[low:high] for low, high in zip([0, *ends_at], ends_at)
    )
    send_sem, recv_sem = refs[ends_at[-1] :]
    here = lax.axis_index(HOP_AXIS)
    count = lax.axis_size(HOP_AXIS)
    has_next, has_last = here < count - 1, here > 0

    def copy(number):
        other = here + 1 - 2 * sides[number]
        return pltpu.make_async_remote_copy(
            src_ref=sent[number],
            dst_ref=received[number],
            send_sem=send_sem.at[number],
            recv_sem=recv_sem.at[number],
            device_id={HOP_AXIS: other},
            device_id_type=pl.DeviceIdType.MESH,
        )

    first, last = None, None
    if own_in:
        first, last = jnp.bool_(True), jnp.bool_(True)
        for axis in range(GRID_RANK[kernel]):
            first &= pl.program_id(axis) == 0
            last &= pl.program_id(axis) == pl.num_programs(axis) - 1

    def start():
        barrier = pltpu.get_barrier_semaphore()
        for there, step in ((has_next, 1), (has_last, -1)):

            @pl.when(there)
            def _():
                pl.semaphore_signal(
                    barrier,
                    inc=1,
                    device_id={HOP_AXIS: here + step},
                    device_id_type=pl.DeviceIdType.MESH,
                )

        pl.semaphore_wait(barrier, has_next.astype(jnp.int32) + has_last.astype(jnp.int32))
        for number, side in enumerate(sides):
            pl.when((has_next, has_last)[side])(lambda number=number: copy(number).start())

    def finish():
        for number, side in enumerate(sides):
            pl.when((has_next, has_last)[side])(lambda number=number: copy(number).wait_send())
            pl.when((has_last, has_next)[side])(lambda number=number: copy(number).wait_recv())

    if own_in:
        pl.when(first)(start)
        kernel(*ins, *outs, *scratch)
        pl.when(last)(finish)
    else:
        start()
        finish()


GRID_RANK = {}


def hop_call(kernel, sends, *args, grid=(), in_specs=(), out_specs=(), out_shape=(),
             scratch_shapes=(), number=0, cost_estimate=None):
    sides = tuple(side for _, side in sends)
    values = [value for value, _ in sends]
    anywhere = pl.BlockSpec(memory_space=pl.ANY)
    if kernel is not None:
        GRID_RANK[kernel] = len(grid)
    counts = (len(args), len(out_shape), len(scratch_shapes))
    results = pl.pallas_call(
        functools.partial(with_hops, kernel, counts, sides),
        grid=grid,
        in_specs=[*in_specs, *[anywhere] * len(values)],
        out_specs=[*out_specs, *[anywhere] * len(values)],
        out_shape=[*out_shape, *[jax.ShapeDtypeStruct(v.shape, v.dtype) for v in values]],
        scratch_shapes=[
            *scratch_shapes,
            pltpu.SemaphoreType.DMA((len(values),)),
            pltpu.SemaphoreType.DMA((len(values),)),
        ],
        compiler_params=pltpu.CompilerParams(
            collective_id=4 * number + len(values) // 2, has_side_effects=True
        ),
        cost_estimate=cost_estimate,
    )(*args, *values)
    return results[: len(out_shape)], results[len(out_shape) :]


def attend_backward(q_wide, kv_full, do_wide, ids, q_heads, kv_heads, rows, sends):
    trees, tree_len, _ = kv_full.shape
    group = q_heads // kv_heads
    first, last = attention_specs(rows, tree_len, group, kv_heads)
    block = min(rows, 256)
    work = trees * q_heads * rows * tree_len
    grad_spec = pl.BlockSpec((1, tree_len, LANES), lambda b, h: (b, 0, h // group))
    grad_shape = jax.ShapeDtypeStruct((trees, tree_len, kv_heads * LANES), F32)
    return hop_call(
        functools.partial(backward_kernel, rows, tree_len, block, group),
        sends,
        *(q_wide, kv_full, kv_full, do_wide, *ids),
        grid=(trees, q_heads),
        in_specs=first + [first[0]] + last,
        out_specs=[first[0], grad_spec, grad_spec],
        out_shape=[jax.ShapeDtypeStruct(q_wide.shape, BF16), grad_shape, grad_shape],
        scratch_shapes=[pltpu.VMEM((rows, tree_len), F32)],
        cost_estimate=pl.CostEstimate(
            flops=10 * LANES * work, bytes_accessed=12 * q_wide.size, transcendentals=work
        ),
        number=2,
    )


def feed_back_kernel(dgate_up, mixed, gate_up_w, down_w, dn2_ref, out_ref):
    dn2_ref[...] = mm_nt(dgate_up[...], gate_up_w[...]).astype(BF16)
    out_ref[...] = mm_nt(mixed[...], down_w[...]).astype(BF16)


def feed_back(dgate_up, mixed, gate_up_w, down_w, sends):
    rows, hidden = mixed.shape
    width = down_w.shape[0]
    tile = width // 5
    result = pl.BlockSpec((rows, tile), lambda i: (0, i))
    shape = jax.ShapeDtypeStruct((rows, width), BF16)
    return hop_call(
        feed_back_kernel,
        sends,
        *(dgate_up, mixed, gate_up_w, down_w),
        grid=(width // tile,),
        in_specs=[
            pl.BlockSpec((rows, 2 * hidden), lambda i: (0, 0)),
            pl.BlockSpec((rows, hidden), lambda i: (0, 0)),
            pl.BlockSpec((tile, 2 * hidden), lambda i: (i, 0)),
            pl.BlockSpec((tile, hidden), lambda i: (i, 0)),
        ],
        out_specs=[result] * 2,
        out_shape=[shape] * 2,
        cost_estimate=pl.CostEstimate(
            flops=6 * rows * hidden * width,
            bytes_accessed=6 * hidden * (rows + width) + 4 * rows * width,
            transcendentals=0,
        ),
        number=1,
    )


def piece(values, index, size):
    return lax.dynamic_slice_in_dim(values, index * size, size, 1)


class LineSum:
    def __init__(self, values, size, axis):
        self.axis = axis
        self.count = lax.axis_size(axis)
        self.pieces = [values[:, i * size : (i + 1) * size] for i in range(self.count)]
        self.step = 0
        self.got = None
        here = lax.axis_index(axis)
        self.valid = (here > 0, here < self.count - 1)

    def sends(self):
        self.step += 1
        step, count = self.step, self.count
        rights = [(i, i + 1) for i in range(step)]
        lefts = [(count - 1 - i, count - 2 - i) for i in range(step)]
        found = []
        for side, slot, pairs in ((0, step, rights), (1, count - step, lefts)):
            value = self.pieces[slot]
            if self.got is not None:
                value = (value.astype(F32) + self.arrived(side)).astype(BF16)
            found.append((value, self.axis, pairs, side))
        return found

    def arrived(self, side):
        return jnp.where(self.valid[side], self.got[side].astype(F32), 0.0)

    def loose(self):
        return self.step == 1 and self.count > 2

    def receive(self, results):
        self.got = results

    def result(self):
        assert self.step == self.count - 1
        total = self.pieces[0].astype(F32)
        for side in (0, 1) if self.got else ():
            total = total + self.arrived(side)
        return total


class LineGather:
    def __init__(self, own, axis):
        self.own, self.axis = own, axis
        self.count = lax.axis_size(axis)
        self.lefts, self.rights = [own], [own]

    def sends(self):
        step, count = len(self.lefts), self.count
        return [
            (self.lefts[-1], self.axis, [(i, i + 1) for i in range(step - 1, count - 1)], 0),
            (self.rights[-1], self.axis, [(i, i - 1) for i in range(count - step, 0, -1)], 1),
        ]

    def loose(self):
        return len(self.lefts) == self.count - 1 and self.count > 2

    def receive(self, results):
        self.lefts.append(results[0])
        self.rights.append(results[1])

    def result(self):
        count = self.count
        here = lax.axis_index(self.axis)
        assert len(self.lefts) == count
        others = [
            jnp.where(here >= step, self.lefts[step], self.rights[count - step])
            for step in range(1, count)
        ]
        return jnp.concatenate([self.own, *others], axis=1)


class EarlierGather:
    def __init__(self, own, axis):
        self.own, self.axis = own, axis
        self.count = lax.axis_size(axis)

    def sends(self):
        count = self.count
        return [
            (self.own, self.axis, [(i, i + step) for i in range(count - step)], None)
            for step in range(1, count)
        ]

    def receive(self, results):
        self.others = results

    def result(self):
        count, own = self.count, self.own
        here = lax.axis_index(self.axis)
        trees, rows, width = own.shape
        result = jnp.zeros((trees, count * rows, width), own.dtype)
        result = lax.dynamic_update_slice_in_dim(result, own, here * rows, 1)
        for step, other in enumerate(self.others, 1):
            slot = lax.rem(here - step + count, count)
            result = lax.dynamic_update_slice_in_dim(result, other, slot * rows, 1)
        return result


class EarlierReturn:
    def __init__(self, full, axis):
        self.full, self.axis = full, axis
        self.count = lax.axis_size(axis)
        self.rows = full.shape[1] // self.count

    def sends(self):
        count = self.count
        here = lax.axis_index(self.axis)
        found = []
        for step in range(1, count):
            slot = lax.rem(here - step + count, count)
            value = piece(self.full, slot, self.rows).astype(BF16)
            found.append((value, self.axis, [(i + step, i) for i in range(count - step)], None))
        return found

    def receive(self, results):
        self.others = results

    def result(self):
        total = piece(self.full, lax.axis_index(self.axis), self.rows)
        for other in self.others:
            total = total + other.astype(F32)
        return total


def ends(pairs, which):
    return {pair[which] for pair in pairs}


def disjoint(left, right):
    return not any(ends(left, which) & ends(right, which) for which in (0, 1))


def joined(sends, loose):
    groups = []
    for number, (value, axis, pairs, side) in enumerate(sends):
        for group in groups:
            if side is None or group.axis != axis or not disjoint(pairs, group.pairs):
                continue
            if group.side != side and not loose:
                continue
            here = lax.axis_index(axis)
            mine = functools.reduce(jnp.logical_or, [here == i for i in sorted(ends(pairs, 0))])
            group.value = jnp.where(mine, value, group.value)
            group.pairs = group.pairs + pairs
            group.members.append(number)
            break
        else:
            groups.append(
                SimpleNamespace(value=value, axis=axis, pairs=pairs, side=side, members=[number])
            )
    return groups


class Stages:
    def __init__(self):
        self.token = ()
        self.number = 0

    def wait_for(self, *values):
        self.token += values

    def __call__(self, transfers, compute=None, inputs=(), fused=False):
        self.number += 1
        kept = []
        for t in transfers:
            if t.count > 1:
                kept.append(t)
            else:
                t.receive([])
        transfers = kept
        sends = [t.sends() for t in transfers]
        lines = [t for t in transfers if hasattr(t, "loose")]
        loose = len(lines) == 1 and lines[0].loose() and not fused
        groups = joined([send for of_one in sends for send in of_one], loose)
        values = [group.value for group in groups]
        tied = lax.optimization_barrier((*values, *inputs, *self.token))
        results = {}
        token = []
        by_kernel = []
        for value, group in zip(tied, groups):
            if fused and group.side is not None:
                by_kernel.append((value, group))
                continue
            other = lax.ppermute(value, group.axis, group.pairs)
            token.append(other)
            results.update({number: other for number in group.members})
        given = tied[len(groups) : len(groups) + len(inputs)]
        if by_kernel:
            line_sends = [(value, group.side) for value, group in by_kernel]
            if compute is None:
                outs, others = hop_call(None, line_sends)
            else:
                outs, others = compute(*given, line_sends)
            for other, (_, group) in zip(others, by_kernel):
                token.append(other)
                results.update({number: other for number in group.members})
        else:
            outs = compute(*given) if compute else ()
        at = 0
        for transfer, of_one in zip(transfers, sends):
            transfer.receive([results[at + i] for i in range(len(of_one))])
            at += len(of_one)
        self.token = (*token, *outs)
        return outs


def turned(values, dim, axis):
    count = lax.axis_size(axis)
    here = lax.axis_index(axis)
    size = values.shape[dim] // count
    return jnp.concatenate(
        [
            lax.dynamic_slice_in_dim(
                values, lax.rem(here - i + count, count) * size, size, dim
            )
            for i in range(count)
        ],
        axis=dim,
    )


class SmallSum:
    def __init__(self, values, axis):
        self.values, self.axis = values, axis
        self.count = lax.axis_size(axis)

    def sends(self):
        count = self.count
        return [
            (self.values, self.axis, [(i, (i + step) % count) for i in range(count)], None)
            for step in range(1, count)
        ]

    def receive(self, results):
        self.others = results

    def result(self):
        return sum(self.others, self.values)


def norm_back(grad, values, gain):
    root = lax.rsqrt(jnp.mean(values * values, axis=-1, keepdims=True) + EPS)
    weighted = grad * gain
    mean = jnp.mean(weighted * values, axis=-1, keepdims=True)
    return root * weighted - values * (root * root * root) * mean


def on_device(
    tokens, norm_one, q_weight, k_weight, v_weight, o_weight, norm_two,
    gate_weight, up_weight, down_weight, segment_ids, parent_ids, path_pos, cotangent,
):
    ctx = lax.axis_index("context")
    ctx_count = lax.axis_size("context")
    ten_count = lax.axis_size(HOP_AXIS)
    tree_count, rows, width = tokens.shape
    share = rows // ten_count
    trees = tree_count // MICRO
    flat = trees * rows
    part, q_width = q_weight.shape
    kv_width = k_weight.shape[1]
    q_heads = q_width // HEAD
    kv_heads = kv_width // HEAD
    used = q_width + 2 * kv_width
    packed_width = round_up(used + 2, LANES)

    attention_block = jnp.concatenate(
        [
            q_weight, k_weight, v_weight, norm_one[:, None], norm_two[:, None],
            jnp.zeros((part, packed_width - used - 2), BF16),
        ],
        axis=1,
    )
    attention_full = lax.all_gather(attention_block, WEIGHT_AXES, axis=0, tiled=True)
    o_full = lax.all_gather(o_weight.T, WEIGHT_AXES, axis=0, tiled=True)
    hidden = gate_weight.shape[1]
    wide = round_up(hidden, LANES)

    def widened(values):
        return jnp.pad(values, ((0, 0), (0, wide - hidden)))

    down_full = lax.all_gather(widened(down_weight.T), WEIGHT_AXES, axis=0, tiled=True)
    gate_up_block = jnp.concatenate([widened(gate_weight), widened(up_weight)], axis=1)
    gate_up_full = lax.all_gather(gate_up_block, WEIGHT_AXES, axis=0, tiled=True)
    gain_one = attention_full[:, used].astype(F32)
    gain_two = attention_full[:, used + 1].astype(F32)

    lane = np.arange(q_heads * LANES)
    column = np.arange(q_width)
    select = jnp.asarray(
        (lane[:, None] // LANES == column[None, :] // HEAD)
        & (lane[:, None] % LANES == column[None, :] % HEAD),
        BF16,
    )
    frequency = THETA ** (-(jnp.arange(HALF, dtype=F32) * 2.0 / HEAD))
    pad = jnp.zeros((flat, LANES - HEAD), F32)
    ctx_ref = jnp.reshape(ctx, (1,)).astype(jnp.int32)

    tokens = turned(tokens, 1, HOP_AXIS)
    cotangent = turned(cotangent, 1, HOP_AXIS)
    segment_ids, parent_ids, path_pos = [
        turned(ids.reshape(-1, ctx_count, rows), 2, HOP_AXIS).reshape(ids.shape)
        for ids in (segment_ids, parent_ids, path_pos)
    ]
    state = []
    for micro in range(MICRO):
        pick = slice(micro * trees, (micro + 1) * trees)
        m = SimpleNamespace()
        state.append(m)
        m.number = micro
        m.x = tokens[pick]
        m.dy = cotangent[pick]
        seg, par, pos = segment_ids[pick], parent_ids[pick], path_pos[pick]

        def here(ids):
            return lax.dynamic_slice_in_dim(ids, ctx * rows, rows, 1)

        m.ids = (
            here(seg)[:, :, None], here(par)[:, :, None], here(pos)[:, :, None],
            seg[:, None, :], pos[:, None, :],
        )
        angles = here(pos).reshape(flat).astype(F32)[:, None] * frequency[None, :]
        cosine, sine = jnp.cos(angles), jnp.sin(angles)
        m.cos = jnp.concatenate([cosine, cosine, pad], axis=1)
        m.sin = jnp.concatenate([-sine, sine, pad], axis=1)
        x = m.x.reshape(flat, width).astype(F32)
        m.root_one = lax.rsqrt(jnp.mean(x * x, axis=-1, keepdims=True) + EPS)
        m.x_here = m.x[:, :share].astype(F32)
        m.dy_here = m.dy[:, :share].astype(F32)

    def together(*parts):
        return jnp.concatenate([part.reshape(flat, -1) for part in parts], axis=0)

    def shaped(product):
        return product.reshape(trees, rows, width)

    x_all = tokens.reshape(-1, width).astype(F32)
    root_all = jnp.concatenate([m.root_one for m in state], axis=0)
    normed_all = (x_all * root_all * gain_one).astype(BF16)
    stage = Stages()
    a, b = state

    def project(m):
        def run(root):
            at = m.number * flat
            packed = mm(normed_all[at : at + flat], attention_full)
            m.q, kv = split_heads(packed, m.cos, m.sin, q_heads, kv_heads, rows)
            m.kv = EarlierGather(kv.reshape(trees, rows, -1), "context")
            return (m.q,)

        return run

    def attend(m):
        def run(q):
            m.kv_full = m.kv.result()
            wide = attend_forward(ctx_ref, q, m.kv_full, m.ids, q_heads, kv_heads, rows)
            m.attended = mm(wide, select).astype(BF16)
            product = mm_nt(m.attended, o_full).astype(BF16)
            m.sum1 = LineSum(shaped(product), share, HOP_AXIS)
            return (product,)

        return run

    def mixed_back(m):
        def run(dy):
            m.dmixed = row_major(mm(dy.reshape(flat, width), down_full))
            return (m.dmixed,)

        return run

    def norm_two_of(m):
        middle = m.x_here + m.sum1.result()
        root = lax.rsqrt(jnp.mean(middle * middle, axis=-1, keepdims=True) + EPS)
        m.middle, m.root_two = middle, root
        m.gather1 = LineGather((middle * root * gain_two).astype(BF16), HOP_AXIS)

    def feed_forward(m):
        def run(normed_two):
            m.normed_two = normed_two
            both = row_major(mm(normed_two, gate_up_full))
            dmixed, both = lax.optimization_barrier((m.dmixed, both))
            gate, up = both[:, :wide], both[:, wide:]
            sigmoid = 1.0 / (1.0 + jnp.exp(-gate))
            silu = gate * sigmoid
            slope = sigmoid * (1.0 + gate * (1.0 - sigmoid))
            m.mixed = (silu * up).astype(BF16)
            dgate = (dmixed * up * slope).astype(BF16)
            dup = (dmixed * silu).astype(BF16)
            m.dgate_up = jnp.concatenate([dgate, dup], axis=1)
            return (m.mixed, m.dgate_up)

        return run

    def back_of(m):
        def run(dgate_up, sends):
            (product, out), others = feed_back(
                dgate_up, m.mixed, gate_up_full, down_full, sends
            )
            m.sum3 = LineSum(shaped(product), share, HOP_AXIS)
            m.out_part = shaped(out)
            return (product, out), others

        return run

    def norm_two_back(m):
        middle, dn2 = m.middle, m.sum3.result()
        m.gain_two_grad = jnp.sum(dn2 * middle * m.root_two, axis=(0, 1))
        m.dmiddle = m.dy_here + norm_back(dn2, middle, gain_two)
        m.gather2 = LineGather(m.dmiddle.astype(BF16), HOP_AXIS)

    def attended_back(m):
        def run(dmb):
            m.dmb = dmb
            dattended = mm(dmb, o_full).astype(BF16)
            m.do = mm_nt(dattended, select).astype(BF16)
            return (m.do,)

        return run

    def attend_back(m):
        def run(do_wide, sends):
            (m.dq, dk, dv), others = attend_backward(
                m.q, m.kv_full, do_wide, m.ids, q_heads, kv_heads, rows, sends
            )
            m.dkv = EarlierReturn(jnp.concatenate([dk, dv], axis=2), "context")
            return (m.dq,), others

        return run

    def norm_one_back(m):
        def run(dq):
            dkv = m.dkv.result().reshape(flat, -1)
            m.dqkv = pack_heads(
                dq, dkv, m.cos, m.sin, q_heads, kv_heads, packed_width, rows
            )
            dn1 = mm_nt(m.dqkv, attention_full).astype(BF16)
            x = m.x.reshape(flat, width).astype(F32)
            m.gain_one_grad = jnp.sum(after(dn1).astype(F32) * x * m.root_one, axis=0)
            m.sum4 = LineSum(shaped(dn1), share, HOP_AXIS)
            return (dn1,)

        return run

    class WeightGrad:
        def __init__(self, right_of):
            self.right_of = right_of

        def __call__(self, left):
            self.grad = row_major(mm_tn(left, self.right_of()).astype(BF16))
            return (self.grad,)

        def scattered(self):
            return lax.psum_scatter(self.grad, WEIGHT_AXES, scatter_dimension=0, tiled=True)

    def gathered(transfer):
        return transfer.result().reshape(flat, width)

    stage([], project(a), [a.root_one])
    stage([a.kv], project(b), [b.root_one])
    stage([b.kv], attend(a), [a.q])
    stage([a.sum1], attend(b), [b.q])
    stage([a.sum1], fused=True)
    stage([a.sum1], mixed_back(a), [a.dy])
    norm_two_of(a)
    stage([a.gather1], mixed_back(b), [b.dy])
    stage([a.gather1, b.sum1], fused=True)
    stage([a.gather1, b.sum1], fused=True)
    stage([b.sum1], fused=True)
    norm_two_of(b)
    stage([b.gather1], feed_forward(a), [gathered(a.gather1)])
    stage([b.gather1], back_of(a), [a.dgate_up], fused=True)
    stage([b.gather1, a.sum3], fused=True)
    stage([a.sum3], feed_forward(b), [gathered(b.gather1)])
    dy_all = cotangent.reshape(-1, width)
    mixed_all = together(a.mixed, b.mixed)
    down_grad = WeightGrad(lambda: mixed_all)
    stage([a.sum3], down_grad, [dy_all])
    down_grad = down_grad.scattered()
    norm_two_back(a)
    a.sum2 = LineSum(a.out_part, share, HOP_AXIS)
    stage([a.gather2, a.sum2], back_of(b), [b.dgate_up], fused=True)
    b.sum2 = LineSum(b.out_part, share, HOP_AXIS)
    gate_up_grad = WeightGrad(lambda: together(a.dgate_up, b.dgate_up))
    stage([a.gather2, b.sum3], gate_up_grad, [together(a.normed_two, b.normed_two)])
    gate_up_grad = gate_up_grad.scattered()
    stage([a.gather2, b.sum3], fused=True)
    stage([b.sum3], attended_back(a), [gathered(a.gather2)])
    norm_two_back(b)
    stage([b.gather2], attend_back(a), [a.do], fused=True)
    stage([b.gather2, b.sum2, a.dkv], fused=True)
    stage([b.gather2, a.sum2], norm_one_back(a), [a.dq])
    stage.wait_for(down_grad)
    stage([a.sum4], attended_back(b), [gathered(b.gather2)])
    stage([a.sum4, a.sum2], attend_back(b), [b.do], fused=True)
    stage.wait_for(gate_up_grad)
    o_grad = WeightGrad(lambda: together(a.attended, b.attended))
    stage([a.sum4, b.dkv], o_grad, [together(a.dmb, b.dmb)])
    o_grad = o_grad.scattered()
    stage([b.sum2], norm_one_back(b), [b.dq])
    gains = jnp.stack([a.gain_one_grad + b.gain_one_grad, a.gain_two_grad + b.gain_two_grad])
    gains = SmallSum(gains, HOP_AXIS)
    attention_grad = WeightGrad(lambda: together(a.dqkv, b.dqkv))
    stage([b.sum4, b.sum2, gains], attention_grad, [normed_all])
    attention_grad = attention_grad.scattered().astype(F32)
    gains = SmallSum(gains.result(), "context")
    stage([b.sum4, gains], fused=True)
    stage.wait_for(o_grad)
    gains = SmallSum(gains.result(), "fsdp")
    stage([b.sum4, gains], fused=True)
    block = lax.axis_index("fsdp") * ctx_count + ctx
    gains = lax.dynamic_slice_in_dim(gains.result(), block * part, part, 1)
    for m in state:
        m.out_sum = m.sum2.result()
    for m in state:
        middle, out_sum = lax.optimization_barrier((m.middle, m.out_sum))
        m.out = (middle + out_sum.astype(F32)).astype(BF16)
        m.dx = (m.dmiddle + norm_back(m.sum4.result(), m.x_here, gain_one)).astype(BF16)

    return (
        jnp.concatenate([m.out for m in state], axis=0),
        jnp.concatenate([m.dx for m in state], axis=0),
        gains[0],
        attention_grad[:, :q_width],
        attention_grad[:, q_width : q_width + kv_width],
        attention_grad[:, q_width + kv_width : used],
        o_grad.T.astype(F32),
        gains[1],
        gate_up_grad[:, :hidden].astype(F32),
        gate_up_grad[:, wide : wide + hidden].astype(F32),
        down_grad[:, :hidden].T.astype(F32),
    )


def solution(mesh):
    weights = WEIGHT_AXES
    return jax.shard_map(
        on_device,
        mesh=mesh,
        in_specs=(
            P("fsdp", "context", None),
            P(weights),
            P(weights, "tensor"),
            P(weights, "tensor"),
            P(weights, "tensor"),
            P("tensor", weights),
            P(weights),
            P(weights, "tensor"),
            P(weights, "tensor"),
            P("tensor", weights),
            P("fsdp", None),
            P("fsdp", None),
            P("fsdp", None),
            P("fsdp", "context", None),
        ),
        out_specs=(
            P("fsdp", ("context", "tensor"), None),
            P("fsdp", ("context", "tensor"), None),
            P(weights),
            P(weights, "tensor"),
            P(weights, "tensor"),
            P(weights, "tensor"),
            P("tensor", weights),
            P(weights),
            P(weights, "tensor"),
            P(weights, "tensor"),
            P("tensor", weights),
        ),
        check_vma=False,
    )
```

```python
import functools
from types import SimpleNamespace

import jax
import jax.numpy as jnp
import numpy as np
from jax import lax
from jax.experimental import pallas as pl
from jax.experimental.pallas import tpu as pltpu
from jax.experimental.layout import Layout, with_layout_constraint
from jax.sharding import PartitionSpec as P


HEAD = 80
HALF = HEAD // 2
LANES = 128
MICRO = 2
EPS = 1e-05
THETA = 10000.0
NEG = -1000000000.0
TRUNK = 512
WEIGHT_AXES = ("fsdp", "context")
BF16 = jnp.bfloat16
F32 = jnp.float32


def row_major(value):
    return with_layout_constraint(value, Layout(major_to_minor=(0, 1)))


def round_up(value, unit):
    return (value + unit - 1) // unit * unit


def mm(left, right):
    return lax.dot_general(left, right, (((1,), (0,)), ((), ())), preferred_element_type=F32)


def mm_nt(left, right):
    return lax.dot_general(left, right, (((1,), (1,)), ((), ())), preferred_element_type=F32)


def mm_tn(left, right):
    return lax.dot_general(left, right, (((0,), (0,)), ((), ())), preferred_element_type=F32)


def rotated(values, cos_table, sin_table):
    lane = lax.broadcasted_iota(jnp.int32, values.shape, 1)
    swapped = jnp.where(
        lane < HALF, pltpu.roll(values, LANES - HALF, 1), pltpu.roll(values, HALF, 1)
    )
    return values * cos_table + swapped * sin_table


def window_of(head):
    start = head * HEAD
    base = start // LANES * LANES
    return base, start - base


def split_kernel(q_heads, kv_heads, x_ref, cos_ref, sin_ref, q_ref, kv_ref):
    cos_table = cos_ref[...]
    sin_table = sin_ref[...]
    for head in range(q_heads + 2 * kv_heads):
        base, shift = window_of(head)
        window = x_ref[:, base : base + 2 * LANES]
        if shift:
            window = pltpu.roll(window, 2 * LANES - shift, 1)
        values = window[:, :LANES]
        if head < q_heads + kv_heads:
            result = rotated(values, cos_table, sin_table)
        else:
            lane = lax.broadcasted_iota(jnp.int32, values.shape, 1)
            result = jnp.where(lane < HEAD, values, 0.0)
        result = result.astype(BF16)
        if head < q_heads:
            q_ref[:, head * LANES : (head + 1) * LANES] = result
        else:
            at = (head - q_heads) * LANES
            kv_ref[:, at : at + LANES] = result


def split_heads(packed, cos_table, sin_table, q_heads, kv_heads, rows):
    total, width = packed.shape
    q_wide = q_heads * LANES
    kv_wide = 2 * kv_heads * LANES
    return pl.pallas_call(
        functools.partial(split_kernel, q_heads, kv_heads),
        grid=(total // rows,),
        in_specs=[
            pl.BlockSpec((rows, width), lambda b: (b, 0)),
            pl.BlockSpec((rows, LANES), lambda b: (b, 0)),
            pl.BlockSpec((rows, LANES), lambda b: (b, 0)),
        ],
        out_specs=[
            pl.BlockSpec((rows, q_wide), lambda b: (b, 0)),
            pl.BlockSpec((rows, kv_wide), lambda b: (b, 0)),
        ],
        out_shape=[
            jax.ShapeDtypeStruct((total, q_wide), BF16),
            jax.ShapeDtypeStruct((total, kv_wide), BF16),
        ],
        cost_estimate=pl.CostEstimate(
            flops=10 * total * width, bytes_accessed=7 * total * width, transcendentals=0
        ),
        name="split_heads",
    )(packed, cos_table, sin_table)


def fill_bias(seg_q, par_q, pos_q, seg_k, pos_k, bias_ref):
    same = (seg_k == seg_q) | (seg_k == par_q) | (seg_k == 0)
    bias_ref[...] = jnp.where(same & (pos_k <= pos_q), 0.0, NEG)


def probabilities(q_block, keys, bias):
    scores = mm_nt(q_block, keys) * HEAD ** (-0.5) + bias
    top = jnp.max(scores, axis=1, keepdims=True)
    raised = jnp.exp(scores - top)
    return raised * (1.0 / jnp.sum(raised, axis=1, keepdims=True))


def forward_kernel(
    rows, tree_len, block,
    ctx_ref, q_ref, k_ref, v_ref, seg_q, par_q, pos_q, seg_k, pos_k, out_ref, bias_ref,
):
    @pl.when(pl.program_id(1) == 0)
    def _():
        fill_bias(seg_q[0], par_q[0], pos_q[0], seg_k[0], pos_k[0], bias_ref)

    in_trunk = (ctx_ref[0] + 1) * rows <= TRUNK

    def run(keys):
        @pl.loop(0, rows // block)
        def _(step):
            at = pl.ds(pl.multiple_of(step * block, block), block)
            probs = probabilities(q_ref[at, :], k_ref[0, :keys, :], bias_ref[at, :keys])
            out_ref[at, :] = mm(probs.astype(BF16), v_ref[0, :keys, :]).astype(BF16)

    pl.when(in_trunk)(lambda: run(min(TRUNK, tree_len)))
    pl.when(jnp.logical_not(in_trunk))(lambda: run(tree_len))


def backward_kernel(
    rows, tree_len, block, group,
    q_ref, k_ref, v_ref, do_ref, seg_q, par_q, pos_q, seg_k, pos_k,
    dq_ref, dk_ref, dv_ref, bias_ref,
):
    head = pl.program_id(1)

    @pl.when(head == 0)
    def _():
        fill_bias(seg_q[0], par_q[0], pos_q[0], seg_k[0], pos_k[0], bias_ref)

    @pl.when(lax.rem(head, group) == 0)
    def _():
        dk_ref[...] = jnp.zeros_like(dk_ref)
        dv_ref[...] = jnp.zeros_like(dv_ref)

    in_trunk = (lax.axis_index("context") + 1) * rows <= TRUNK
    scale = HEAD ** (-0.5)

    def run(keys):
        @pl.loop(0, rows // block)
        def _(step):
            at = pl.ds(pl.multiple_of(step * block, block), block)
            q_block = q_ref[at, :]
            do_block = do_ref[at, :]
            k_all = k_ref[0, :keys, :]
            probs = probabilities(q_block, k_all, bias_ref[at, :keys])
            dprobs = mm_nt(do_block, v_ref[0, :keys, :])
            delta = jnp.sum(probs * dprobs, axis=1, keepdims=True)
            dscores = (probs * (dprobs - delta)).astype(BF16)
            dq_ref[at, :] = (mm(dscores, k_all) * scale).astype(BF16)
            dk_ref[0, :keys, :] += mm_tn(dscores, q_block) * scale
            dv_ref[0, :keys, :] += mm_tn(probs.astype(BF16), do_block)

    pl.when(in_trunk)(lambda: run(min(TRUNK, tree_len)))
    pl.when(jnp.logical_not(in_trunk))(lambda: run(tree_len))


def attention_specs(rows, tree_len, group, kv_heads):
    def column(b, h, *c):
        return (b, h)

    def whole(b, h, *c):
        return (b, 0, 0)

    return [
        pl.BlockSpec((rows, LANES), column),
        pl.BlockSpec((1, tree_len, LANES), lambda b, h, *c: (b, 0, h // group)),
        pl.BlockSpec((1, tree_len, LANES), lambda b, h, *c: (b, 0, kv_heads + h // group)),
    ], [
        pl.BlockSpec((1, rows, 1), whole),
        pl.BlockSpec((1, rows, 1), whole),
        pl.BlockSpec((1, rows, 1), whole),
        pl.BlockSpec((1, 1, tree_len), whole),
        pl.BlockSpec((1, 1, tree_len), whole),
    ]


def attend_forward(ctx, q_wide, kv_full, ids, q_heads, kv_heads, rows):
    trees, tree_len, _ = kv_full.shape
    group = q_heads // kv_heads
    first, last = attention_specs(rows, tree_len, group, kv_heads)
    block = min(rows, 256)
    work = trees * q_heads * rows * tree_len
    return pl.pallas_call(
        functools.partial(forward_kernel, rows, tree_len, block),
        grid_spec=pltpu.PrefetchScalarGridSpec(
            num_scalar_prefetch=1,
            grid=(trees, q_heads),
            in_specs=first + last,
            out_specs=pl.BlockSpec((rows, LANES), lambda b, h, c: (b, h)),
            scratch_shapes=[pltpu.VMEM((rows, tree_len), F32)],
        ),
        out_shape=jax.ShapeDtypeStruct(q_wide.shape, BF16),
        cost_estimate=pl.CostEstimate(
            flops=4 * LANES * work, bytes_accessed=8 * q_wide.size, transcendentals=work
        ),
        name="attend_forward",
    )(ctx, q_wide, kv_full, kv_full, *ids)


HOP_AXIS = "tensor"


def with_hops(kernel, counts, sides, *refs):
    own_in, own_out, own_scratch = counts
    sends = len(sides)
    ends_at = []
    for size in (own_in, sends, own_out, sends, own_scratch):
        ends_at.append((ends_at[-1] if ends_at else 0) + size)
    ins, sent, outs, received, scratch = (
        refs[low:high] for low, high in zip([0, *ends_at], ends_at)
    )
    send_sem, recv_sem = refs[ends_at[-1] :]
    here = lax.axis_index(HOP_AXIS)
    count = lax.axis_size(HOP_AXIS)
    has_next, has_last = here < count - 1, here > 0

    def copy(number):
        other = here + 1 - 2 * sides[number]
        return pltpu.make_async_remote_copy(
            src_ref=sent[number],
            dst_ref=received[number],
            send_sem=send_sem.at[number],
            recv_sem=recv_sem.at[number],
            device_id={HOP_AXIS: other},
            device_id_type=pl.DeviceIdType.MESH,
        )

    first, last = None, None
    if own_in:
        first, last = jnp.bool_(True), jnp.bool_(True)
        for axis in range(GRID_RANK[kernel]):
            first &= pl.program_id(axis) == 0
            last &= pl.program_id(axis) == pl.num_programs(axis) - 1

    def start():
        barrier = pltpu.get_barrier_semaphore()
        for there, step in ((has_next, 1), (has_last, -1)):

            @pl.when(there)
            def _():
                pl.semaphore_signal(
                    barrier,
                    inc=1,
                    device_id={HOP_AXIS: here + step},
                    device_id_type=pl.DeviceIdType.MESH,
                )

        pl.semaphore_wait(barrier, has_next.astype(jnp.int32) + has_last.astype(jnp.int32))
        for number, side in enumerate(sides):
            pl.when((has_next, has_last)[side])(lambda number=number: copy(number).start())

    def finish():
        for number, side in enumerate(sides):
            pl.when((has_next, has_last)[side])(lambda number=number: copy(number).wait_send())
            pl.when((has_last, has_next)[side])(lambda number=number: copy(number).wait_recv())

    if own_in:
        pl.when(first)(start)
        kernel(*ins, *outs, *scratch)
        pl.when(last)(finish)
    else:
        start()
        finish()


GRID_RANK = {}


def hop_call(kernel, sends, *args, grid=(), in_specs=(), out_specs=(), out_shape=(),
             scratch_shapes=(), number=0, cost_estimate=None):
    sides = tuple(side for _, side in sends)
    values = [value for value, _ in sends]
    anywhere = pl.BlockSpec(memory_space=pl.ANY)
    if kernel is not None:
        GRID_RANK[kernel] = len(grid)
    counts = (len(args), len(out_shape), len(scratch_shapes))
    results = pl.pallas_call(
        functools.partial(with_hops, kernel, counts, sides),
        grid=grid,
        in_specs=[*in_specs, *[anywhere] * len(values)],
        out_specs=[*out_specs, *[anywhere] * len(values)],
        out_shape=[*out_shape, *[jax.ShapeDtypeStruct(v.shape, v.dtype) for v in values]],
        scratch_shapes=[
            *scratch_shapes,
            pltpu.SemaphoreType.DMA((len(values),)),
            pltpu.SemaphoreType.DMA((len(values),)),
        ],
        compiler_params=pltpu.CompilerParams(
            collective_id=4 * number + len(values) // 2, has_side_effects=True
        ),
        cost_estimate=cost_estimate,
    )(*args, *values)
    return results[: len(out_shape)], results[len(out_shape) :]


def attend_backward(q_wide, kv_full, do_wide, ids, q_heads, kv_heads, rows, sends):
    trees, tree_len, _ = kv_full.shape
    group = q_heads // kv_heads
    first, last = attention_specs(rows, tree_len, group, kv_heads)
    block = min(rows, 256)
    work = trees * q_heads * rows * tree_len
    grad_spec = pl.BlockSpec((1, tree_len, LANES), lambda b, h: (b, 0, h // group))
    grad_shape = jax.ShapeDtypeStruct((trees, tree_len, kv_heads * LANES), F32)
    return hop_call(
        functools.partial(backward_kernel, rows, tree_len, block, group),
        sends,
        *(q_wide, kv_full, kv_full, do_wide, *ids),
        grid=(trees, q_heads),
        in_specs=first + [first[0]] + last,
        out_specs=[first[0], grad_spec, grad_spec],
        out_shape=[jax.ShapeDtypeStruct(q_wide.shape, BF16), grad_shape, grad_shape],
        scratch_shapes=[pltpu.VMEM((rows, tree_len), F32)],
        cost_estimate=pl.CostEstimate(
            flops=10 * LANES * work, bytes_accessed=12 * q_wide.size, transcendentals=work
        ),
        number=2,
    )


def pack_kernel(
    q_heads, kv_heads, dq_ref, dkv_ref, cos_ref, sin_ref, weight, packed_ref, product_ref, sum_ref
):
    @pl.when(pl.program_id(0) == 0)
    def _():
        cos_table = cos_ref[...]
        sin_table = -sin_ref[...]
        sum_ref[...] = jnp.zeros_like(sum_ref)
        for head in range(q_heads + 2 * kv_heads):
            base, shift = window_of(head)
            if head < q_heads:
                values = dq_ref[:, head * LANES : (head + 1) * LANES].astype(F32)
            else:
                at = (head - q_heads) * LANES
                values = dkv_ref[:, at : at + LANES].astype(BF16).astype(F32)
            if head < q_heads + kv_heads:
                values = rotated(values, cos_table, sin_table)
            wide = jnp.concatenate([values, jnp.zeros_like(values)], axis=1)
            if shift:
                wide = pltpu.roll(wide, shift, 1)
            sum_ref[:, base : base + 2 * LANES] += wide
        packed_ref[...] = sum_ref[...].astype(BF16)

    product_ref[...] = mm_nt(packed_ref[...], weight[...]).astype(BF16)


def pack_heads(dq_wide, dkv, cos_table, sin_table, weight, q_heads, kv_heads, sends):
    rows = dq_wide.shape[0]
    width, packed = weight.shape
    tile = width // 5

    def whole(values):
        return pl.BlockSpec(values.shape, lambda i: (0, 0))

    return hop_call(
        functools.partial(pack_kernel, q_heads, kv_heads),
        sends,
        *(dq_wide, dkv, cos_table, sin_table, weight),
        grid=(width // tile,),
        in_specs=[
            whole(dq_wide), whole(dkv), whole(cos_table), whole(sin_table),
            pl.BlockSpec((tile, packed), lambda i: (i, 0)),
        ],
        out_specs=[
            pl.BlockSpec((rows, packed), lambda i: (0, 0)),
            pl.BlockSpec((rows, tile), lambda i: (0, i)),
        ],
        out_shape=[
            jax.ShapeDtypeStruct((rows, packed), BF16),
            jax.ShapeDtypeStruct((rows, width), BF16),
        ],
        scratch_shapes=[pltpu.VMEM((rows, packed), F32)],
        cost_estimate=pl.CostEstimate(
            flops=2 * rows * width * packed,
            bytes_accessed=2 * width * packed + 8 * rows * packed + 2 * rows * width,
            transcendentals=0,
        ),
        number=5,
    )


def feed_forward_kernel(normed, gate_w, up_w, dmixed, mixed_ref, dgate_ref, dup_ref):
    gate = mm(normed[...], gate_w[...])
    up = mm(normed[...], up_w[...])
    sigmoid = 1.0 / (1.0 + jnp.exp(-gate))
    silu = gate * sigmoid
    slope = sigmoid * (1.0 + gate * (1.0 - sigmoid))
    mixed_ref[...] = (silu * up).astype(BF16)
    dgate_ref[...] = (dmixed[...] * up * slope).astype(BF16)
    dup_ref[...] = (dmixed[...] * silu).astype(BF16)


def feed_forward_hidden(normed, gate_up_w, dmixed, sends):
    rows, width = normed.shape
    hidden = dmixed.shape[1]
    tile = 2 * LANES
    count = hidden // tile
    result = pl.BlockSpec((rows, tile), lambda i: (0, i))
    return hop_call(
        feed_forward_kernel,
        sends,
        *(normed, gate_up_w, gate_up_w, dmixed),
        grid=(count,),
        in_specs=[
            pl.BlockSpec((rows, width), lambda i: (0, 0)),
            pl.BlockSpec((width, tile), lambda i: (0, i)),
            pl.BlockSpec((width, tile), lambda i: (0, i + count)),
            result,
        ],
        out_specs=[result] * 3,
        out_shape=[jax.ShapeDtypeStruct((rows, hidden), BF16)] * 3,
        cost_estimate=pl.CostEstimate(
            flops=4 * rows * hidden * width,
            bytes_accessed=4 * hidden * width + 2 * rows * width + 10 * rows * hidden,
            transcendentals=rows * hidden,
        ),
        number=3,
    )


def feed_back_kernel(dgate, dup, mixed, gate_w, up_w, down_w, dn2_ref, out_ref):
    dn2 = mm_nt(dgate[...], gate_w[...]) + mm_nt(dup[...], up_w[...])
    dn2_ref[...] = dn2.astype(BF16)
    out_ref[...] = mm_nt(mixed[...], down_w[...]).astype(BF16)


def feed_back(dgate, dup, mixed, gate_up_w, down_w, sends):
    rows, hidden = mixed.shape
    width = down_w.shape[0]
    tile = width // 5
    left = pl.BlockSpec((rows, hidden), lambda i: (0, 0))
    right = pl.BlockSpec((tile, hidden), lambda i: (i, 0))
    result = pl.BlockSpec((rows, tile), lambda i: (0, i))
    return hop_call(
        feed_back_kernel,
        sends,
        *(dgate, dup, mixed, gate_up_w, gate_up_w, down_w),
        grid=(width // tile,),
        in_specs=[
            *[left] * 3,
            right,
            pl.BlockSpec((tile, hidden), lambda i: (i, 1)),
            right,
        ],
        out_specs=[result] * 2,
        out_shape=[jax.ShapeDtypeStruct((rows, width), BF16)] * 2,
        cost_estimate=pl.CostEstimate(
            flops=6 * rows * hidden * width,
            bytes_accessed=6 * hidden * (rows + width) + 4 * rows * width,
            transcendentals=0,
        ),
        number=1,
    )


def out_back_kernel(grad, weight, select, result_ref):
    narrow = mm(grad[...], weight[...]).astype(BF16)
    result_ref[...] = mm_nt(narrow, select[...]).astype(BF16)


def out_back(grad, weight, select, sends):
    rows, wide = grad.shape[0], select.shape[0]

    def whole(values):
        return pl.BlockSpec(values.shape, lambda i: (0, 0))

    return hop_call(
        out_back_kernel,
        sends,
        *(grad, weight, select),
        grid=(1,),
        in_specs=[whole(grad), whole(weight), whole(select)],
        out_specs=[pl.BlockSpec((rows, wide), lambda i: (0, 0))],
        out_shape=[jax.ShapeDtypeStruct((rows, wide), BF16)],
        cost_estimate=pl.CostEstimate(
            flops=2 * rows * weight.size + 2 * rows * select.size,
            bytes_accessed=2 * (grad.size + weight.size + select.size + rows * wide),
            transcendentals=0,
        ),
        number=4,
    )


def piece(values, index, size):
    return lax.dynamic_slice_in_dim(values, index * size, size, 1)


class LineSum:
    def __init__(self, values, size, axis):
        self.axis = axis
        self.count = lax.axis_size(axis)
        self.pieces = [values[:, i * size : (i + 1) * size] for i in range(self.count)]
        self.step = 0
        self.got = None
        here = lax.axis_index(axis)
        self.valid = (here > 0, here < self.count - 1)

    def sends(self):
        self.step += 1
        step, count = self.step, self.count
        rights = [(i, i + 1) for i in range(step)]
        lefts = [(count - 1 - i, count - 2 - i) for i in range(step)]
        found = []
        for side, slot, pairs in ((0, step, rights), (1, count - step, lefts)):
            value = self.pieces[slot]
            if self.got is not None:
                value = (value.astype(F32) + self.arrived(side)).astype(BF16)
            found.append((value, self.axis, pairs, side))
        return found

    def arrived(self, side):
        return jnp.where(self.valid[side], self.got[side].astype(F32), 0.0)

    def loose(self):
        return self.step == 1 and self.count > 2

    def receive(self, results):
        self.got = results

    def result(self):
        assert self.step == self.count - 1
        total = self.pieces[0].astype(F32)
        for side in (0, 1) if self.got else ():
            total = total + self.arrived(side)
        return total


class LineGather:
    def __init__(self, own, axis):
        self.own, self.axis = own, axis
        self.count = lax.axis_size(axis)
        self.lefts, self.rights = [own], [own]

    def sends(self):
        step, count = len(self.lefts), self.count
        return [
            (self.lefts[-1], self.axis, [(i, i + 1) for i in range(step - 1, count - 1)], 0),
            (self.rights[-1], self.axis, [(i, i - 1) for i in range(count - step, 0, -1)], 1),
        ]

    def loose(self):
        return len(self.lefts) == self.count - 1 and self.count > 2

    def receive(self, results):
        self.lefts.append(results[0])
        self.rights.append(results[1])

    def result(self):
        count = self.count
        here = lax.axis_index(self.axis)
        assert len(self.lefts) == count
        others = [
            jnp.where(here >= step, self.lefts[step], self.rights[count - step])
            for step in range(1, count)
        ]
        return jnp.concatenate([self.own, *others], axis=1)


class EarlierGather:
    def __init__(self, own, axis):
        self.own, self.axis = own, axis
        self.count = lax.axis_size(axis)

    def sends(self):
        count = self.count
        return [
            (self.own, self.axis, [(i, i + step) for i in range(count - step)], None)
            for step in range(1, count)
        ]

    def receive(self, results):
        self.others = results

    def result(self):
        count, own = self.count, self.own
        here = lax.axis_index(self.axis)
        trees, rows, width = own.shape
        result = jnp.zeros((trees, count * rows, width), own.dtype)
        result = lax.dynamic_update_slice_in_dim(result, own, here * rows, 1)
        for step, other in enumerate(self.others, 1):
            slot = lax.rem(here - step + count, count)
            result = lax.dynamic_update_slice_in_dim(result, other, slot * rows, 1)
        return result


class EarlierReturn:
    def __init__(self, full, axis):
        self.full, self.axis = full, axis
        self.count = lax.axis_size(axis)
        self.rows = full.shape[1] // self.count

    def sends(self):
        count = self.count
        here = lax.axis_index(self.axis)
        found = []
        for step in range(1, count):
            slot = lax.rem(here - step + count, count)
            value = piece(self.full, slot, self.rows).astype(BF16)
            found.append((value, self.axis, [(i + step, i) for i in range(count - step)], None))
        return found

    def receive(self, results):
        self.others = results

    def result(self):
        total = piece(self.full, lax.axis_index(self.axis), self.rows)
        for other in self.others:
            total = total + other.astype(F32)
        return total


def ends(pairs, which):
    return {pair[which] for pair in pairs}


def disjoint(left, right):
    return not any(ends(left, which) & ends(right, which) for which in (0, 1))


def joined(sends, loose):
    groups = []
    for number, (value, axis, pairs, side) in enumerate(sends):
        for group in groups:
            if side is None or group.axis != axis or not disjoint(pairs, group.pairs):
                continue
            if group.side != side and not loose:
                continue
            here = lax.axis_index(axis)
            mine = functools.reduce(jnp.logical_or, [here == i for i in sorted(ends(pairs, 0))])
            group.value = jnp.where(mine, value, group.value)
            group.pairs = group.pairs + pairs
            group.members.append(number)
            break
        else:
            groups.append(
                SimpleNamespace(value=value, axis=axis, pairs=pairs, side=side, members=[number])
            )
    return groups


class Stages:
    def __init__(self):
        self.token = ()
        self.number = 0

    def wait_for(self, *values):
        self.token += values

    def __call__(self, transfers, compute=None, inputs=(), fused=False):
        self.number += 1
        kept = []
        for t in transfers:
            if t.count > 1:
                kept.append(t)
            else:
                t.receive([])
        transfers = kept
        sends = [t.sends() for t in transfers]
        lines = [t for t in transfers if hasattr(t, "loose")]
        loose = len(lines) == 1 and lines[0].loose() and not fused
        groups = joined([send for of_one in sends for send in of_one], loose)
        values = [group.value for group in groups]
        tied = lax.optimization_barrier((*values, *inputs, *self.token))
        results = {}
        token = []
        by_kernel = []
        for value, group in zip(tied, groups):
            if fused and group.side is not None:
                by_kernel.append((value, group))
                continue
            other = lax.ppermute(value, group.axis, group.pairs)
            token.append(other)
            results.update({number: other for number in group.members})
        given = tied[len(groups) : len(groups) + len(inputs)]
        if by_kernel:
            line_sends = [(value, group.side) for value, group in by_kernel]
            if compute is None:
                outs, others = hop_call(None, line_sends)
            else:
                outs, others = compute(*given, line_sends)
            for other, (_, group) in zip(others, by_kernel):
                token.append(other)
                results.update({number: other for number in group.members})
        else:
            outs = compute(*given) if compute else ()
        at = 0
        for transfer, of_one in zip(transfers, sends):
            transfer.receive([results[at + i] for i in range(len(of_one))])
            at += len(of_one)
        self.token = (*token, *outs)
        return outs


def turned(values, dim, axis):
    count = lax.axis_size(axis)
    here = lax.axis_index(axis)
    size = values.shape[dim] // count
    return jnp.concatenate(
        [
            lax.dynamic_slice_in_dim(
                values, lax.rem(here - i + count, count) * size, size, dim
            )
            for i in range(count)
        ],
        axis=dim,
    )


class SmallSum:
    def __init__(self, values, axis):
        self.values, self.axis = values, axis
        self.count = lax.axis_size(axis)

    def sends(self):
        count = self.count
        return [
            (self.values, self.axis, [(i, (i + step) % count) for i in range(count)], None)
            for step in range(1, count)
        ]

    def receive(self, results):
        self.others = results

    def result(self):
        return sum(self.others, self.values)


def norm_back(grad, values, gain):
    root = lax.rsqrt(jnp.mean(values * values, axis=-1, keepdims=True) + EPS)
    weighted = grad * gain
    mean = jnp.mean(weighted * values, axis=-1, keepdims=True)
    return root * weighted - values * (root * root * root) * mean


def on_device(
    tokens, norm_one, q_weight, k_weight, v_weight, o_weight, norm_two,
    gate_weight, up_weight, down_weight, segment_ids, parent_ids, path_pos, cotangent,
):
    ctx = lax.axis_index("context")
    ctx_count = lax.axis_size("context")
    ten_count = lax.axis_size(HOP_AXIS)
    tree_count, rows, width = tokens.shape
    share = rows // ten_count
    trees = tree_count // MICRO
    flat = trees * rows
    part, q_width = q_weight.shape
    kv_width = k_weight.shape[1]
    q_heads = q_width // HEAD
    kv_heads = kv_width // HEAD
    used = q_width + 2 * kv_width
    packed_width = round_up(used + 2, LANES)

    attention_block = jnp.concatenate(
        [
            q_weight, k_weight, v_weight, norm_one[:, None], norm_two[:, None],
            jnp.zeros((part, packed_width - used - 2), BF16),
        ],
        axis=1,
    )
    attention_full = lax.all_gather(attention_block, WEIGHT_AXES, axis=0, tiled=True)
    o_full = lax.all_gather(o_weight.T, WEIGHT_AXES, axis=0, tiled=True)
    hidden = gate_weight.shape[1]
    wide = round_up(hidden, LANES)

    def widened(values):
        return jnp.pad(values, ((0, 0), (0, wide - hidden)))

    down_full = lax.all_gather(widened(down_weight.T), WEIGHT_AXES, axis=0, tiled=True)
    gate_up_block = jnp.concatenate([widened(gate_weight), widened(up_weight)], axis=1)
    gate_up_full = lax.all_gather(gate_up_block, WEIGHT_AXES, axis=0, tiled=True)
    gain_one = attention_full[:, used].astype(F32)
    gain_two = attention_full[:, used + 1].astype(F32)

    lane = np.arange(q_heads * LANES)
    column = np.arange(q_width)
    select = jnp.asarray(
        (lane[:, None] // LANES == column[None, :] // HEAD)
        & (lane[:, None] % LANES == column[None, :] % HEAD),
        BF16,
    )
    frequency = THETA ** (-(jnp.arange(HALF, dtype=F32) * 2.0 / HEAD))
    pad = jnp.zeros((flat, LANES - HEAD), F32)
    ctx_ref = jnp.reshape(ctx, (1,)).astype(jnp.int32)

    tokens = turned(tokens, 1, HOP_AXIS)
    cotangent = turned(cotangent, 1, HOP_AXIS)
    segment_ids, parent_ids, path_pos = [
        turned(ids.reshape(-1, ctx_count, rows), 2, HOP_AXIS).reshape(ids.shape)
        for ids in (segment_ids, parent_ids, path_pos)
    ]
    state = []
    for micro in range(MICRO):
        pick = slice(micro * trees, (micro + 1) * trees)
        m = SimpleNamespace()
        state.append(m)
        m.number = micro
        m.x = tokens[pick]
        m.dy = cotangent[pick]
        seg, par, pos = segment_ids[pick], parent_ids[pick], path_pos[pick]

        def here(ids):
            return lax.dynamic_slice_in_dim(ids, ctx * rows, rows, 1)

        m.ids = (
            here(seg)[:, :, None], here(par)[:, :, None], here(pos)[:, :, None],
            seg[:, None, :], pos[:, None, :],
        )
        angles = here(pos).reshape(flat).astype(F32)[:, None] * frequency[None, :]
        cosine, sine = jnp.cos(angles), jnp.sin(angles)
        m.cos = jnp.concatenate([cosine, cosine, pad], axis=1)
        m.sin = jnp.concatenate([-sine, sine, pad], axis=1)
        x = m.x.reshape(flat, width).astype(F32)
        m.root_one = lax.rsqrt(jnp.mean(x * x, axis=-1, keepdims=True) + EPS)
        m.x_here = m.x[:, :share].astype(F32)
        m.dy_here = m.dy[:, :share].astype(F32)

    def together(*parts):
        return jnp.concatenate([part.reshape(flat, -1) for part in parts], axis=0)

    def shaped(product):
        return product.reshape(trees, rows, width)

    x_all = tokens.reshape(-1, width).astype(F32)
    root_all = jnp.concatenate([m.root_one for m in state], axis=0)
    normed_all = (x_all * root_all * gain_one).astype(BF16)
    stage = Stages()
    a, b = state

    def project(m):
        def run(root):
            at = m.number * flat
            packed = mm(normed_all[at : at + flat], attention_full)
            m.q, kv = split_heads(packed, m.cos, m.sin, q_heads, kv_heads, rows)
            m.kv = EarlierGather(kv.reshape(trees, rows, -1), "context")
            return (m.q,)

        return run

    def attend(m):
        def run(q):
            m.kv_full = m.kv.result()
            wide = attend_forward(ctx_ref, q, m.kv_full, m.ids, q_heads, kv_heads, rows)
            m.attended = mm(wide, select).astype(BF16)
            product = mm_nt(m.attended, o_full).astype(BF16)
            m.sum1 = LineSum(shaped(product), share, HOP_AXIS)
            return (product,)

        return run

    def mixed_back(m):
        def run(dy):
            m.dmixed = row_major(mm(dy.reshape(flat, width), down_full))
            return (m.dmixed,)

        return run

    def norm_two_of(m):
        middle = m.x_here + m.sum1.result()
        root = lax.rsqrt(jnp.mean(middle * middle, axis=-1, keepdims=True) + EPS)
        m.middle, m.root_two = middle, root
        m.gather1 = LineGather((middle * root * gain_two).astype(BF16), HOP_AXIS)

    def feed_forward(m):
        def run(normed_two, sends):
            m.normed_two = normed_two
            (m.mixed, m.dgate, m.dup), others = feed_forward_hidden(
                normed_two, gate_up_full, m.dmixed, sends
            )
            return (m.mixed, m.dgate, m.dup), others

        return run

    def back_of(m):
        def run(dgate, sends):
            (product, out), others = feed_back(
                dgate, m.dup, m.mixed, gate_up_full, down_full, sends
            )
            m.sum3 = LineSum(shaped(product), share, HOP_AXIS)
            m.out_part = shaped(out)
            return (product, out), others

        return run

    def norm_two_back(m):
        middle, dn2 = m.middle, m.sum3.result()
        m.gain_two_grad = jnp.sum(dn2 * middle * m.root_two, axis=(0, 1))
        m.dmiddle = m.dy_here + norm_back(dn2, middle, gain_two)
        m.gather2 = LineGather(m.dmiddle.astype(BF16), HOP_AXIS)

    def attended_back(m):
        def run(dmb, sends):
            m.dmb = dmb
            (m.do,), others = out_back(dmb, o_full, select, sends)
            return (m.do,), others

        return run

    def attend_back(m):
        def run(do_wide, sends):
            (m.dq, dk, dv), others = attend_backward(
                m.q, m.kv_full, do_wide, m.ids, q_heads, kv_heads, rows, sends
            )
            m.dkv = EarlierReturn(jnp.concatenate([dk, dv], axis=2), "context")
            return (m.dq,), others

        return run

    def norm_one_back(m):
        def run(dq, sends):
            dkv = m.dkv.result().reshape(flat, -1)
            (m.dqkv, dn1), others = pack_heads(
                dq, dkv, m.cos, m.sin, attention_full, q_heads, kv_heads, sends
            )
            x = m.x.reshape(flat, width).astype(F32)
            m.gain_one_grad = jnp.sum(dn1.astype(F32) * x * m.root_one, axis=0)
            m.sum4 = LineSum(shaped(dn1), share, HOP_AXIS)
            return (m.dqkv, dn1), others

        return run

    class WeightGrad:
        def __init__(self, right_of):
            self.right_of = right_of

        def __call__(self, left):
            self.grad = row_major(mm_tn(left, self.right_of()).astype(BF16))
            return (self.grad,)

        def scattered(self):
            return lax.psum_scatter(self.grad, WEIGHT_AXES, scatter_dimension=0, tiled=True)

    def gathered(transfer):
        return transfer.result().reshape(flat, width)

    stage([], project(a), [a.root_one])
    stage([a.kv], project(b), [b.root_one])
    stage([b.kv], attend(a), [a.q])
    stage([a.sum1], attend(b), [b.q])
    stage([a.sum1], fused=True)
    stage([a.sum1], mixed_back(a), [a.dy])
    norm_two_of(a)
    stage([a.gather1], mixed_back(b), [b.dy])
    stage([a.gather1, b.sum1], fused=True)
    stage([a.gather1, b.sum1], fused=True)
    stage([b.sum1], fused=True)
    norm_two_of(b)
    stage([b.gather1], feed_forward(a), [gathered(a.gather1)], fused=True)
    stage([b.gather1], back_of(a), [a.dgate], fused=True)
    stage([b.gather1, a.sum3], fused=True)
    stage([a.sum3], feed_forward(b), [gathered(b.gather1)], fused=True)
    dy_all = cotangent.reshape(-1, width)
    mixed_all = together(a.mixed, b.mixed)
    down_grad = WeightGrad(lambda: mixed_all)
    stage([a.sum3], down_grad, [dy_all])
    down_grad = down_grad.scattered()
    norm_two_back(a)
    a.sum2 = LineSum(a.out_part, share, HOP_AXIS)
    stage([a.gather2, a.sum2], back_of(b), [b.dgate], fused=True)
    b.sum2 = LineSum(b.out_part, share, HOP_AXIS)
    gate_up_grad = WeightGrad(
        lambda: jnp.concatenate([together(a.dgate, b.dgate), together(a.dup, b.dup)], axis=1)
    )
    stage([a.gather2, b.sum3], gate_up_grad, [together(a.normed_two, b.normed_two)])
    gate_up_grad = gate_up_grad.scattered()
    stage([a.gather2, b.sum3], fused=True)
    stage([b.sum3], attended_back(a), [gathered(a.gather2)], fused=True)
    norm_two_back(b)
    stage([b.gather2], attend_back(a), [a.do], fused=True)
    stage([b.gather2, b.sum2, a.dkv], fused=True)
    stage([b.gather2, a.sum2], norm_one_back(a), [a.dq], fused=True)
    stage.wait_for(down_grad)
    stage([a.sum4], attended_back(b), [gathered(b.gather2)], fused=True)
    stage([a.sum4, a.sum2], attend_back(b), [b.do], fused=True)
    stage.wait_for(gate_up_grad)
    o_grad = WeightGrad(lambda: together(a.attended, b.attended))
    stage([a.sum4, b.dkv], o_grad, [together(a.dmb, b.dmb)])
    o_grad = o_grad.scattered()
    stage([b.sum2], norm_one_back(b), [b.dq], fused=True)
    gains = jnp.stack([a.gain_one_grad + b.gain_one_grad, a.gain_two_grad + b.gain_two_grad])
    gains = SmallSum(gains, HOP_AXIS)
    attention_grad = WeightGrad(lambda: together(a.dqkv, b.dqkv))
    stage([b.sum4, b.sum2, gains], attention_grad, [normed_all])
    attention_grad = attention_grad.scattered().astype(F32)
    gains = SmallSum(gains.result(), "context")
    stage([b.sum4, gains], fused=True)
    stage.wait_for(o_grad)
    gains = SmallSum(gains.result(), "fsdp")
    stage([b.sum4, gains], fused=True)
    block = lax.axis_index("fsdp") * ctx_count + ctx
    gains = lax.dynamic_slice_in_dim(gains.result(), block * part, part, 1)
    for m in state:
        m.out_sum = m.sum2.result()
    for m in state:
        middle, out_sum = lax.optimization_barrier((m.middle, m.out_sum))
        m.out = (middle + out_sum.astype(F32)).astype(BF16)
        m.dx = (m.dmiddle + norm_back(m.sum4.result(), m.x_here, gain_one)).astype(BF16)

    return (
        jnp.concatenate([m.out for m in state], axis=0),
        jnp.concatenate([m.dx for m in state], axis=0),
        gains[0],
        attention_grad[:, :q_width],
        attention_grad[:, q_width : q_width + kv_width],
        attention_grad[:, q_width + kv_width : used],
        o_grad.T.astype(F32),
        gains[1],
        gate_up_grad[:, :hidden].astype(F32),
        gate_up_grad[:, wide : wide + hidden].astype(F32),
        down_grad[:, :hidden].T.astype(F32),
    )


def solution(mesh):
    weights = WEIGHT_AXES
    return jax.shard_map(
        on_device,
        mesh=mesh,
        in_specs=(
            P("fsdp", "context", None),
            P(weights),
            P(weights, "tensor"),
            P(weights, "tensor"),
            P(weights, "tensor"),
            P("tensor", weights),
            P(weights),
            P(weights, "tensor"),
            P(weights, "tensor"),
            P("tensor", weights),
            P("fsdp", None),
            P("fsdp", None),
            P("fsdp", None),
            P("fsdp", "context", None),
        ),
        out_specs=(
            P("fsdp", ("context", "tensor"), None),
            P("fsdp", ("context", "tensor"), None),
            P(weights),
            P(weights, "tensor"),
            P(weights, "tensor"),
            P(weights, "tensor"),
            P("tensor", weights),
            P(weights),
            P(weights, "tensor"),
            P(weights, "tensor"),
            P("tensor", weights),
        ),
        check_vma=False,
    )
```

```python
import functools
from types import SimpleNamespace

import jax
import jax.numpy as jnp
import numpy as np
from jax import lax
from jax.experimental import pallas as pl
from jax.experimental.pallas import tpu as pltpu
from jax.experimental.layout import Layout, with_layout_constraint
from jax.sharding import PartitionSpec as P


HEAD = 80
HALF = HEAD // 2
LANES = 128
MICRO = 2
EPS = 1e-05
THETA = 10000.0
NEG = -1000000000.0
TRUNK = 512
WEIGHT_AXES = ("fsdp", "context")
BF16 = jnp.bfloat16
F32 = jnp.float32


def row_major(value):
    return with_layout_constraint(value, Layout(major_to_minor=(0, 1)))


def round_up(value, unit):
    return (value + unit - 1) // unit * unit


def mm(left, right):
    return lax.dot_general(left, right, (((1,), (0,)), ((), ())), preferred_element_type=F32)


def mm_nt(left, right):
    return lax.dot_general(left, right, (((1,), (1,)), ((), ())), preferred_element_type=F32)


def mm_tn(left, right):
    return lax.dot_general(left, right, (((0,), (0,)), ((), ())), preferred_element_type=F32)


def rotated(values, cos_table, sin_table):
    lane = lax.broadcasted_iota(jnp.int32, values.shape, 1)
    swapped = jnp.where(
        lane < HALF, pltpu.roll(values, LANES - HALF, 1), pltpu.roll(values, HALF, 1)
    )
    return values * cos_table + swapped * sin_table


def window_of(head):
    start = head * HEAD
    base = start // LANES * LANES
    return base, start - base


def split_kernel(q_heads, kv_heads, x_ref, cos_ref, sin_ref, q_ref, kv_ref):
    cos_table = cos_ref[...]
    sin_table = sin_ref[...]
    for head in range(q_heads + 2 * kv_heads):
        base, shift = window_of(head)
        window = x_ref[:, base : base + 2 * LANES]
        if shift:
            window = pltpu.roll(window, 2 * LANES - shift, 1)
        values = window[:, :LANES]
        if head < q_heads + kv_heads:
            result = rotated(values, cos_table, sin_table)
        else:
            lane = lax.broadcasted_iota(jnp.int32, values.shape, 1)
            result = jnp.where(lane < HEAD, values, 0.0)
        result = result.astype(BF16)
        if head < q_heads:
            q_ref[:, head * LANES : (head + 1) * LANES] = result
        else:
            at = (head - q_heads) * LANES
            kv_ref[:, at : at + LANES] = result


def split_heads(packed, cos_table, sin_table, q_heads, kv_heads, rows):
    total, width = packed.shape
    q_wide = q_heads * LANES
    kv_wide = 2 * kv_heads * LANES
    return pl.pallas_call(
        functools.partial(split_kernel, q_heads, kv_heads),
        grid=(total // rows,),
        in_specs=[
            pl.BlockSpec((rows, width), lambda b: (b, 0)),
            pl.BlockSpec((rows, LANES), lambda b: (b, 0)),
            pl.BlockSpec((rows, LANES), lambda b: (b, 0)),
        ],
        out_specs=[
            pl.BlockSpec((rows, q_wide), lambda b: (b, 0)),
            pl.BlockSpec((rows, kv_wide), lambda b: (b, 0)),
        ],
        out_shape=[
            jax.ShapeDtypeStruct((total, q_wide), BF16),
            jax.ShapeDtypeStruct((total, kv_wide), BF16),
        ],
        cost_estimate=pl.CostEstimate(
            flops=10 * total * width, bytes_accessed=7 * total * width, transcendentals=0
        ),
        name="split_heads",
    )(packed, cos_table, sin_table)


def fill_bias(seg_q, par_q, pos_q, seg_k, pos_k, bias_ref):
    same = (seg_k == seg_q) | (seg_k == par_q) | (seg_k == 0)
    bias_ref[...] = jnp.where(same & (pos_k <= pos_q), 0.0, NEG)


def probabilities(q_block, keys, bias):
    scores = mm_nt(q_block, keys) * HEAD ** (-0.5) + bias
    top = jnp.max(scores, axis=1, keepdims=True)
    raised = jnp.exp(scores - top)
    return raised * (1.0 / jnp.sum(raised, axis=1, keepdims=True))


def forward_kernel(
    rows, tree_len, block,
    ctx_ref, q_ref, k_ref, v_ref, seg_q, par_q, pos_q, seg_k, pos_k, out_ref, bias_ref,
):
    @pl.when(pl.program_id(1) == 0)
    def _():
        fill_bias(seg_q[0], par_q[0], pos_q[0], seg_k[0], pos_k[0], bias_ref)

    in_trunk = (ctx_ref[0] + 1) * rows <= TRUNK

    def run(keys):
        @pl.loop(0, rows // block)
        def _(step):
            at = pl.ds(pl.multiple_of(step * block, block), block)
            probs = probabilities(q_ref[at, :], k_ref[0, :keys, :], bias_ref[at, :keys])
            out_ref[at, :] = mm(probs.astype(BF16), v_ref[0, :keys, :]).astype(BF16)

    pl.when(in_trunk)(lambda: run(min(TRUNK, tree_len)))
    pl.when(jnp.logical_not(in_trunk))(lambda: run(tree_len))


def backward_kernel(
    rows, tree_len, block, group,
    q_ref, k_ref, v_ref, do_ref, seg_q, par_q, pos_q, seg_k, pos_k,
    dq_ref, dk_ref, dv_ref, bias_ref,
):
    head = pl.program_id(1)

    @pl.when(head == 0)
    def _():
        fill_bias(seg_q[0], par_q[0], pos_q[0], seg_k[0], pos_k[0], bias_ref)

    @pl.when(lax.rem(head, group) == 0)
    def _():
        dk_ref[...] = jnp.zeros_like(dk_ref)
        dv_ref[...] = jnp.zeros_like(dv_ref)

    in_trunk = (lax.axis_index("context") + 1) * rows <= TRUNK
    scale = HEAD ** (-0.5)

    def run(keys):
        @pl.loop(0, rows // block)
        def _(step):
            at = pl.ds(pl.multiple_of(step * block, block), block)
            q_block = q_ref[at, :]
            do_block = do_ref[at, :]
            k_all = k_ref[0, :keys, :]
            probs = probabilities(q_block, k_all, bias_ref[at, :keys])
            dprobs = mm_nt(do_block, v_ref[0, :keys, :])
            delta = jnp.sum(probs * dprobs, axis=1, keepdims=True)
            dscores = (probs * (dprobs - delta)).astype(BF16)
            dq_ref[at, :] = (mm(dscores, k_all) * scale).astype(BF16)
            dk_ref[0, :keys, :] += mm_tn(dscores, q_block) * scale
            dv_ref[0, :keys, :] += mm_tn(probs.astype(BF16), do_block)

    pl.when(in_trunk)(lambda: run(min(TRUNK, tree_len)))
    pl.when(jnp.logical_not(in_trunk))(lambda: run(tree_len))


def attention_specs(rows, tree_len, group, kv_heads):
    def column(b, h, *c):
        return (b, h)

    def whole(b, h, *c):
        return (b, 0, 0)

    return [
        pl.BlockSpec((rows, LANES), column),
        pl.BlockSpec((1, tree_len, LANES), lambda b, h, *c: (b, 0, h // group)),
        pl.BlockSpec((1, tree_len, LANES), lambda b, h, *c: (b, 0, kv_heads + h // group)),
    ], [
        pl.BlockSpec((1, rows, 1), whole),
        pl.BlockSpec((1, rows, 1), whole),
        pl.BlockSpec((1, rows, 1), whole),
        pl.BlockSpec((1, 1, tree_len), whole),
        pl.BlockSpec((1, 1, tree_len), whole),
    ]


def attend_forward(ctx, q_wide, kv_full, ids, q_heads, kv_heads, rows):
    trees, tree_len, _ = kv_full.shape
    group = q_heads // kv_heads
    first, last = attention_specs(rows, tree_len, group, kv_heads)
    block = min(rows, 256)
    work = trees * q_heads * rows * tree_len
    return pl.pallas_call(
        functools.partial(forward_kernel, rows, tree_len, block),
        grid_spec=pltpu.PrefetchScalarGridSpec(
            num_scalar_prefetch=1,
            grid=(trees, q_heads),
            in_specs=first + last,
            out_specs=pl.BlockSpec((rows, LANES), lambda b, h, c: (b, h)),
            scratch_shapes=[pltpu.VMEM((rows, tree_len), F32)],
        ),
        out_shape=jax.ShapeDtypeStruct(q_wide.shape, BF16),
        cost_estimate=pl.CostEstimate(
            flops=4 * LANES * work, bytes_accessed=8 * q_wide.size, transcendentals=work
        ),
        name="attend_forward",
    )(ctx, q_wide, kv_full, kv_full, *ids)


HOP_AXIS = "tensor"


def copies_of(ways):
    found = []
    for number, way in enumerate(ways):
        if way in (0, 1):
            found.append((number, HOP_AXIS, 1 - 2 * way, way))
        else:
            found += [(number, way, step, None) for step in range(1, lax.axis_size(way))]
    return found


def with_hops(kernel, rank, counts, ways, *refs):
    own_in, own_out, own_scratch = counts
    copies = copies_of(ways)
    ends_at = [0]
    for size in (own_in, len(ways), own_out, len(copies), own_scratch):
        ends_at.append(ends_at[-1] + size)
    ins, sent, outs, received, scratch = (
        refs[low:high] for low, high in zip(ends_at, ends_at[1:])
    )
    send_sem, recv_sem = refs[ends_at[-1] :]
    here = lax.axis_index(HOP_AXIS)
    has_next, has_last = here < lax.axis_size(HOP_AXIS) - 1, here > 0

    def device(axis, step, side):
        at = lax.axis_index(axis) + step
        if side is None:
            at = lax.rem(at, lax.axis_size(axis))
        return {axis: at}

    def copy(at):
        number, axis, step, side = copies[at]
        return pltpu.make_async_remote_copy(
            src_ref=sent[number],
            dst_ref=received[at],
            send_sem=send_sem.at[at],
            recv_sem=recv_sem.at[at],
            device_id=device(axis, step, side),
            device_id_type=pl.DeviceIdType.MESH,
        )

    def start():
        barrier = pltpu.get_barrier_semaphore()

        def greet(axis, step, side):
            pl.semaphore_signal(
                barrier,
                inc=1,
                device_id=device(axis, step, side),
                device_id_type=pl.DeviceIdType.MESH,
            )

        everyone = {axis for _, axis, _, side in copies if side is None}
        peers = sum(lax.axis_size(axis) - 1 for axis in everyone)
        for axis in sorted(everyone):
            for step in range(1, lax.axis_size(axis)):
                greet(axis, step, None)
        if HOP_AXIS not in everyone:
            pl.when(has_next)(lambda: greet(HOP_AXIS, 1, 0))
            pl.when(has_last)(lambda: greet(HOP_AXIS, -1, 1))
            peers = peers + has_next.astype(jnp.int32) + has_last.astype(jnp.int32)
        pl.semaphore_wait(barrier, peers)
        for at, (_, _, _, side) in enumerate(copies):
            if side is None:
                copy(at).start()
            else:
                pl.when((has_next, has_last)[side])(lambda at=at: copy(at).start())

    def finish():
        for at, (_, _, _, side) in enumerate(copies):
            if side is None:
                copy(at).wait()
            else:
                pl.when((has_next, has_last)[side])(lambda at=at: copy(at).wait_send())
                pl.when((has_last, has_next)[side])(lambda at=at: copy(at).wait_recv())

    if kernel is None:
        start()
        finish()
    else:
        first, last = jnp.bool_(True), jnp.bool_(True)
        for axis in range(rank):
            first &= pl.program_id(axis) == 0
            last &= pl.program_id(axis) == pl.num_programs(axis) - 1
        pl.when(first)(start)
        kernel(*ins, *outs, *scratch)
        pl.when(last)(finish)


HOP_IDS = {}


def hop_call(kernel, sends, *args, grid=(), in_specs=(), out_specs=(), out_shape=(),
             scratch_shapes=(), name="hop", cost_estimate=None):
    ways = tuple(way for _, way in sends)
    values = [value for value, _ in sends]
    copies = copies_of(ways)
    anywhere = pl.BlockSpec(memory_space=pl.ANY)
    counts = (len(args), len(out_shape), len(scratch_shapes))
    key = (name, ways, tuple(v.shape for v in values), tuple(v.shape for v in args))
    results = pl.pallas_call(
        functools.partial(with_hops, kernel, len(grid), counts, ways),
        grid=grid,
        in_specs=[*in_specs, *[anywhere] * len(values)],
        out_specs=[*out_specs, *[anywhere] * len(copies)],
        out_shape=[
            *out_shape,
            *[jax.ShapeDtypeStruct(values[c[0]].shape, values[c[0]].dtype) for c in copies],
        ],
        scratch_shapes=[
            *scratch_shapes,
            pltpu.SemaphoreType.DMA((len(copies),)),
            pltpu.SemaphoreType.DMA((len(copies),)),
        ],
        compiler_params=pltpu.CompilerParams(
            collective_id=HOP_IDS.setdefault(key, len(HOP_IDS)), has_side_effects=True
        ),
        cost_estimate=cost_estimate,
    )(*args, *values)
    return results[: len(out_shape)], results[len(out_shape) :]


def attend_backward(q_wide, kv_full, do_wide, ids, q_heads, kv_heads, rows, sends):
    trees, tree_len, _ = kv_full.shape
    group = q_heads // kv_heads
    first, last = attention_specs(rows, tree_len, group, kv_heads)
    block = min(rows, 256)
    work = trees * q_heads * rows * tree_len
    grad_spec = pl.BlockSpec((1, tree_len, LANES), lambda b, h: (b, 0, h // group))
    grad_shape = jax.ShapeDtypeStruct((trees, tree_len, kv_heads * LANES), F32)
    return hop_call(
        functools.partial(backward_kernel, rows, tree_len, block, group),
        sends,
        *(q_wide, kv_full, kv_full, do_wide, *ids),
        grid=(trees, q_heads),
        in_specs=first + [first[0]] + last,
        out_specs=[first[0], grad_spec, grad_spec],
        out_shape=[jax.ShapeDtypeStruct(q_wide.shape, BF16), grad_shape, grad_shape],
        scratch_shapes=[pltpu.VMEM((rows, tree_len), F32)],
        cost_estimate=pl.CostEstimate(
            flops=10 * LANES * work, bytes_accessed=12 * q_wide.size, transcendentals=work
        ),
        name="attend_backward",
    )


def pack_kernel(
    q_heads, kv_heads, dq_ref, dkv_ref, cos_ref, sin_ref, weight, x_ref, root_ref,
    packed_ref, product_ref, gain_ref, sum_ref,
):
    @pl.when(pl.program_id(0) == 0)
    def _():
        cos_table = cos_ref[...]
        sin_table = -sin_ref[...]
        sum_ref[...] = jnp.zeros_like(sum_ref)
        for head in range(q_heads + 2 * kv_heads):
            base, shift = window_of(head)
            if head < q_heads:
                values = dq_ref[:, head * LANES : (head + 1) * LANES].astype(F32)
            else:
                at = (head - q_heads) * LANES
                values = dkv_ref[:, at : at + LANES].astype(BF16).astype(F32)
            if head < q_heads + kv_heads:
                values = rotated(values, cos_table, sin_table)
            wide = jnp.concatenate([values, jnp.zeros_like(values)], axis=1)
            if shift:
                wide = pltpu.roll(wide, shift, 1)
            sum_ref[:, base : base + 2 * LANES] += wide
        packed_ref[...] = sum_ref[...].astype(BF16)

    product = mm_nt(packed_ref[...], weight[...])
    product_ref[...] = product.astype(BF16)
    gain_ref[...] = jnp.sum(product * x_ref[...].astype(F32) * root_ref[...], axis=0, keepdims=True)


def pack_heads(
    dq_wide, dkv, cos_table, sin_table, weight, x_rows, root, q_heads, kv_heads, sends
):
    rows = dq_wide.shape[0]
    width, packed = weight.shape
    tile = width // 5

    def whole(values):
        return pl.BlockSpec(values.shape, lambda i: (0, 0))

    return hop_call(
        functools.partial(pack_kernel, q_heads, kv_heads),
        sends,
        *(dq_wide, dkv, cos_table, sin_table, weight, x_rows, root),
        grid=(width // tile,),
        in_specs=[
            whole(dq_wide), whole(dkv), whole(cos_table), whole(sin_table),
            pl.BlockSpec((tile, packed), lambda i: (i, 0)),
            pl.BlockSpec((rows, tile), lambda i: (0, i)),
            whole(root),
        ],
        out_specs=[
            pl.BlockSpec((rows, packed), lambda i: (0, 0)),
            pl.BlockSpec((rows, tile), lambda i: (0, i)),
            pl.BlockSpec((1, tile), lambda i: (0, i)),
        ],
        out_shape=[
            jax.ShapeDtypeStruct((rows, packed), BF16),
            jax.ShapeDtypeStruct((rows, width), BF16),
            jax.ShapeDtypeStruct((1, width), F32),
        ],
        scratch_shapes=[pltpu.VMEM((rows, packed), F32)],
        cost_estimate=pl.CostEstimate(
            flops=2 * rows * width * packed,
            bytes_accessed=2 * width * packed + 8 * rows * packed + 2 * rows * width,
            transcendentals=0,
        ),
        name="pack_heads",
    )


def feed_forward_kernel(normed, gate_w, up_w, dmixed, mixed_ref, dgate_ref, dup_ref):
    gate = mm(normed[...], gate_w[...])
    up = mm(normed[...], up_w[...])
    sigmoid = 1.0 / (1.0 + jnp.exp(-gate))
    silu = gate * sigmoid
    slope = sigmoid * (1.0 + gate * (1.0 - sigmoid))
    mixed_ref[...] = (silu * up).astype(BF16)
    dgate_ref[...] = (dmixed[...] * up * slope).astype(BF16)
    dup_ref[...] = (dmixed[...] * silu).astype(BF16)


def feed_forward_hidden(normed, gate_up_w, dmixed, sends):
    rows, width = normed.shape
    hidden = dmixed.shape[1]
    tile = 2 * LANES
    count = hidden // tile
    result = pl.BlockSpec((rows, tile), lambda i: (0, i))
    return hop_call(
        feed_forward_kernel,
        sends,
        *(normed, gate_up_w, gate_up_w, dmixed),
        grid=(count,),
        in_specs=[
            pl.BlockSpec((rows, width), lambda i: (0, 0)),
            pl.BlockSpec((width, tile), lambda i: (0, i)),
            pl.BlockSpec((width, tile), lambda i: (0, i + count)),
            result,
        ],
        out_specs=[result] * 3,
        out_shape=[jax.ShapeDtypeStruct((rows, hidden), BF16)] * 3,
        cost_estimate=pl.CostEstimate(
            flops=4 * rows * hidden * width,
            bytes_accessed=4 * hidden * width + 2 * rows * width + 10 * rows * hidden,
            transcendentals=rows * hidden,
        ),
        name="feed_forward",
    )


def feed_back_kernel(dgate, dup, mixed, gate_w, up_w, down_w, dn2_ref, out_ref):
    dn2 = mm_nt(dgate[...], gate_w[...]) + mm_nt(dup[...], up_w[...])
    dn2_ref[...] = dn2.astype(BF16)
    out_ref[...] = mm_nt(mixed[...], down_w[...]).astype(BF16)


def feed_back(dgate, dup, mixed, gate_up_w, down_w, sends):
    rows, hidden = mixed.shape
    width = down_w.shape[0]
    tile = width // 5
    left = pl.BlockSpec((rows, hidden), lambda i: (0, 0))
    right = pl.BlockSpec((tile, hidden), lambda i: (i, 0))
    result = pl.BlockSpec((rows, tile), lambda i: (0, i))
    return hop_call(
        feed_back_kernel,
        sends,
        *(dgate, dup, mixed, gate_up_w, gate_up_w, down_w),
        grid=(width // tile,),
        in_specs=[
            *[left] * 3,
            right,
            pl.BlockSpec((tile, hidden), lambda i: (i, 1)),
            right,
        ],
        out_specs=[result] * 2,
        out_shape=[jax.ShapeDtypeStruct((rows, width), BF16)] * 2,
        cost_estimate=pl.CostEstimate(
            flops=6 * rows * hidden * width,
            bytes_accessed=6 * hidden * (rows + width) + 4 * rows * width,
            transcendentals=0,
        ),
        name="feed_back",
    )


def out_back_kernel(grad, weight, select, result_ref):
    narrow = mm(grad[...], weight[...]).astype(BF16)
    result_ref[...] = mm_nt(narrow, select[...]).astype(BF16)


def out_back(grad, weight, select, sends):
    rows, wide = grad.shape[0], select.shape[0]

    def whole(values):
        return pl.BlockSpec(values.shape, lambda i: (0, 0))

    return hop_call(
        out_back_kernel,
        sends,
        *(grad, weight, select),
        grid=(1,),
        in_specs=[whole(grad), whole(weight), whole(select)],
        out_specs=[pl.BlockSpec((rows, wide), lambda i: (0, 0))],
        out_shape=[jax.ShapeDtypeStruct((rows, wide), BF16)],
        cost_estimate=pl.CostEstimate(
            flops=2 * rows * weight.size + 2 * rows * select.size,
            bytes_accessed=2 * (grad.size + weight.size + select.size + rows * wide),
            transcendentals=0,
        ),
        name="out_back",
    )


def piece(values, index, size):
    return lax.dynamic_slice_in_dim(values, index * size, size, 1)


class LineSum:
    def __init__(self, values, size, axis):
        self.axis = axis
        self.count = lax.axis_size(axis)
        self.pieces = [values[:, i * size : (i + 1) * size] for i in range(self.count)]
        self.step = 0
        self.got = None
        here = lax.axis_index(axis)
        self.valid = (here > 0, here < self.count - 1)

    def sends(self):
        self.step += 1
        step, count = self.step, self.count
        rights = [(i, i + 1) for i in range(step)]
        lefts = [(count - 1 - i, count - 2 - i) for i in range(step)]
        found = []
        for side, slot, pairs in ((0, step, rights), (1, count - step, lefts)):
            value = self.pieces[slot]
            if self.got is not None:
                value = (value.astype(F32) + self.arrived(side)).astype(BF16)
            found.append((value, self.axis, pairs, side))
        return found

    def arrived(self, side):
        return jnp.where(self.valid[side], self.got[side].astype(F32), 0.0)

    def loose(self):
        return self.step == 1 and self.count > 2

    def receive(self, results):
        self.got = results

    def result(self):
        assert self.step == self.count - 1
        total = self.pieces[0].astype(F32)
        for side in (0, 1) if self.got else ():
            total = total + self.arrived(side)
        return total


class LineGather:
    def __init__(self, own, axis):
        self.own, self.axis = own, axis
        self.count = lax.axis_size(axis)
        self.lefts, self.rights = [own], [own]

    def sends(self):
        step, count = len(self.lefts), self.count
        return [
            (self.lefts[-1], self.axis, [(i, i + 1) for i in range(step - 1, count - 1)], 0),
            (self.rights[-1], self.axis, [(i, i - 1) for i in range(count - step, 0, -1)], 1),
        ]

    def loose(self):
        return len(self.lefts) == self.count - 1 and self.count > 2

    def receive(self, results):
        self.lefts.append(results[0])
        self.rights.append(results[1])

    def result(self):
        count = self.count
        here = lax.axis_index(self.axis)
        assert len(self.lefts) == count
        others = [
            jnp.where(here >= step, self.lefts[step], self.rights[count - step])
            for step in range(1, count)
        ]
        return jnp.concatenate([self.own, *others], axis=1)


class EarlierGather:
    def __init__(self, own, axis):
        self.own, self.axis = own, axis
        self.count = lax.axis_size(axis)

    def sends(self):
        count = self.count
        return [
            (self.own, self.axis, [(i, i + step) for i in range(count - step)], None)
            for step in range(1, count)
        ]

    def receive(self, results):
        self.others = results

    def result(self):
        count, own = self.count, self.own
        here = lax.axis_index(self.axis)
        trees, rows, width = own.shape
        result = jnp.zeros((trees, count * rows, width), own.dtype)
        result = lax.dynamic_update_slice_in_dim(result, own, here * rows, 1)
        for step, other in enumerate(self.others, 1):
            slot = lax.rem(here - step + count, count)
            result = lax.dynamic_update_slice_in_dim(result, other, slot * rows, 1)
        return result


class EarlierReturn:
    def __init__(self, full, axis):
        self.full, self.axis = full, axis
        self.count = lax.axis_size(axis)
        self.rows = full.shape[1] // self.count

    def sends(self):
        count = self.count
        here = lax.axis_index(self.axis)
        found = []
        for step in range(1, count):
            slot = lax.rem(here - step + count, count)
            value = piece(self.full, slot, self.rows).astype(BF16)
            found.append((value, self.axis, [(i + step, i) for i in range(count - step)], None))
        return found

    def receive(self, results):
        self.others = results

    def result(self):
        total = piece(self.full, lax.axis_index(self.axis), self.rows)
        for other in self.others:
            total = total + other.astype(F32)
        return total


def ends(pairs, which):
    return {pair[which] for pair in pairs}


def disjoint(left, right):
    return not any(ends(left, which) & ends(right, which) for which in (0, 1))


def joined(sends, loose):
    groups = []
    for number, (value, axis, pairs, side) in enumerate(sends):
        for group in groups:
            if side is None or group.axis != axis or not disjoint(pairs, group.pairs):
                continue
            if group.side != side and not loose:
                continue
            here = lax.axis_index(axis)
            mine = functools.reduce(jnp.logical_or, [here == i for i in sorted(ends(pairs, 0))])
            group.value = jnp.where(mine, value, group.value)
            group.pairs = group.pairs + pairs
            group.members.append(number)
            break
        else:
            groups.append(
                SimpleNamespace(value=value, axis=axis, pairs=pairs, side=side, members=[number])
            )
    return groups


class Stages:
    def __init__(self):
        self.token = ()
        self.number = 0

    def wait_for(self, *values):
        self.token += values

    def __call__(self, transfers, compute=None, inputs=(), fused=False):
        self.number += 1
        kept = []
        for t in transfers:
            if t.count > 1:
                kept.append(t)
            else:
                t.receive([])
        small = [t for t in kept if fused and hasattr(t, "everyone")]
        transfers = [t for t in kept if t not in small]
        sends = [t.sends() for t in transfers]
        lines = [t for t in transfers if hasattr(t, "loose")]
        loose = len(lines) == 1 and lines[0].loose() and not fused
        groups = joined([send for of_one in sends for send in of_one], loose)
        values = [group.value for group in groups]
        tied = lax.optimization_barrier(
            (*values, *inputs, *[t.values for t in small], *self.token)
        )
        results = {}
        token = []
        by_kernel = []
        for value, group in zip(tied, groups):
            if fused and group.side is not None:
                by_kernel.append((value, group))
                continue
            other = lax.ppermute(value, group.axis, group.pairs)
            token.append(other)
            results.update({number: other for number in group.members})
        given = tied[len(groups) : len(groups) + len(inputs)]
        if by_kernel:
            line_sends = [(value, group.side) for value, group in by_kernel]
            first = len(groups) + len(inputs)
            for at, transfer in enumerate(small, first):
                line_sends.append((tied[at], transfer.axis))
            if compute is None:
                outs, others = hop_call(None, line_sends)
            else:
                outs, others = compute(*given, line_sends)
            token += others
            for other, (_, group) in zip(others, by_kernel):
                results.update({number: other for number in group.members})
            others = others[len(by_kernel) :]
            for transfer in small:
                transfer.receive(others[: transfer.count - 1])
                others = others[transfer.count - 1 :]
        else:
            outs = compute(*given) if compute else ()
        at = 0
        for transfer, of_one in zip(transfers, sends):
            transfer.receive([results[at + i] for i in range(len(of_one))])
            at += len(of_one)
        self.token = (*token, *outs)
        return outs


def turned(values, dim, axis):
    count = lax.axis_size(axis)
    here = lax.axis_index(axis)
    size = values.shape[dim] // count
    return jnp.concatenate(
        [
            lax.dynamic_slice_in_dim(
                values, lax.rem(here - i + count, count) * size, size, dim
            )
            for i in range(count)
        ],
        axis=dim,
    )


class SmallSum:
    everyone = True

    def __init__(self, values, axis):
        self.values, self.axis = values, axis
        self.count = lax.axis_size(axis)

    def sends(self):
        count = self.count
        return [
            (self.values, self.axis, [(i, (i + step) % count) for i in range(count)], None)
            for step in range(1, count)
        ]

    def receive(self, results):
        self.others = results

    def result(self):
        return sum(self.others, self.values)


def norm_back(grad, values, gain):
    root = lax.rsqrt(jnp.mean(values * values, axis=-1, keepdims=True) + EPS)
    weighted = grad * gain
    mean = jnp.mean(weighted * values, axis=-1, keepdims=True)
    return root * weighted - values * (root * root * root) * mean


def on_device(
    tokens, norm_one, q_weight, k_weight, v_weight, o_weight, norm_two,
    gate_weight, up_weight, down_weight, segment_ids, parent_ids, path_pos, cotangent,
):
    ctx = lax.axis_index("context")
    ctx_count = lax.axis_size("context")
    ten_count = lax.axis_size(HOP_AXIS)
    tree_count, rows, width = tokens.shape
    share = rows // ten_count
    trees = tree_count // MICRO
    flat = trees * rows
    part, q_width = q_weight.shape
    kv_width = k_weight.shape[1]
    q_heads = q_width // HEAD
    kv_heads = kv_width // HEAD
    used = q_width + 2 * kv_width
    packed_width = round_up(used + 2, LANES)

    attention_block = jnp.concatenate(
        [
            q_weight, k_weight, v_weight, norm_one[:, None], norm_two[:, None],
            jnp.zeros((part, packed_width - used - 2), BF16),
        ],
        axis=1,
    )
    attention_full = lax.all_gather(attention_block, WEIGHT_AXES, axis=0, tiled=True)
    o_full = lax.all_gather(o_weight.T, WEIGHT_AXES, axis=0, tiled=True)
    hidden = gate_weight.shape[1]
    wide = round_up(hidden, LANES)

    def widened(values):
        return jnp.pad(values, ((0, 0), (0, wide - hidden)))

    down_full = lax.all_gather(widened(down_weight.T), WEIGHT_AXES, axis=0, tiled=True)
    gate_up_block = jnp.concatenate([widened(gate_weight), widened(up_weight)], axis=1)
    gate_up_full = lax.all_gather(gate_up_block, WEIGHT_AXES, axis=0, tiled=True)
    gain_one = attention_full[:, used].astype(F32)
    gain_two = attention_full[:, used + 1].astype(F32)

    lane = np.arange(q_heads * LANES)
    column = np.arange(q_width)
    select = jnp.asarray(
        (lane[:, None] // LANES == column[None, :] // HEAD)
        & (lane[:, None] % LANES == column[None, :] % HEAD),
        BF16,
    )
    frequency = THETA ** (-(jnp.arange(HALF, dtype=F32) * 2.0 / HEAD))
    pad = jnp.zeros((flat, LANES - HEAD), F32)
    ctx_ref = jnp.reshape(ctx, (1,)).astype(jnp.int32)

    tokens = turned(tokens, 1, HOP_AXIS)
    cotangent = turned(cotangent, 1, HOP_AXIS)
    segment_ids, parent_ids, path_pos = [
        turned(ids.reshape(-1, ctx_count, rows), 2, HOP_AXIS).reshape(ids.shape)
        for ids in (segment_ids, parent_ids, path_pos)
    ]
    state = []
    for micro in range(MICRO):
        pick = slice(micro * trees, (micro + 1) * trees)
        m = SimpleNamespace()
        state.append(m)
        m.number = micro
        m.x = tokens[pick]
        m.dy = cotangent[pick]
        seg, par, pos = segment_ids[pick], parent_ids[pick], path_pos[pick]

        def here(ids):
            return lax.dynamic_slice_in_dim(ids, ctx * rows, rows, 1)

        m.ids = (
            here(seg)[:, :, None], here(par)[:, :, None], here(pos)[:, :, None],
            seg[:, None, :], pos[:, None, :],
        )
        angles = here(pos).reshape(flat).astype(F32)[:, None] * frequency[None, :]
        cosine, sine = jnp.cos(angles), jnp.sin(angles)
        m.cos = jnp.concatenate([cosine, cosine, pad], axis=1)
        m.sin = jnp.concatenate([-sine, sine, pad], axis=1)
        x = m.x.reshape(flat, width).astype(F32)
        m.root_one = lax.rsqrt(jnp.mean(x * x, axis=-1, keepdims=True) + EPS)
        m.x_here = m.x[:, :share].astype(F32)
        m.dy_here = m.dy[:, :share].astype(F32)

    def together(*parts):
        return jnp.concatenate([part.reshape(flat, -1) for part in parts], axis=0)

    def shaped(product):
        return product.reshape(trees, rows, width)

    x_all = tokens.reshape(-1, width).astype(F32)
    root_all = jnp.concatenate([m.root_one for m in state], axis=0)
    normed_all = (x_all * root_all * gain_one).astype(BF16)
    stage = Stages()
    a, b = state

    def project(m):
        def run(root):
            at = m.number * flat
            packed = mm(normed_all[at : at + flat], attention_full)
            m.q, kv = split_heads(packed, m.cos, m.sin, q_heads, kv_heads, rows)
            m.kv = EarlierGather(kv.reshape(trees, rows, -1), "context")
            return (m.q,)

        return run

    def attend(m):
        def run(q):
            m.kv_full = m.kv.result()
            wide = attend_forward(ctx_ref, q, m.kv_full, m.ids, q_heads, kv_heads, rows)
            m.attended = mm(wide, select).astype(BF16)
            product = mm_nt(m.attended, o_full).astype(BF16)
            m.sum1 = LineSum(shaped(product), share, HOP_AXIS)
            return (product,)

        return run

    def mixed_back(m):
        def run(dy):
            m.dmixed = row_major(mm(dy.reshape(flat, width), down_full))
            return (m.dmixed,)

        return run

    def norm_two_of(m):
        middle = m.x_here + m.sum1.result()
        root = lax.rsqrt(jnp.mean(middle * middle, axis=-1, keepdims=True) + EPS)
        m.middle, m.root_two = middle, root
        m.gather1 = LineGather((middle * root * gain_two).astype(BF16), HOP_AXIS)

    def feed_forward(m):
        def run(normed_two, sends):
            m.normed_two = normed_two
            (m.mixed, m.dgate, m.dup), others = feed_forward_hidden(
                normed_two, gate_up_full, m.dmixed, sends
            )
            return (m.mixed, m.dgate, m.dup), others

        return run

    def back_of(m):
        def run(dgate, sends):
            (product, out), others = feed_back(
                dgate, m.dup, m.mixed, gate_up_full, down_full, sends
            )
            m.sum3 = LineSum(shaped(product), share, HOP_AXIS)
            m.out_part = shaped(out)
            return (product, out), others

        return run

    def norm_two_back(m):
        middle, dn2 = m.middle, m.sum3.result()
        m.gain_two_grad = jnp.sum(dn2 * middle * m.root_two, axis=(0, 1))
        m.dmiddle = m.dy_here + norm_back(dn2, middle, gain_two)
        m.gather2 = LineGather(m.dmiddle.astype(BF16), HOP_AXIS)

    def attended_back(m):
        def run(dmb, sends):
            m.dmb = dmb
            (m.do,), others = out_back(dmb, o_full, select, sends)
            return (m.do,), others

        return run

    def attend_back(m):
        def run(do_wide, sends):
            (m.dq, dk, dv), others = attend_backward(
                m.q, m.kv_full, do_wide, m.ids, q_heads, kv_heads, rows, sends
            )
            m.dkv = EarlierReturn(jnp.concatenate([dk, dv], axis=2), "context")
            return (m.dq,), others

        return run

    def norm_one_back(m):
        def run(dq, sends):
            dkv = m.dkv.result().reshape(flat, -1)
            (m.dqkv, dn1, gain), others = pack_heads(
                *(dq, dkv, m.cos, m.sin, attention_full, m.x.reshape(flat, width), m.root_one),
                *(q_heads, kv_heads, sends),
            )
            m.gain_one_grad = gain[0]
            m.sum4 = LineSum(shaped(dn1), share, HOP_AXIS)
            return (m.dqkv, dn1), others

        return run

    class WeightGrad:
        def __init__(self, right_of):
            self.right_of = right_of

        def __call__(self, left):
            self.grad = row_major(mm_tn(left, self.right_of()).astype(BF16))
            return (self.grad,)

        def scattered(self):
            return lax.psum_scatter(self.grad, WEIGHT_AXES, scatter_dimension=0, tiled=True)

    def gathered(transfer):
        return transfer.result().reshape(flat, width)

    stage([], project(a), [a.root_one])
    stage([a.kv], project(b), [b.root_one])
    stage([b.kv], attend(a), [a.q])
    stage([a.sum1], attend(b), [b.q])
    stage([a.sum1], fused=True)
    stage([a.sum1], mixed_back(a), [a.dy])
    norm_two_of(a)
    stage([a.gather1], mixed_back(b), [b.dy])
    stage([a.gather1, b.sum1], fused=True)
    stage([a.gather1, b.sum1], fused=True)
    stage([b.sum1], fused=True)
    norm_two_of(b)
    stage([b.gather1], feed_forward(a), [gathered(a.gather1)], fused=True)
    stage([b.gather1], back_of(a), [a.dgate], fused=True)
    stage([b.gather1, a.sum3], fused=True)
    stage([a.sum3], feed_forward(b), [gathered(b.gather1)], fused=True)
    dy_all = cotangent.reshape(-1, width)
    mixed_all = together(a.mixed, b.mixed)
    down_grad = WeightGrad(lambda: mixed_all)
    stage([a.sum3], down_grad, [dy_all])
    down_grad = down_grad.scattered()
    norm_two_back(a)
    a.sum2 = LineSum(a.out_part, share, HOP_AXIS)
    stage([a.gather2, a.sum2], back_of(b), [b.dgate], fused=True)
    b.sum2 = LineSum(b.out_part, share, HOP_AXIS)
    gate_up_grad = WeightGrad(
        lambda: jnp.concatenate([together(a.dgate, b.dgate), together(a.dup, b.dup)], axis=1)
    )
    stage([a.gather2, b.sum3], gate_up_grad, [together(a.normed_two, b.normed_two)])
    gate_up_grad = gate_up_grad.scattered()
    stage([a.gather2, b.sum3], fused=True)
    stage([b.sum3], attended_back(a), [gathered(a.gather2)], fused=True)
    norm_two_back(b)
    stage([b.gather2], attend_back(a), [a.do], fused=True)
    stage([b.gather2, b.sum2, a.dkv], fused=True)
    stage([b.gather2, a.sum2], norm_one_back(a), [a.dq], fused=True)
    stage.wait_for(down_grad)
    stage([a.sum4], attended_back(b), [gathered(b.gather2)], fused=True)
    stage([a.sum4, a.sum2], attend_back(b), [b.do], fused=True)
    stage.wait_for(gate_up_grad)
    o_grad = WeightGrad(lambda: together(a.attended, b.attended))
    stage([a.sum4, b.dkv], o_grad, [together(a.dmb, b.dmb)])
    o_grad = o_grad.scattered()
    stage([b.sum2], norm_one_back(b), [b.dq], fused=True)
    gains = jnp.stack([a.gain_one_grad + b.gain_one_grad, a.gain_two_grad + b.gain_two_grad])
    gains = SmallSum(gains, HOP_AXIS)
    attention_grad = WeightGrad(lambda: together(a.dqkv, b.dqkv))
    stage([], attention_grad, [normed_all])
    attention_grad = attention_grad.scattered().astype(F32)
    stage([b.sum4, b.sum2, gains], fused=True)
    gains = SmallSum(gains.result(), "context")
    stage([b.sum4, gains], fused=True)
    stage.wait_for(o_grad)
    gains = SmallSum(gains.result(), "fsdp")
    stage([b.sum4, gains], fused=True)
    block = lax.axis_index("fsdp") * ctx_count + ctx
    gains = lax.dynamic_slice_in_dim(gains.result(), block * part, part, 1)
    for m in state:
        m.out_sum = m.sum2.result()
    for m in state:
        middle, out_sum = lax.optimization_barrier((m.middle, m.out_sum))
        m.out = (middle + out_sum.astype(F32)).astype(BF16)
        m.dx = (m.dmiddle + norm_back(m.sum4.result(), m.x_here, gain_one)).astype(BF16)

    return (
        jnp.concatenate([m.out for m in state], axis=0),
        jnp.concatenate([m.dx for m in state], axis=0),
        gains[0],
        attention_grad[:, :q_width],
        attention_grad[:, q_width : q_width + kv_width],
        attention_grad[:, q_width + kv_width : used],
        o_grad.T.astype(F32),
        gains[1],
        gate_up_grad[:, :hidden].astype(F32),
        gate_up_grad[:, wide : wide + hidden].astype(F32),
        down_grad[:, :hidden].T.astype(F32),
    )


def solution(mesh):
    HOP_IDS.clear()
    weights = WEIGHT_AXES
    return jax.shard_map(
        on_device,
        mesh=mesh,
        in_specs=(
            P("fsdp", "context", None),
            P(weights),
            P(weights, "tensor"),
            P(weights, "tensor"),
            P(weights, "tensor"),
            P("tensor", weights),
            P(weights),
            P(weights, "tensor"),
            P(weights, "tensor"),
            P("tensor", weights),
            P("fsdp", None),
            P("fsdp", None),
            P("fsdp", None),
            P("fsdp", "context", None),
        ),
        out_specs=(
            P("fsdp", ("context", "tensor"), None),
            P("fsdp", ("context", "tensor"), None),
            P(weights),
            P(weights, "tensor"),
            P(weights, "tensor"),
            P(weights, "tensor"),
            P("tensor", weights),
            P(weights),
            P(weights, "tensor"),
            P(weights, "tensor"),
            P("tensor", weights),
        ),
        check_vma=False,
    )
```

```python
import functools
from types import SimpleNamespace

import jax
import jax.numpy as jnp
import numpy as np
from jax import lax
from jax.experimental import pallas as pl
from jax.experimental.pallas import tpu as pltpu
from jax.experimental.layout import Layout, with_layout_constraint
from jax.sharding import PartitionSpec as P


HEAD = 80
HALF = HEAD // 2
LANES = 128
MICRO = 2
EPS = 1e-05
THETA = 10000.0
NEG = -1000000000.0
TRUNK = 512
WEIGHT_AXES = ("fsdp", "context")
BF16 = jnp.bfloat16
F32 = jnp.float32


def row_major(value):
    return with_layout_constraint(value, Layout(major_to_minor=(0, 1)))


def round_up(value, unit):
    return (value + unit - 1) // unit * unit


def mm(left, right):
    return lax.dot_general(left, right, (((1,), (0,)), ((), ())), preferred_element_type=F32)


def mm_nt(left, right):
    return lax.dot_general(left, right, (((1,), (1,)), ((), ())), preferred_element_type=F32)


def mm_tn(left, right):
    return lax.dot_general(left, right, (((0,), (0,)), ((), ())), preferred_element_type=F32)


def rotated(values, cos_table, sin_table):
    lane = lax.broadcasted_iota(jnp.int32, values.shape, 1)
    swapped = jnp.where(
        lane < HALF, pltpu.roll(values, LANES - HALF, 1), pltpu.roll(values, HALF, 1)
    )
    return values * cos_table + swapped * sin_table


def window_of(head):
    start = head * HEAD
    base = start // LANES * LANES
    return base, start - base


def split_kernel(q_heads, kv_heads, x_ref, cos_ref, sin_ref, q_ref, kv_ref):
    cos_table = cos_ref[...]
    sin_table = sin_ref[...]
    for head in range(q_heads + 2 * kv_heads):
        base, shift = window_of(head)
        window = x_ref[:, base : base + 2 * LANES]
        if shift:
            window = pltpu.roll(window, 2 * LANES - shift, 1)
        values = window[:, :LANES]
        if head < q_heads + kv_heads:
            result = rotated(values, cos_table, sin_table)
        else:
            lane = lax.broadcasted_iota(jnp.int32, values.shape, 1)
            result = jnp.where(lane < HEAD, values, 0.0)
        result = result.astype(BF16)
        if head < q_heads:
            q_ref[:, head * LANES : (head + 1) * LANES] = result
        else:
            at = (head - q_heads) * LANES
            kv_ref[:, at : at + LANES] = result


def split_heads(packed, cos_table, sin_table, q_heads, kv_heads, rows):
    total, width = packed.shape
    q_wide = q_heads * LANES
    kv_wide = 2 * kv_heads * LANES
    return pl.pallas_call(
        functools.partial(split_kernel, q_heads, kv_heads),
        grid=(total // rows,),
        in_specs=[
            pl.BlockSpec((rows, width), lambda b: (b, 0)),
            pl.BlockSpec((rows, LANES), lambda b: (b, 0)),
            pl.BlockSpec((rows, LANES), lambda b: (b, 0)),
        ],
        out_specs=[
            pl.BlockSpec((rows, q_wide), lambda b: (b, 0)),
            pl.BlockSpec((rows, kv_wide), lambda b: (b, 0)),
        ],
        out_shape=[
            jax.ShapeDtypeStruct((total, q_wide), BF16),
            jax.ShapeDtypeStruct((total, kv_wide), BF16),
        ],
        cost_estimate=pl.CostEstimate(
            flops=10 * total * width, bytes_accessed=7 * total * width, transcendentals=0
        ),
        name="split_heads",
    )(packed, cos_table, sin_table)


def fill_bias(seg_q, par_q, pos_q, seg_k, pos_k, bias_ref):
    same = (seg_k == seg_q) | (seg_k == par_q) | (seg_k == 0)
    bias_ref[...] = jnp.where(same & (pos_k <= pos_q), 0.0, NEG)


def probabilities(q_block, keys, bias):
    scores = mm_nt(q_block, keys) * HEAD ** (-0.5) + bias
    top = jnp.max(scores, axis=1, keepdims=True)
    raised = jnp.exp(scores - top)
    return raised * (1.0 / jnp.sum(raised, axis=1, keepdims=True))


def forward_kernel(
    rows, tree_len, block,
    ctx_ref, q_ref, k_ref, v_ref, seg_q, par_q, pos_q, seg_k, pos_k, out_ref, bias_ref,
):
    @pl.when(pl.program_id(1) == 0)
    def _():
        fill_bias(seg_q[0], par_q[0], pos_q[0], seg_k[0], pos_k[0], bias_ref)

    in_trunk = (ctx_ref[0] + 1) * rows <= TRUNK

    def run(keys):
        @pl.loop(0, rows // block)
        def _(step):
            at = pl.ds(pl.multiple_of(step * block, block), block)
            probs = probabilities(q_ref[at, :], k_ref[0, :keys, :], bias_ref[at, :keys])
            out_ref[at, :] = mm(probs.astype(BF16), v_ref[0, :keys, :]).astype(BF16)

    pl.when(in_trunk)(lambda: run(min(TRUNK, tree_len)))
    pl.when(jnp.logical_not(in_trunk))(lambda: run(tree_len))


def backward_kernel(
    rows, tree_len, block, group,
    q_ref, k_ref, v_ref, do_ref, seg_q, par_q, pos_q, seg_k, pos_k,
    dq_ref, dk_ref, dv_ref, bias_ref,
):
    head = pl.program_id(1)

    @pl.when(head == 0)
    def _():
        fill_bias(seg_q[0], par_q[0], pos_q[0], seg_k[0], pos_k[0], bias_ref)

    @pl.when(lax.rem(head, group) == 0)
    def _():
        dk_ref[...] = jnp.zeros_like(dk_ref)
        dv_ref[...] = jnp.zeros_like(dv_ref)

    in_trunk = (lax.axis_index("context") + 1) * rows <= TRUNK
    scale = HEAD ** (-0.5)

    def run(keys):
        @pl.loop(0, rows // block)
        def _(step):
            at = pl.ds(pl.multiple_of(step * block, block), block)
            q_block = q_ref[at, :]
            do_block = do_ref[at, :]
            k_all = k_ref[0, :keys, :]
            probs = probabilities(q_block, k_all, bias_ref[at, :keys])
            dprobs = mm_nt(do_block, v_ref[0, :keys, :])
            delta = jnp.sum(probs * dprobs, axis=1, keepdims=True)
            dscores = (probs * (dprobs - delta)).astype(BF16)
            dq_ref[at, :] = (mm(dscores, k_all) * scale).astype(BF16)
            dk_ref[0, :keys, :] += mm_tn(dscores, q_block) * scale
            dv_ref[0, :keys, :] += mm_tn(probs.astype(BF16), do_block)

    pl.when(in_trunk)(lambda: run(min(TRUNK, tree_len)))
    pl.when(jnp.logical_not(in_trunk))(lambda: run(tree_len))


def attention_specs(rows, tree_len, group, kv_heads):
    def column(b, h, *c):
        return (b, h)

    def whole(b, h, *c):
        return (b, 0, 0)

    return [
        pl.BlockSpec((rows, LANES), column),
        pl.BlockSpec((1, tree_len, LANES), lambda b, h, *c: (b, 0, h // group)),
        pl.BlockSpec((1, tree_len, LANES), lambda b, h, *c: (b, 0, kv_heads + h // group)),
    ], [
        pl.BlockSpec((1, rows, 1), whole),
        pl.BlockSpec((1, rows, 1), whole),
        pl.BlockSpec((1, rows, 1), whole),
        pl.BlockSpec((1, 1, tree_len), whole),
        pl.BlockSpec((1, 1, tree_len), whole),
    ]


def attend_forward(ctx, q_wide, kv_full, ids, q_heads, kv_heads, rows):
    trees, tree_len, _ = kv_full.shape
    group = q_heads // kv_heads
    first, last = attention_specs(rows, tree_len, group, kv_heads)
    block = min(rows, 256)
    work = trees * q_heads * rows * tree_len
    return pl.pallas_call(
        functools.partial(forward_kernel, rows, tree_len, block),
        grid_spec=pltpu.PrefetchScalarGridSpec(
            num_scalar_prefetch=1,
            grid=(trees, q_heads),
            in_specs=first + last,
            out_specs=pl.BlockSpec((rows, LANES), lambda b, h, c: (b, h)),
            scratch_shapes=[pltpu.VMEM((rows, tree_len), F32)],
        ),
        out_shape=jax.ShapeDtypeStruct(q_wide.shape, BF16),
        cost_estimate=pl.CostEstimate(
            flops=4 * LANES * work, bytes_accessed=8 * q_wide.size, transcendentals=work
        ),
        name="attend_forward",
    )(ctx, q_wide, kv_full, kv_full, *ids)


HOP_AXIS = "tensor"


def with_hops(kernel, counts, sides, *refs):
    own_in, own_out, own_scratch = counts
    sends = len(sides)
    ends_at = []
    for size in (own_in, sends, own_out, sends, own_scratch):
        ends_at.append((ends_at[-1] if ends_at else 0) + size)
    ins, sent, outs, received, scratch = (
        refs[low:high] for low, high in zip([0, *ends_at], ends_at)
    )
    send_sem, recv_sem = refs[ends_at[-1] :]
    here = lax.axis_index(HOP_AXIS)
    count = lax.axis_size(HOP_AXIS)
    has_next, has_last = here < count - 1, here > 0

    def copy(number):
        other = here + 1 - 2 * sides[number]
        return pltpu.make_async_remote_copy(
            src_ref=sent[number],
            dst_ref=received[number],
            send_sem=send_sem.at[number],
            recv_sem=recv_sem.at[number],
            device_id={HOP_AXIS: other},
            device_id_type=pl.DeviceIdType.MESH,
        )

    first, last = None, None
    if own_in:
        first, last = jnp.bool_(True), jnp.bool_(True)
        for axis in range(GRID_RANK[kernel]):
            first &= pl.program_id(axis) == 0
            last &= pl.program_id(axis) == pl.num_programs(axis) - 1

    def start():
        barrier = pltpu.get_barrier_semaphore()
        for there, step in ((has_next, 1), (has_last, -1)):

            @pl.when(there)
            def _():
                pl.semaphore_signal(
                    barrier,
                    inc=1,
                    device_id={HOP_AXIS: here + step},
                    device_id_type=pl.DeviceIdType.MESH,
                )

        pl.semaphore_wait(barrier, has_next.astype(jnp.int32) + has_last.astype(jnp.int32))
        for number, side in enumerate(sides):
            pl.when((has_next, has_last)[side])(lambda number=number: copy(number).start())

    def finish():
        for number, side in enumerate(sides):
            pl.when((has_next, has_last)[side])(lambda number=number: copy(number).wait_send())
            pl.when((has_last, has_next)[side])(lambda number=number: copy(number).wait_recv())

    if own_in:
        pl.when(first)(start)
        kernel(*ins, *outs, *scratch)
        pl.when(last)(finish)
    else:
        start()
        finish()


GRID_RANK = {}
HOP_IDS = {}


def hop_call(kernel, sends, *args, grid=(), in_specs=(), out_specs=(), out_shape=(),
             scratch_shapes=(), name="hop", cost_estimate=None):
    sides = tuple(side for _, side in sends)
    values = [value for value, _ in sends]
    anywhere = pl.BlockSpec(memory_space=pl.ANY)
    if kernel is not None:
        GRID_RANK[kernel] = len(grid)
    counts = (len(args), len(out_shape), len(scratch_shapes))
    key = (name, sides, tuple(v.shape for v in (*values, *args)))
    results = pl.pallas_call(
        functools.partial(with_hops, kernel, counts, sides),
        grid=grid,
        in_specs=[*in_specs, *[anywhere] * len(values)],
        out_specs=[*out_specs, *[anywhere] * len(values)],
        out_shape=[*out_shape, *[jax.ShapeDtypeStruct(v.shape, v.dtype) for v in values]],
        scratch_shapes=[
            *scratch_shapes,
            pltpu.SemaphoreType.DMA((len(values),)),
            pltpu.SemaphoreType.DMA((len(values),)),
        ],
        compiler_params=pltpu.CompilerParams(
            collective_id=HOP_IDS.setdefault(key, len(HOP_IDS)), has_side_effects=True
        ),
        cost_estimate=cost_estimate,
    )(*args, *values)
    return results[: len(out_shape)], results[len(out_shape) :]


def attend_backward(q_wide, kv_full, do_wide, ids, q_heads, kv_heads, rows, sends):
    trees, tree_len, _ = kv_full.shape
    group = q_heads // kv_heads
    first, last = attention_specs(rows, tree_len, group, kv_heads)
    block = min(rows, 256)
    work = trees * q_heads * rows * tree_len
    grad_spec = pl.BlockSpec((1, tree_len, LANES), lambda b, h: (b, 0, h // group))
    grad_shape = jax.ShapeDtypeStruct((trees, tree_len, kv_heads * LANES), F32)
    return hop_call(
        functools.partial(backward_kernel, rows, tree_len, block, group),
        sends,
        *(q_wide, kv_full, kv_full, do_wide, *ids),
        grid=(trees, q_heads),
        in_specs=first + [first[0]] + last,
        out_specs=[first[0], grad_spec, grad_spec],
        out_shape=[jax.ShapeDtypeStruct(q_wide.shape, BF16), grad_shape, grad_shape],
        scratch_shapes=[pltpu.VMEM((rows, tree_len), F32)],
        cost_estimate=pl.CostEstimate(
            flops=10 * LANES * work, bytes_accessed=12 * q_wide.size, transcendentals=work
        ),
        name="attend_backward",
    )


def pack_kernel(
    q_heads, kv_heads, dq_ref, dkv_ref, cos_ref, sin_ref, weight, packed_ref, product_ref, sum_ref
):
    @pl.when(pl.program_id(0) == 0)
    def _():
        cos_table = cos_ref[...]
        sin_table = -sin_ref[...]
        sum_ref[...] = jnp.zeros_like(sum_ref)
        for head in range(q_heads + 2 * kv_heads):
            base, shift = window_of(head)
            if head < q_heads:
                values = dq_ref[:, head * LANES : (head + 1) * LANES].astype(F32)
            else:
                at = (head - q_heads) * LANES
                values = dkv_ref[:, at : at + LANES].astype(BF16).astype(F32)
            if head < q_heads + kv_heads:
                values = rotated(values, cos_table, sin_table)
            wide = jnp.concatenate([values, jnp.zeros_like(values)], axis=1)
            if shift:
                wide = pltpu.roll(wide, shift, 1)
            sum_ref[:, base : base + 2 * LANES] += wide
        packed_ref[...] = sum_ref[...].astype(BF16)

    product_ref[...] = mm_nt(packed_ref[...], weight[...]).astype(BF16)


def pack_heads(dq_wide, dkv, cos_table, sin_table, weight, q_heads, kv_heads, sends):
    rows = dq_wide.shape[0]
    width, packed = weight.shape
    tile = width // 5

    def whole(values):
        return pl.BlockSpec(values.shape, lambda i: (0, 0))

    return hop_call(
        functools.partial(pack_kernel, q_heads, kv_heads),
        sends,
        *(dq_wide, dkv, cos_table, sin_table, weight),
        grid=(width // tile,),
        in_specs=[
            whole(dq_wide), whole(dkv), whole(cos_table), whole(sin_table),
            pl.BlockSpec((tile, packed), lambda i: (i, 0)),
        ],
        out_specs=[
            pl.BlockSpec((rows, packed), lambda i: (0, 0)),
            pl.BlockSpec((rows, tile), lambda i: (0, i)),
        ],
        out_shape=[
            jax.ShapeDtypeStruct((rows, packed), BF16),
            jax.ShapeDtypeStruct((rows, width), BF16),
        ],
        scratch_shapes=[pltpu.VMEM((rows, packed), F32)],
        cost_estimate=pl.CostEstimate(
            flops=2 * rows * width * packed,
            bytes_accessed=2 * width * packed + 8 * rows * packed + 2 * rows * width,
            transcendentals=0,
        ),
        name="pack_heads",
    )


def weight_grad_kernel(left, right, grad_ref):
    grad_ref[...] = mm_tn(left[...], right[...]).astype(BF16)


def weight_grad(left, right, sends):
    rows, width = left.shape
    columns = right.shape[1]
    tile = width // 5
    return hop_call(
        weight_grad_kernel,
        sends,
        *(left, right),
        grid=(width // tile,),
        in_specs=[
            pl.BlockSpec((rows, tile), lambda i: (0, i)),
            pl.BlockSpec((rows, columns), lambda i: (0, 0)),
        ],
        out_specs=[pl.BlockSpec((tile, columns), lambda i: (i, 0))],
        out_shape=[jax.ShapeDtypeStruct((width, columns), BF16)],
        cost_estimate=pl.CostEstimate(
            flops=2 * rows * width * columns,
            bytes_accessed=2 * (left.size + right.size + width * columns),
            transcendentals=0,
        ),
        name="weight_grad",
    )


def feed_forward_kernel(normed, gate_w, up_w, dmixed, mixed_ref, dgate_ref, dup_ref):
    gate = mm(normed[...], gate_w[...])
    up = mm(normed[...], up_w[...])
    sigmoid = 1.0 / (1.0 + jnp.exp(-gate))
    silu = gate * sigmoid
    slope = sigmoid * (1.0 + gate * (1.0 - sigmoid))
    mixed_ref[...] = (silu * up).astype(BF16)
    dgate_ref[...] = (dmixed[...] * up * slope).astype(BF16)
    dup_ref[...] = (dmixed[...] * silu).astype(BF16)


def feed_forward_hidden(normed, gate_up_w, dmixed, sends):
    rows, width = normed.shape
    hidden = dmixed.shape[1]
    tile = 2 * LANES
    count = hidden // tile
    result = pl.BlockSpec((rows, tile), lambda i: (0, i))
    return hop_call(
        feed_forward_kernel,
        sends,
        *(normed, gate_up_w, gate_up_w, dmixed),
        grid=(count,),
        in_specs=[
            pl.BlockSpec((rows, width), lambda i: (0, 0)),
            pl.BlockSpec((width, tile), lambda i: (0, i)),
            pl.BlockSpec((width, tile), lambda i: (0, i + count)),
            result,
        ],
        out_specs=[result] * 3,
        out_shape=[jax.ShapeDtypeStruct((rows, hidden), BF16)] * 3,
        cost_estimate=pl.CostEstimate(
            flops=4 * rows * hidden * width,
            bytes_accessed=4 * hidden * width + 2 * rows * width + 10 * rows * hidden,
            transcendentals=rows * hidden,
        ),
        name="feed_forward",
    )


def feed_back_kernel(dgate, dup, mixed, gate_w, up_w, down_w, dn2_ref, out_ref):
    dn2 = mm_nt(dgate[...], gate_w[...]) + mm_nt(dup[...], up_w[...])
    dn2_ref[...] = dn2.astype(BF16)
    out_ref[...] = mm_nt(mixed[...], down_w[...]).astype(BF16)


def feed_back(dgate, dup, mixed, gate_up_w, down_w, sends):
    rows, hidden = mixed.shape
    width = down_w.shape[0]
    tile = width // 5
    left = pl.BlockSpec((rows, hidden), lambda i: (0, 0))
    right = pl.BlockSpec((tile, hidden), lambda i: (i, 0))
    result = pl.BlockSpec((rows, tile), lambda i: (0, i))
    return hop_call(
        feed_back_kernel,
        sends,
        *(dgate, dup, mixed, gate_up_w, gate_up_w, down_w),
        grid=(width // tile,),
        in_specs=[
            *[left] * 3,
            right,
            pl.BlockSpec((tile, hidden), lambda i: (i, 1)),
            right,
        ],
        out_specs=[result] * 2,
        out_shape=[jax.ShapeDtypeStruct((rows, width), BF16)] * 2,
        cost_estimate=pl.CostEstimate(
            flops=6 * rows * hidden * width,
            bytes_accessed=6 * hidden * (rows + width) + 4 * rows * width,
            transcendentals=0,
        ),
        name="feed_back",
    )


def out_back_kernel(grad, weight, select, result_ref):
    narrow = mm(grad[...], weight[...]).astype(BF16)
    result_ref[...] = mm_nt(narrow, select[...]).astype(BF16)


def out_back(grad, weight, select, sends):
    rows, wide = grad.shape[0], select.shape[0]

    def whole(values):
        return pl.BlockSpec(values.shape, lambda i: (0, 0))

    return hop_call(
        out_back_kernel,
        sends,
        *(grad, weight, select),
        grid=(1,),
        in_specs=[whole(grad), whole(weight), whole(select)],
        out_specs=[pl.BlockSpec((rows, wide), lambda i: (0, 0))],
        out_shape=[jax.ShapeDtypeStruct((rows, wide), BF16)],
        cost_estimate=pl.CostEstimate(
            flops=2 * rows * weight.size + 2 * rows * select.size,
            bytes_accessed=2 * (grad.size + weight.size + select.size + rows * wide),
            transcendentals=0,
        ),
        name="out_back",
    )


def piece(values, index, size):
    return lax.dynamic_slice_in_dim(values, index * size, size, 1)


class LineSum:
    def __init__(self, values, size, axis):
        self.axis = axis
        self.count = lax.axis_size(axis)
        self.pieces = [values[:, i * size : (i + 1) * size] for i in range(self.count)]
        self.step = 0
        self.got = None
        here = lax.axis_index(axis)
        self.valid = (here > 0, here < self.count - 1)

    def sends(self):
        self.step += 1
        step, count = self.step, self.count
        rights = [(i, i + 1) for i in range(step)]
        lefts = [(count - 1 - i, count - 2 - i) for i in range(step)]
        found = []
        for side, slot, pairs in ((0, step, rights), (1, count - step, lefts)):
            value = self.pieces[slot]
            if self.got is not None:
                value = (value.astype(F32) + self.arrived(side)).astype(BF16)
            found.append((value, self.axis, pairs, side))
        return found

    def arrived(self, side):
        return jnp.where(self.valid[side], self.got[side].astype(F32), 0.0)

    def loose(self):
        return self.step == 1 and self.count > 2

    def receive(self, results):
        self.got = results

    def result(self):
        assert self.step == self.count - 1
        total = self.pieces[0].astype(F32)
        for side in (0, 1) if self.got else ():
            total = total + self.arrived(side)
        return total


class LineGather:
    def __init__(self, own, axis):
        self.own, self.axis = own, axis
        self.count = lax.axis_size(axis)
        self.lefts, self.rights = [own], [own]

    def sends(self):
        step, count = len(self.lefts), self.count
        return [
            (self.lefts[-1], self.axis, [(i, i + 1) for i in range(step - 1, count - 1)], 0),
            (self.rights[-1], self.axis, [(i, i - 1) for i in range(count - step, 0, -1)], 1),
        ]

    def loose(self):
        return len(self.lefts) == self.count - 1 and self.count > 2

    def receive(self, results):
        self.lefts.append(results[0])
        self.rights.append(results[1])

    def result(self):
        count = self.count
        here = lax.axis_index(self.axis)
        assert len(self.lefts) == count
        others = [
            jnp.where(here >= step, self.lefts[step], self.rights[count - step])
            for step in range(1, count)
        ]
        return jnp.concatenate([self.own, *others], axis=1)


class EarlierGather:
    def __init__(self, own, axis):
        self.own, self.axis = own, axis
        self.count = lax.axis_size(axis)

    def sends(self):
        count = self.count
        return [
            (self.own, self.axis, [(i, i + step) for i in range(count - step)], None)
            for step in range(1, count)
        ]

    def receive(self, results):
        self.others = results

    def result(self):
        count, own = self.count, self.own
        here = lax.axis_index(self.axis)
        trees, rows, width = own.shape
        result = jnp.zeros((trees, count * rows, width), own.dtype)
        result = lax.dynamic_update_slice_in_dim(result, own, here * rows, 1)
        for step, other in enumerate(self.others, 1):
            slot = lax.rem(here - step + count, count)
            result = lax.dynamic_update_slice_in_dim(result, other, slot * rows, 1)
        return result


class EarlierReturn:
    def __init__(self, full, axis):
        self.full, self.axis = full, axis
        self.count = lax.axis_size(axis)
        self.rows = full.shape[1] // self.count

    def sends(self):
        count = self.count
        here = lax.axis_index(self.axis)
        found = []
        for step in range(1, count):
            slot = lax.rem(here - step + count, count)
            value = piece(self.full, slot, self.rows).astype(BF16)
            found.append((value, self.axis, [(i + step, i) for i in range(count - step)], None))
        return found

    def receive(self, results):
        self.others = results

    def result(self):
        total = piece(self.full, lax.axis_index(self.axis), self.rows)
        for other in self.others:
            total = total + other.astype(F32)
        return total


def ends(pairs, which):
    return {pair[which] for pair in pairs}


def disjoint(left, right):
    return not any(ends(left, which) & ends(right, which) for which in (0, 1))


def joined(sends, loose):
    groups = []
    for number, (value, axis, pairs, side) in enumerate(sends):
        for group in groups:
            if side is None or group.axis != axis or not disjoint(pairs, group.pairs):
                continue
            if group.side != side and not loose:
                continue
            here = lax.axis_index(axis)
            mine = functools.reduce(jnp.logical_or, [here == i for i in sorted(ends(pairs, 0))])
            group.value = jnp.where(mine, value, group.value)
            group.pairs = group.pairs + pairs
            group.members.append(number)
            break
        else:
            groups.append(
                SimpleNamespace(value=value, axis=axis, pairs=pairs, side=side, members=[number])
            )
    return groups


class Stages:
    def __init__(self):
        self.token = ()
        self.number = 0

    def wait_for(self, *values):
        self.token += values

    def __call__(self, transfers, compute=None, inputs=(), fused=False):
        self.number += 1
        kept = []
        for t in transfers:
            if t.count > 1:
                kept.append(t)
            else:
                t.receive([])
        transfers = kept
        sends = [t.sends() for t in transfers]
        lines = [t for t in transfers if hasattr(t, "loose")]
        loose = len(lines) == 1 and lines[0].loose() and not fused
        groups = joined([send for of_one in sends for send in of_one], loose)
        values = [group.value for group in groups]
        tied = lax.optimization_barrier((*values, *inputs, *self.token))
        results = {}
        token = []
        by_kernel = []
        for value, group in zip(tied, groups):
            if fused and group.side is not None:
                by_kernel.append((value, group))
                continue
            other = lax.ppermute(value, group.axis, group.pairs)
            token.append(other)
            results.update({number: other for number in group.members})
        given = tied[len(groups) : len(groups) + len(inputs)]
        if by_kernel:
            line_sends = [(value, group.side) for value, group in by_kernel]
            if compute is None:
                outs, others = hop_call(None, line_sends)
            else:
                outs, others = compute(*given, line_sends)
            for other, (_, group) in zip(others, by_kernel):
                token.append(other)
                results.update({number: other for number in group.members})
        else:
            outs = compute(*given) if compute else ()
        at = 0
        for transfer, of_one in zip(transfers, sends):
            transfer.receive([results[at + i] for i in range(len(of_one))])
            at += len(of_one)
        self.token = (*token, *outs)
        return outs


def turned(values, dim, axis):
    count = lax.axis_size(axis)
    here = lax.axis_index(axis)
    size = values.shape[dim] // count
    return jnp.concatenate(
        [
            lax.dynamic_slice_in_dim(
                values, lax.rem(here - i + count, count) * size, size, dim
            )
            for i in range(count)
        ],
        axis=dim,
    )


class SmallSum:
    def __init__(self, values, axis):
        self.values, self.axis = values, axis
        self.count = lax.axis_size(axis)

    def sends(self):
        count = self.count
        return [
            (self.values, self.axis, [(i, (i + step) % count) for i in range(count)], None)
            for step in range(1, count)
        ]

    def receive(self, results):
        self.others = results

    def result(self):
        return sum(self.others, self.values)


def norm_back(grad, values, gain):
    root = lax.rsqrt(jnp.mean(values * values, axis=-1, keepdims=True) + EPS)
    weighted = grad * gain
    mean = jnp.mean(weighted * values, axis=-1, keepdims=True)
    return root * weighted - values * (root * root * root) * mean


def on_device(
    tokens, norm_one, q_weight, k_weight, v_weight, o_weight, norm_two,
    gate_weight, up_weight, down_weight, segment_ids, parent_ids, path_pos, cotangent,
):
    ctx = lax.axis_index("context")
    ctx_count = lax.axis_size("context")
    ten_count = lax.axis_size(HOP_AXIS)
    tree_count, rows, width = tokens.shape
    share = rows // ten_count
    trees = tree_count // MICRO
    flat = trees * rows
    part, q_width = q_weight.shape
    kv_width = k_weight.shape[1]
    q_heads = q_width // HEAD
    kv_heads = kv_width // HEAD
    used = q_width + 2 * kv_width
    packed_width = round_up(used + 2, LANES)

    attention_block = jnp.concatenate(
        [
            q_weight, k_weight, v_weight, norm_one[:, None], norm_two[:, None],
            jnp.zeros((part, packed_width - used - 2), BF16),
        ],
        axis=1,
    )
    attention_full = lax.all_gather(attention_block, WEIGHT_AXES, axis=0, tiled=True)
    o_full = lax.all_gather(o_weight.T, WEIGHT_AXES, axis=0, tiled=True)
    hidden = gate_weight.shape[1]
    wide = round_up(hidden, LANES)

    def widened(values):
        return jnp.pad(values, ((0, 0), (0, wide - hidden)))

    down_full = lax.all_gather(widened(down_weight.T), WEIGHT_AXES, axis=0, tiled=True)
    gate_up_block = jnp.concatenate([widened(gate_weight), widened(up_weight)], axis=1)
    gate_up_full = lax.all_gather(gate_up_block, WEIGHT_AXES, axis=0, tiled=True)
    gain_one = attention_full[:, used].astype(F32)
    gain_two = attention_full[:, used + 1].astype(F32)

    lane = np.arange(q_heads * LANES)
    column = np.arange(q_width)
    select = jnp.asarray(
        (lane[:, None] // LANES == column[None, :] // HEAD)
        & (lane[:, None] % LANES == column[None, :] % HEAD),
        BF16,
    )
    frequency = THETA ** (-(jnp.arange(HALF, dtype=F32) * 2.0 / HEAD))
    pad = jnp.zeros((flat, LANES - HEAD), F32)
    ctx_ref = jnp.reshape(ctx, (1,)).astype(jnp.int32)

    tokens = turned(tokens, 1, HOP_AXIS)
    cotangent = turned(cotangent, 1, HOP_AXIS)
    segment_ids, parent_ids, path_pos = [
        turned(ids.reshape(-1, ctx_count, rows), 2, HOP_AXIS).reshape(ids.shape)
        for ids in (segment_ids, parent_ids, path_pos)
    ]
    state = []
    for micro in range(MICRO):
        pick = slice(micro * trees, (micro + 1) * trees)
        m = SimpleNamespace()
        state.append(m)
        m.number = micro
        m.x = tokens[pick]
        m.dy = cotangent[pick]
        seg, par, pos = segment_ids[pick], parent_ids[pick], path_pos[pick]

        def here(ids):
            return lax.dynamic_slice_in_dim(ids, ctx * rows, rows, 1)

        m.ids = (
            here(seg)[:, :, None], here(par)[:, :, None], here(pos)[:, :, None],
            seg[:, None, :], pos[:, None, :],
        )
        angles = here(pos).reshape(flat).astype(F32)[:, None] * frequency[None, :]
        cosine, sine = jnp.cos(angles), jnp.sin(angles)
        m.cos = jnp.concatenate([cosine, cosine, pad], axis=1)
        m.sin = jnp.concatenate([-sine, sine, pad], axis=1)
        x = m.x.reshape(flat, width).astype(F32)
        m.root_one = lax.rsqrt(jnp.mean(x * x, axis=-1, keepdims=True) + EPS)
        m.x_here = m.x[:, :share].astype(F32)
        m.dy_here = m.dy[:, :share].astype(F32)

    def together(*parts):
        return jnp.concatenate([part.reshape(flat, -1) for part in parts], axis=0)

    def shaped(product):
        return product.reshape(trees, rows, width)

    x_all = tokens.reshape(-1, width).astype(F32)
    root_all = jnp.concatenate([m.root_one for m in state], axis=0)
    normed_all = (x_all * root_all * gain_one).astype(BF16)
    stage = Stages()
    a, b = state

    def project(m):
        def run(root):
            at = m.number * flat
            packed = mm(normed_all[at : at + flat], attention_full)
            m.q, kv = split_heads(packed, m.cos, m.sin, q_heads, kv_heads, rows)
            m.kv = EarlierGather(kv.reshape(trees, rows, -1), "context")
            return (m.q,)

        return run

    def attend(m):
        def run(q):
            m.kv_full = m.kv.result()
            wide = attend_forward(ctx_ref, q, m.kv_full, m.ids, q_heads, kv_heads, rows)
            m.attended = mm(wide, select).astype(BF16)
            product = mm_nt(m.attended, o_full).astype(BF16)
            m.sum1 = LineSum(shaped(product), share, HOP_AXIS)
            return (product,)

        return run

    def mixed_back(m):
        def run(dy):
            m.dmixed = row_major(mm(dy.reshape(flat, width), down_full))
            return (m.dmixed,)

        return run

    def norm_two_of(m):
        middle = m.x_here + m.sum1.result()
        root = lax.rsqrt(jnp.mean(middle * middle, axis=-1, keepdims=True) + EPS)
        m.middle, m.root_two = middle, root
        m.gather1 = LineGather((middle * root * gain_two).astype(BF16), HOP_AXIS)

    def feed_forward(m):
        def run(normed_two, sends):
            m.normed_two = normed_two
            (m.mixed, m.dgate, m.dup), others = feed_forward_hidden(
                normed_two, gate_up_full, m.dmixed, sends
            )
            return (m.mixed, m.dgate, m.dup), others

        return run

    def back_of(m):
        def run(dgate, sends):
            (product, out), others = feed_back(
                dgate, m.dup, m.mixed, gate_up_full, down_full, sends
            )
            m.sum3 = LineSum(shaped(product), share, HOP_AXIS)
            m.out_part = shaped(out)
            return (product, out), others

        return run

    def norm_two_back(m):
        middle, dn2 = m.middle, m.sum3.result()
        m.gain_two_grad = jnp.sum(dn2 * middle * m.root_two, axis=(0, 1))
        m.dmiddle = m.dy_here + norm_back(dn2, middle, gain_two)
        m.gather2 = LineGather(m.dmiddle.astype(BF16), HOP_AXIS)

    def attended_back(m):
        def run(dmb, sends):
            m.dmb = dmb
            (m.do,), others = out_back(dmb, o_full, select, sends)
            return (m.do,), others

        return run

    def attend_back(m):
        def run(do_wide, sends):
            (m.dq, dk, dv), others = attend_backward(
                m.q, m.kv_full, do_wide, m.ids, q_heads, kv_heads, rows, sends
            )
            m.dkv = EarlierReturn(jnp.concatenate([dk, dv], axis=2), "context")
            return (m.dq,), others

        return run

    def norm_one_back(m):
        def run(dq, sends):
            dkv = m.dkv.result().reshape(flat, -1)
            (m.dqkv, dn1), others = pack_heads(
                dq, dkv, m.cos, m.sin, attention_full, q_heads, kv_heads, sends
            )
            x = m.x.reshape(flat, width).astype(F32)
            m.gain_one_grad = jnp.sum(dn1.astype(F32) * x * m.root_one, axis=0)
            m.sum4 = LineSum(shaped(dn1), share, HOP_AXIS)
            return (m.dqkv, dn1), others

        return run

    class WeightGrad:
        def __init__(self, right_of):
            self.right_of = right_of

        def __call__(self, left, sends):
            (self.grad,), others = weight_grad(left, self.right_of(), sends)
            return (self.grad,), others

        def scattered(self):
            return lax.psum_scatter(self.grad, WEIGHT_AXES, scatter_dimension=0, tiled=True)

    def gathered(transfer):
        return transfer.result().reshape(flat, width)

    stage([], project(a), [a.root_one])
    stage([a.kv], project(b), [b.root_one])
    stage([b.kv], attend(a), [a.q])
    stage([a.sum1], attend(b), [b.q])
    stage([a.sum1], fused=True)
    stage([a.sum1], mixed_back(a), [a.dy])
    norm_two_of(a)
    stage([a.gather1], mixed_back(b), [b.dy])
    stage([a.gather1, b.sum1], fused=True)
    stage([a.gather1, b.sum1], fused=True)
    stage([b.sum1], fused=True)
    norm_two_of(b)
    stage([b.gather1], feed_forward(a), [gathered(a.gather1)], fused=True)
    stage([b.gather1], back_of(a), [a.dgate], fused=True)
    stage([b.gather1, a.sum3], fused=True)
    stage([a.sum3], feed_forward(b), [gathered(b.gather1)], fused=True)
    dy_all = cotangent.reshape(-1, width)
    mixed_all = together(a.mixed, b.mixed)
    down_grad = WeightGrad(lambda: mixed_all)
    stage([a.sum3], down_grad, [dy_all], fused=True)
    down_grad = down_grad.scattered()
    norm_two_back(a)
    a.sum2 = LineSum(a.out_part, share, HOP_AXIS)
    stage([a.gather2, a.sum2], back_of(b), [b.dgate], fused=True)
    b.sum2 = LineSum(b.out_part, share, HOP_AXIS)
    normed_two_all = together(a.normed_two, b.normed_two)
    gate_grad = WeightGrad(lambda: together(a.dgate, b.dgate))
    stage([a.gather2, b.sum3], gate_grad, [normed_two_all], fused=True)
    gate_grad = gate_grad.scattered()
    up_grad = WeightGrad(lambda: together(a.dup, b.dup))
    stage([a.gather2, b.sum3], up_grad, [normed_two_all], fused=True)
    up_grad = up_grad.scattered()
    stage([b.sum3], attended_back(a), [gathered(a.gather2)], fused=True)
    norm_two_back(b)
    stage([b.gather2], attend_back(a), [a.do], fused=True)
    stage([b.gather2, b.sum2, a.dkv], fused=True)
    stage([b.gather2, a.sum2], norm_one_back(a), [a.dq], fused=True)
    stage.wait_for(down_grad)
    stage([a.sum4], attended_back(b), [gathered(b.gather2)], fused=True)
    stage.wait_for(gate_grad)
    stage([a.sum4, a.sum2], attend_back(b), [b.do], fused=True)
    stage.wait_for(up_grad)
    o_grad = WeightGrad(lambda: together(a.attended, b.attended))
    stage([a.sum4, b.dkv], o_grad, [together(a.dmb, b.dmb)], fused=True)
    o_grad = o_grad.scattered()
    stage([b.sum2], norm_one_back(b), [b.dq], fused=True)
    gains = jnp.stack([a.gain_one_grad + b.gain_one_grad, a.gain_two_grad + b.gain_two_grad])
    gains = SmallSum(gains, HOP_AXIS)
    attention_grad = WeightGrad(lambda: together(a.dqkv, b.dqkv))
    stage([b.sum4, b.sum2, gains], attention_grad, [normed_all], fused=True)
    attention_grad = attention_grad.scattered().astype(F32)
    gains = SmallSum(gains.result(), "context")
    stage([b.sum4, gains], fused=True)
    stage.wait_for(o_grad)
    gains = SmallSum(gains.result(), "fsdp")
    stage([b.sum4, gains], fused=True)
    block = lax.axis_index("fsdp") * ctx_count + ctx
    gains = lax.dynamic_slice_in_dim(gains.result(), block * part, part, 1)
    for m in state:
        m.out_sum = m.sum2.result()
    for m in state:
        middle, out_sum = lax.optimization_barrier((m.middle, m.out_sum))
        m.out = (middle + out_sum.astype(F32)).astype(BF16)
        m.dx = (m.dmiddle + norm_back(m.sum4.result(), m.x_here, gain_one)).astype(BF16)

    return (
        jnp.concatenate([m.out for m in state], axis=0),
        jnp.concatenate([m.dx for m in state], axis=0),
        gains[0],
        attention_grad[:, :q_width],
        attention_grad[:, q_width : q_width + kv_width],
        attention_grad[:, q_width + kv_width : used],
        o_grad.T.astype(F32),
        gains[1],
        gate_grad[:, :hidden].astype(F32),
        up_grad[:, :hidden].astype(F32),
        down_grad[:, :hidden].T.astype(F32),
    )


def solution(mesh):
    HOP_IDS.clear()
    weights = WEIGHT_AXES
    return jax.shard_map(
        on_device,
        mesh=mesh,
        in_specs=(
            P("fsdp", "context", None),
            P(weights),
            P(weights, "tensor"),
            P(weights, "tensor"),
            P(weights, "tensor"),
            P("tensor", weights),
            P(weights),
            P(weights, "tensor"),
            P(weights, "tensor"),
            P("tensor", weights),
            P("fsdp", None),
            P("fsdp", None),
            P("fsdp", None),
            P("fsdp", "context", None),
        ),
        out_specs=(
            P("fsdp", ("context", "tensor"), None),
            P("fsdp", ("context", "tensor"), None),
            P(weights),
            P(weights, "tensor"),
            P(weights, "tensor"),
            P(weights, "tensor"),
            P("tensor", weights),
            P(weights),
            P(weights, "tensor"),
            P(weights, "tensor"),
            P("tensor", weights),
        ),
        check_vma=False,
    )
```

```python
import functools
from types import SimpleNamespace

import jax
import jax.numpy as jnp
import numpy as np
from jax import lax
from jax.experimental import pallas as pl
from jax.experimental.pallas import tpu as pltpu
from jax.experimental.layout import Layout, with_layout_constraint
from jax.sharding import PartitionSpec as P


HEAD = 80
HALF = HEAD // 2
LANES = 128
MICRO = 2
EPS = 1e-05
THETA = 10000.0
NEG = -1000000000.0
TRUNK = 512
WEIGHT_AXES = ("fsdp", "context")
BF16 = jnp.bfloat16
F32 = jnp.float32


def row_major(value):
    return with_layout_constraint(value, Layout(major_to_minor=(0, 1)))


def round_up(value, unit):
    return (value + unit - 1) // unit * unit


def mm(left, right):
    return lax.dot_general(left, right, (((1,), (0,)), ((), ())), preferred_element_type=F32)


def mm_nt(left, right):
    return lax.dot_general(left, right, (((1,), (1,)), ((), ())), preferred_element_type=F32)


def mm_tn(left, right):
    return lax.dot_general(left, right, (((0,), (0,)), ((), ())), preferred_element_type=F32)


def rotated(values, cos_table, sin_table):
    lane = lax.broadcasted_iota(jnp.int32, values.shape, 1)
    swapped = jnp.where(
        lane < HALF, pltpu.roll(values, LANES - HALF, 1), pltpu.roll(values, HALF, 1)
    )
    return values * cos_table + swapped * sin_table


def window_of(head):
    start = head * HEAD
    base = start // LANES * LANES
    return base, start - base


def split_kernel(q_heads, kv_heads, x_ref, cos_ref, sin_ref, q_ref, kv_ref):
    cos_table = cos_ref[...]
    sin_table = sin_ref[...]
    for head in range(q_heads + 2 * kv_heads):
        base, shift = window_of(head)
        window = x_ref[:, base : base + 2 * LANES]
        if shift:
            window = pltpu.roll(window, 2 * LANES - shift, 1)
        values = window[:, :LANES]
        if head < q_heads + kv_heads:
            result = rotated(values, cos_table, sin_table)
        else:
            lane = lax.broadcasted_iota(jnp.int32, values.shape, 1)
            result = jnp.where(lane < HEAD, values, 0.0)
        result = result.astype(BF16)
        if head < q_heads:
            q_ref[:, head * LANES : (head + 1) * LANES] = result
        else:
            at = (head - q_heads) * LANES
            kv_ref[:, at : at + LANES] = result


def split_heads(packed, cos_table, sin_table, q_heads, kv_heads, rows):
    total, width = packed.shape
    q_wide = q_heads * LANES
    kv_wide = 2 * kv_heads * LANES
    return pl.pallas_call(
        functools.partial(split_kernel, q_heads, kv_heads),
        grid=(total // rows,),
        in_specs=[
            pl.BlockSpec((rows, width), lambda b: (b, 0)),
            pl.BlockSpec((rows, LANES), lambda b: (b, 0)),
            pl.BlockSpec((rows, LANES), lambda b: (b, 0)),
        ],
        out_specs=[
            pl.BlockSpec((rows, q_wide), lambda b: (b, 0)),
            pl.BlockSpec((rows, kv_wide), lambda b: (b, 0)),
        ],
        out_shape=[
            jax.ShapeDtypeStruct((total, q_wide), BF16),
            jax.ShapeDtypeStruct((total, kv_wide), BF16),
        ],
        cost_estimate=pl.CostEstimate(
            flops=10 * total * width, bytes_accessed=7 * total * width, transcendentals=0
        ),
        name="split_heads",
    )(packed, cos_table, sin_table)


def fill_bias(seg_q, par_q, pos_q, seg_k, pos_k, bias_ref):
    same = (seg_k == seg_q) | (seg_k == par_q) | (seg_k == 0)
    bias_ref[...] = jnp.where(same & (pos_k <= pos_q), 0.0, NEG)


def probabilities(q_block, keys, bias):
    scores = mm_nt(q_block, keys) * HEAD ** (-0.5) + bias
    top = jnp.max(scores, axis=1, keepdims=True)
    raised = jnp.exp(scores - top)
    return raised * (1.0 / jnp.sum(raised, axis=1, keepdims=True))


def forward_kernel(
    rows, tree_len, block,
    ctx_ref, q_ref, k_ref, v_ref, seg_q, par_q, pos_q, seg_k, pos_k, out_ref, bias_ref,
):
    @pl.when(pl.program_id(1) == 0)
    def _():
        fill_bias(seg_q[0], par_q[0], pos_q[0], seg_k[0], pos_k[0], bias_ref)

    in_trunk = (ctx_ref[0] + 1) * rows <= TRUNK

    def run(keys):
        @pl.loop(0, rows // block)
        def _(step):
            at = pl.ds(pl.multiple_of(step * block, block), block)
            probs = probabilities(q_ref[at, :], k_ref[0, :keys, :], bias_ref[at, :keys])
            out_ref[at, :] = mm(probs.astype(BF16), v_ref[0, :keys, :]).astype(BF16)

    pl.when(in_trunk)(lambda: run(min(TRUNK, tree_len)))
    pl.when(jnp.logical_not(in_trunk))(lambda: run(tree_len))


def backward_kernel(
    rows, tree_len, block, group,
    q_ref, k_ref, v_ref, do_ref, seg_q, par_q, pos_q, seg_k, pos_k,
    dq_ref, dk_ref, dv_ref, bias_ref,
):
    head = pl.program_id(1)

    @pl.when(head == 0)
    def _():
        fill_bias(seg_q[0], par_q[0], pos_q[0], seg_k[0], pos_k[0], bias_ref)

    @pl.when(lax.rem(head, group) == 0)
    def _():
        dk_ref[...] = jnp.zeros_like(dk_ref)
        dv_ref[...] = jnp.zeros_like(dv_ref)

    in_trunk = (lax.axis_index("context") + 1) * rows <= TRUNK
    scale = HEAD ** (-0.5)

    def run(keys):
        @pl.loop(0, rows // block)
        def _(step):
            at = pl.ds(pl.multiple_of(step * block, block), block)
            q_block = q_ref[at, :]
            do_block = do_ref[at, :]
            k_all = k_ref[0, :keys, :]
            probs = probabilities(q_block, k_all, bias_ref[at, :keys])
            dprobs = mm_nt(do_block, v_ref[0, :keys, :])
            delta = jnp.sum(probs * dprobs, axis=1, keepdims=True)
            dscores = (probs * (dprobs - delta)).astype(BF16)
            dq_ref[at, :] = (mm(dscores, k_all) * scale).astype(BF16)
            dk_ref[0, :keys, :] += mm_tn(dscores, q_block) * scale
            dv_ref[0, :keys, :] += mm_tn(probs.astype(BF16), do_block)

    pl.when(in_trunk)(lambda: run(min(TRUNK, tree_len)))
    pl.when(jnp.logical_not(in_trunk))(lambda: run(tree_len))


def attention_specs(rows, tree_len, group, kv_heads):
    def column(b, h, *c):
        return (b, h)

    def whole(b, h, *c):
        return (b, 0, 0)

    return [
        pl.BlockSpec((rows, LANES), column),
        pl.BlockSpec((1, tree_len, LANES), lambda b, h, *c: (b, 0, h // group)),
        pl.BlockSpec((1, tree_len, LANES), lambda b, h, *c: (b, 0, kv_heads + h // group)),
    ], [
        pl.BlockSpec((1, rows, 1), whole),
        pl.BlockSpec((1, rows, 1), whole),
        pl.BlockSpec((1, rows, 1), whole),
        pl.BlockSpec((1, 1, tree_len), whole),
        pl.BlockSpec((1, 1, tree_len), whole),
    ]


def attend_forward(ctx, q_wide, kv_full, ids, q_heads, kv_heads, rows):
    trees, tree_len, _ = kv_full.shape
    group = q_heads // kv_heads
    first, last = attention_specs(rows, tree_len, group, kv_heads)
    block = min(rows, 256)
    work = trees * q_heads * rows * tree_len
    return pl.pallas_call(
        functools.partial(forward_kernel, rows, tree_len, block),
        grid_spec=pltpu.PrefetchScalarGridSpec(
            num_scalar_prefetch=1,
            grid=(trees, q_heads),
            in_specs=first + last,
            out_specs=pl.BlockSpec((rows, LANES), lambda b, h, c: (b, h)),
            scratch_shapes=[pltpu.VMEM((rows, tree_len), F32)],
        ),
        out_shape=jax.ShapeDtypeStruct(q_wide.shape, BF16),
        cost_estimate=pl.CostEstimate(
            flops=4 * LANES * work, bytes_accessed=8 * q_wide.size, transcendentals=work
        ),
        name="attend_forward",
    )(ctx, q_wide, kv_full, kv_full, *ids)


HOP_AXIS = "tensor"


def with_hops(kernel, counts, sides, *refs):
    own_in, own_out, own_scratch = counts
    sends = len(sides)
    ends_at = []
    for size in (own_in, sends, own_out, sends, own_scratch):
        ends_at.append((ends_at[-1] if ends_at else 0) + size)
    ins, sent, outs, received, scratch = (
        refs[low:high] for low, high in zip([0, *ends_at], ends_at)
    )
    send_sem, recv_sem = refs[ends_at[-1] :]
    here = lax.axis_index(HOP_AXIS)
    count = lax.axis_size(HOP_AXIS)
    has_next, has_last = here < count - 1, here > 0

    def copy(number):
        other = here + 1 - 2 * sides[number]
        return pltpu.make_async_remote_copy(
            src_ref=sent[number],
            dst_ref=received[number],
            send_sem=send_sem.at[number],
            recv_sem=recv_sem.at[number],
            device_id={HOP_AXIS: other},
            device_id_type=pl.DeviceIdType.MESH,
        )

    first, last = None, None
    if own_in:
        first, last = jnp.bool_(True), jnp.bool_(True)
        for axis in range(GRID_RANK[kernel]):
            first &= pl.program_id(axis) == 0
            last &= pl.program_id(axis) == pl.num_programs(axis) - 1

    def start():
        barrier = pltpu.get_barrier_semaphore()
        for there, step in ((has_next, 1), (has_last, -1)):

            @pl.when(there)
            def _():
                pl.semaphore_signal(
                    barrier,
                    inc=1,
                    device_id={HOP_AXIS: here + step},
                    device_id_type=pl.DeviceIdType.MESH,
                )

        pl.semaphore_wait(barrier, has_next.astype(jnp.int32) + has_last.astype(jnp.int32))
        for number, side in enumerate(sides):
            pl.when((has_next, has_last)[side])(lambda number=number: copy(number).start())

    def finish():
        for number, side in enumerate(sides):
            pl.when((has_next, has_last)[side])(lambda number=number: copy(number).wait_send())
            pl.when((has_last, has_next)[side])(lambda number=number: copy(number).wait_recv())

    if own_in:
        pl.when(first)(start)
        kernel(*ins, *outs, *scratch)
        pl.when(last)(finish)
    else:
        start()
        finish()


GRID_RANK = {}
HOP_IDS = {}


def hop_call(kernel, sends, *args, grid=(), in_specs=(), out_specs=(), out_shape=(),
             scratch_shapes=(), name="hop", cost_estimate=None):
    sides = tuple(side for _, side in sends)
    values = [value for value, _ in sends]
    anywhere = pl.BlockSpec(memory_space=pl.ANY)
    if kernel is not None:
        GRID_RANK[kernel] = len(grid)
    counts = (len(args), len(out_shape), len(scratch_shapes))
    key = (name, sides, tuple(v.shape for v in (*values, *args)))
    results = pl.pallas_call(
        functools.partial(with_hops, kernel, counts, sides),
        grid=grid,
        in_specs=[*in_specs, *[anywhere] * len(values)],
        out_specs=[*out_specs, *[anywhere] * len(values)],
        out_shape=[*out_shape, *[jax.ShapeDtypeStruct(v.shape, v.dtype) for v in values]],
        scratch_shapes=[
            *scratch_shapes,
            pltpu.SemaphoreType.DMA((len(values),)),
            pltpu.SemaphoreType.DMA((len(values),)),
        ],
        compiler_params=pltpu.CompilerParams(
            collective_id=HOP_IDS.setdefault(key, len(HOP_IDS)), has_side_effects=True
        ),
        cost_estimate=cost_estimate,
    )(*args, *values)
    return results[: len(out_shape)], results[len(out_shape) :]


def attend_backward(q_wide, kv_full, do_wide, ids, q_heads, kv_heads, rows, sends):
    trees, tree_len, _ = kv_full.shape
    group = q_heads // kv_heads
    first, last = attention_specs(rows, tree_len, group, kv_heads)
    block = min(rows, 256)
    work = trees * q_heads * rows * tree_len
    grad_spec = pl.BlockSpec((1, tree_len, LANES), lambda b, h: (b, 0, h // group))
    grad_shape = jax.ShapeDtypeStruct((trees, tree_len, kv_heads * LANES), F32)
    return hop_call(
        functools.partial(backward_kernel, rows, tree_len, block, group),
        sends,
        *(q_wide, kv_full, kv_full, do_wide, *ids),
        grid=(trees, q_heads),
        in_specs=first + [first[0]] + last,
        out_specs=[first[0], grad_spec, grad_spec],
        out_shape=[jax.ShapeDtypeStruct(q_wide.shape, BF16), grad_shape, grad_shape],
        scratch_shapes=[pltpu.VMEM((rows, tree_len), F32)],
        cost_estimate=pl.CostEstimate(
            flops=10 * LANES * work, bytes_accessed=12 * q_wide.size, transcendentals=work
        ),
        name="attend_backward",
    )


def pack_kernel(
    q_heads, kv_heads, dq_ref, dkv_ref, cos_ref, sin_ref, weight, packed_ref, product_ref, sum_ref
):
    @pl.when(pl.program_id(0) == 0)
    def _():
        cos_table = cos_ref[...]
        sin_table = -sin_ref[...]
        sum_ref[...] = jnp.zeros_like(sum_ref)
        for head in range(q_heads + 2 * kv_heads):
            base, shift = window_of(head)
            if head < q_heads:
                values = dq_ref[:, head * LANES : (head + 1) * LANES].astype(F32)
            else:
                at = (head - q_heads) * LANES
                values = dkv_ref[:, at : at + LANES].astype(BF16).astype(F32)
            if head < q_heads + kv_heads:
                values = rotated(values, cos_table, sin_table)
            wide = jnp.concatenate([values, jnp.zeros_like(values)], axis=1)
            if shift:
                wide = pltpu.roll(wide, shift, 1)
            sum_ref[:, base : base + 2 * LANES] += wide
        packed_ref[...] = sum_ref[...].astype(BF16)

    product_ref[...] = mm_nt(packed_ref[...], weight[...]).astype(BF16)


def pack_heads(dq_wide, dkv, cos_table, sin_table, weight, q_heads, kv_heads, sends):
    rows = dq_wide.shape[0]
    width, packed = weight.shape
    tile = width // 5

    def whole(values):
        return pl.BlockSpec(values.shape, lambda i: (0, 0))

    return hop_call(
        functools.partial(pack_kernel, q_heads, kv_heads),
        sends,
        *(dq_wide, dkv, cos_table, sin_table, weight),
        grid=(width // tile,),
        in_specs=[
            whole(dq_wide), whole(dkv), whole(cos_table), whole(sin_table),
            pl.BlockSpec((tile, packed), lambda i: (i, 0)),
        ],
        out_specs=[
            pl.BlockSpec((rows, packed), lambda i: (0, 0)),
            pl.BlockSpec((rows, tile), lambda i: (0, i)),
        ],
        out_shape=[
            jax.ShapeDtypeStruct((rows, packed), BF16),
            jax.ShapeDtypeStruct((rows, width), BF16),
        ],
        scratch_shapes=[pltpu.VMEM((rows, packed), F32)],
        cost_estimate=pl.CostEstimate(
            flops=2 * rows * width * packed,
            bytes_accessed=2 * width * packed + 8 * rows * packed + 2 * rows * width,
            transcendentals=0,
        ),
        name="pack_heads",
    )


def weight_grad_kernel(first_left, last_left, first_right, last_right, grad_ref):
    grad = mm_tn(first_left[...], first_right[...]) + mm_tn(last_left[...], last_right[...])
    grad_ref[...] = grad.astype(BF16)


def weight_grad(lefts, rights, sends):
    rows, columns = rights[0].shape
    if len(lefts) == 1:
        lefts, at = lefts * 2, (0, 1)
    else:
        at = (0, 0)
    width = lefts[0].shape[1]
    tile = width // 5
    right = pl.BlockSpec((rows, columns), lambda i: (0, 0))
    return hop_call(
        weight_grad_kernel,
        sends,
        *(*lefts, *rights),
        grid=(width // tile,),
        in_specs=[
            pl.BlockSpec((rows, tile), lambda i: (at[0], i)),
            pl.BlockSpec((rows, tile), lambda i: (at[1], i)),
            right,
            right,
        ],
        out_specs=[pl.BlockSpec((tile, columns), lambda i: (i, 0))],
        out_shape=[jax.ShapeDtypeStruct((width, columns), BF16)],
        cost_estimate=pl.CostEstimate(
            flops=4 * rows * width * columns,
            bytes_accessed=4 * rows * (width + columns) + 2 * width * columns,
            transcendentals=0,
        ),
        name="weight_grad",
    )


def feed_forward_kernel(normed, gate_w, up_w, dmixed, mixed_ref, dgate_ref, dup_ref):
    gate = mm(normed[...], gate_w[...])
    up = mm(normed[...], up_w[...])
    sigmoid = 1.0 / (1.0 + jnp.exp(-gate))
    silu = gate * sigmoid
    slope = sigmoid * (1.0 + gate * (1.0 - sigmoid))
    mixed_ref[...] = (silu * up).astype(BF16)
    dgate_ref[...] = (dmixed[...] * up * slope).astype(BF16)
    dup_ref[...] = (dmixed[...] * silu).astype(BF16)


def feed_forward_hidden(normed, gate_up_w, dmixed, sends):
    rows, width = normed.shape
    hidden = dmixed.shape[1]
    tile = 2 * LANES
    count = hidden // tile
    result = pl.BlockSpec((rows, tile), lambda i: (0, i))
    return hop_call(
        feed_forward_kernel,
        sends,
        *(normed, gate_up_w, gate_up_w, dmixed),
        grid=(count,),
        in_specs=[
            pl.BlockSpec((rows, width), lambda i: (0, 0)),
            pl.BlockSpec((width, tile), lambda i: (0, i)),
            pl.BlockSpec((width, tile), lambda i: (0, i + count)),
            result,
        ],
        out_specs=[result] * 3,
        out_shape=[jax.ShapeDtypeStruct((rows, hidden), BF16)] * 3,
        cost_estimate=pl.CostEstimate(
            flops=4 * rows * hidden * width,
            bytes_accessed=4 * hidden * width + 2 * rows * width + 10 * rows * hidden,
            transcendentals=rows * hidden,
        ),
        name="feed_forward",
    )


def feed_back_kernel(dgate, dup, mixed, gate_w, up_w, down_w, dn2_ref, out_ref):
    dn2 = mm_nt(dgate[...], gate_w[...]) + mm_nt(dup[...], up_w[...])
    dn2_ref[...] = dn2.astype(BF16)
    out_ref[...] = mm_nt(mixed[...], down_w[...]).astype(BF16)


def feed_back(dgate, dup, mixed, gate_up_w, down_w, sends):
    rows, hidden = mixed.shape
    width = down_w.shape[0]
    tile = width // 5
    left = pl.BlockSpec((rows, hidden), lambda i: (0, 0))
    right = pl.BlockSpec((tile, hidden), lambda i: (i, 0))
    result = pl.BlockSpec((rows, tile), lambda i: (0, i))
    return hop_call(
        feed_back_kernel,
        sends,
        *(dgate, dup, mixed, gate_up_w, gate_up_w, down_w),
        grid=(width // tile,),
        in_specs=[
            *[left] * 3,
            right,
            pl.BlockSpec((tile, hidden), lambda i: (i, 1)),
            right,
        ],
        out_specs=[result] * 2,
        out_shape=[jax.ShapeDtypeStruct((rows, width), BF16)] * 2,
        cost_estimate=pl.CostEstimate(
            flops=6 * rows * hidden * width,
            bytes_accessed=6 * hidden * (rows + width) + 4 * rows * width,
            transcendentals=0,
        ),
        name="feed_back",
    )


def out_back_kernel(grad, weight, select, result_ref):
    narrow = mm(grad[...], weight[...]).astype(BF16)
    result_ref[...] = mm_nt(narrow, select[...]).astype(BF16)


def out_back(grad, weight, select, sends):
    rows, wide = grad.shape[0], select.shape[0]

    def whole(values):
        return pl.BlockSpec(values.shape, lambda i: (0, 0))

    return hop_call(
        out_back_kernel,
        sends,
        *(grad, weight, select),
        grid=(1,),
        in_specs=[whole(grad), whole(weight), whole(select)],
        out_specs=[pl.BlockSpec((rows, wide), lambda i: (0, 0))],
        out_shape=[jax.ShapeDtypeStruct((rows, wide), BF16)],
        cost_estimate=pl.CostEstimate(
            flops=2 * rows * weight.size + 2 * rows * select.size,
            bytes_accessed=2 * (grad.size + weight.size + select.size + rows * wide),
            transcendentals=0,
        ),
        name="out_back",
    )


def piece(values, index, size):
    return lax.dynamic_slice_in_dim(values, index * size, size, 1)


class LineSum:
    def __init__(self, values, size, axis):
        self.axis = axis
        self.count = lax.axis_size(axis)
        self.pieces = [values[:, i * size : (i + 1) * size] for i in range(self.count)]
        self.step = 0
        self.got = None
        here = lax.axis_index(axis)
        self.valid = (here > 0, here < self.count - 1)

    def sends(self):
        self.step += 1
        step, count = self.step, self.count
        rights = [(i, i + 1) for i in range(step)]
        lefts = [(count - 1 - i, count - 2 - i) for i in range(step)]
        found = []
        for side, slot, pairs in ((0, step, rights), (1, count - step, lefts)):
            value = self.pieces[slot]
            if self.got is not None:
                value = (value.astype(F32) + self.arrived(side)).astype(BF16)
            found.append((value, self.axis, pairs, side))
        return found

    def arrived(self, side):
        return jnp.where(self.valid[side], self.got[side].astype(F32), 0.0)

    def loose(self):
        return self.step == 1 and self.count > 2

    def receive(self, results):
        self.got = results

    def result(self):
        assert self.step == self.count - 1
        total = self.pieces[0].astype(F32)
        for side in (0, 1) if self.got else ():
            total = total + self.arrived(side)
        return total


class LineGather:
    def __init__(self, own, axis):
        self.own, self.axis = own, axis
        self.count = lax.axis_size(axis)
        self.lefts, self.rights = [own], [own]

    def sends(self):
        step, count = len(self.lefts), self.count
        return [
            (self.lefts[-1], self.axis, [(i, i + 1) for i in range(step - 1, count - 1)], 0),
            (self.rights[-1], self.axis, [(i, i - 1) for i in range(count - step, 0, -1)], 1),
        ]

    def loose(self):
        return len(self.lefts) == self.count - 1 and self.count > 2

    def receive(self, results):
        self.lefts.append(results[0])
        self.rights.append(results[1])

    def result(self):
        count = self.count
        here = lax.axis_index(self.axis)
        assert len(self.lefts) == count
        others = [
            jnp.where(here >= step, self.lefts[step], self.rights[count - step])
            for step in range(1, count)
        ]
        return jnp.concatenate([self.own, *others], axis=1)


class EarlierGather:
    def __init__(self, own, axis):
        self.own, self.axis = own, axis
        self.count = lax.axis_size(axis)

    def sends(self):
        count = self.count
        return [
            (self.own, self.axis, [(i, i + step) for i in range(count - step)], None)
            for step in range(1, count)
        ]

    def receive(self, results):
        self.others = results

    def result(self):
        count, own = self.count, self.own
        here = lax.axis_index(self.axis)
        trees, rows, width = own.shape
        result = jnp.zeros((trees, count * rows, width), own.dtype)
        result = lax.dynamic_update_slice_in_dim(result, own, here * rows, 1)
        for step, other in enumerate(self.others, 1):
            slot = lax.rem(here - step + count, count)
            result = lax.dynamic_update_slice_in_dim(result, other, slot * rows, 1)
        return result


class EarlierReturn:
    def __init__(self, full, axis):
        self.full, self.axis = full, axis
        self.count = lax.axis_size(axis)
        self.rows = full.shape[1] // self.count

    def sends(self):
        count = self.count
        here = lax.axis_index(self.axis)
        found = []
        for step in range(1, count):
            slot = lax.rem(here - step + count, count)
            value = piece(self.full, slot, self.rows).astype(BF16)
            found.append((value, self.axis, [(i + step, i) for i in range(count - step)], None))
        return found

    def receive(self, results):
        self.others = results

    def result(self):
        total = piece(self.full, lax.axis_index(self.axis), self.rows)
        for other in self.others:
            total = total + other.astype(F32)
        return total


def ends(pairs, which):
    return {pair[which] for pair in pairs}


def disjoint(left, right):
    return not any(ends(left, which) & ends(right, which) for which in (0, 1))


def joined(sends, loose):
    groups = []
    for number, (value, axis, pairs, side) in enumerate(sends):
        for group in groups:
            if side is None or group.axis != axis or not disjoint(pairs, group.pairs):
                continue
            if group.side != side and not loose:
                continue
            here = lax.axis_index(axis)
            mine = functools.reduce(jnp.logical_or, [here == i for i in sorted(ends(pairs, 0))])
            group.value = jnp.where(mine, value, group.value)
            group.pairs = group.pairs + pairs
            group.members.append(number)
            break
        else:
            groups.append(
                SimpleNamespace(value=value, axis=axis, pairs=pairs, side=side, members=[number])
            )
    return groups


class Stages:
    def __init__(self):
        self.token = ()
        self.number = 0

    def wait_for(self, *values):
        self.token += values

    def __call__(self, transfers, compute=None, inputs=(), fused=False):
        self.number += 1
        kept = []
        for t in transfers:
            if t.count > 1:
                kept.append(t)
            else:
                t.receive([])
        transfers = kept
        sends = [t.sends() for t in transfers]
        lines = [t for t in transfers if hasattr(t, "loose")]
        loose = len(lines) == 1 and lines[0].loose() and not fused
        groups = joined([send for of_one in sends for send in of_one], loose)
        values = [group.value for group in groups]
        tied = lax.optimization_barrier((*values, *inputs, *self.token))
        results = {}
        token = []
        by_kernel = []
        for value, group in zip(tied, groups):
            if fused and group.side is not None:
                by_kernel.append((value, group))
                continue
            other = lax.ppermute(value, group.axis, group.pairs)
            token.append(other)
            results.update({number: other for number in group.members})
        given = tied[len(groups) : len(groups) + len(inputs)]
        if by_kernel:
            line_sends = [(value, group.side) for value, group in by_kernel]
            if compute is None:
                outs, others = hop_call(None, line_sends)
            else:
                outs, others = compute(*given, line_sends)
            for other, (_, group) in zip(others, by_kernel):
                token.append(other)
                results.update({number: other for number in group.members})
        else:
            outs = compute(*given) if compute else ()
        at = 0
        for transfer, of_one in zip(transfers, sends):
            transfer.receive([results[at + i] for i in range(len(of_one))])
            at += len(of_one)
        self.token = (*token, *outs)
        return outs


def turned(values, dim, axis):
    count = lax.axis_size(axis)
    here = lax.axis_index(axis)
    size = values.shape[dim] // count
    return jnp.concatenate(
        [
            lax.dynamic_slice_in_dim(
                values, lax.rem(here - i + count, count) * size, size, dim
            )
            for i in range(count)
        ],
        axis=dim,
    )


class SmallSum:
    def __init__(self, values, axis):
        self.values, self.axis = values, axis
        self.count = lax.axis_size(axis)

    def sends(self):
        count = self.count
        return [
            (self.values, self.axis, [(i, (i + step) % count) for i in range(count)], None)
            for step in range(1, count)
        ]

    def receive(self, results):
        self.others = results

    def result(self):
        return sum(self.others, self.values)


def norm_back(grad, values, gain):
    root = lax.rsqrt(jnp.mean(values * values, axis=-1, keepdims=True) + EPS)
    weighted = grad * gain
    mean = jnp.mean(weighted * values, axis=-1, keepdims=True)
    return root * weighted - values * (root * root * root) * mean


def on_device(
    tokens, norm_one, q_weight, k_weight, v_weight, o_weight, norm_two,
    gate_weight, up_weight, down_weight, segment_ids, parent_ids, path_pos, cotangent,
):
    ctx = lax.axis_index("context")
    ctx_count = lax.axis_size("context")
    ten_count = lax.axis_size(HOP_AXIS)
    tree_count, rows, width = tokens.shape
    share = rows // ten_count
    trees = tree_count // MICRO
    flat = trees * rows
    part, q_width = q_weight.shape
    kv_width = k_weight.shape[1]
    q_heads = q_width // HEAD
    kv_heads = kv_width // HEAD
    used = q_width + 2 * kv_width
    packed_width = round_up(used + 2, LANES)

    attention_block = jnp.concatenate(
        [
            q_weight, k_weight, v_weight, norm_one[:, None], norm_two[:, None],
            jnp.zeros((part, packed_width - used - 2), BF16),
        ],
        axis=1,
    )
    attention_full = lax.all_gather(attention_block, WEIGHT_AXES, axis=0, tiled=True)
    o_full = lax.all_gather(o_weight.T, WEIGHT_AXES, axis=0, tiled=True)
    hidden = gate_weight.shape[1]
    wide = round_up(hidden, LANES)

    def widened(values):
        return jnp.pad(values, ((0, 0), (0, wide - hidden)))

    down_full = lax.all_gather(widened(down_weight.T), WEIGHT_AXES, axis=0, tiled=True)
    gate_up_block = jnp.concatenate([widened(gate_weight), widened(up_weight)], axis=1)
    gate_up_full = lax.all_gather(gate_up_block, WEIGHT_AXES, axis=0, tiled=True)
    gain_one = attention_full[:, used].astype(F32)
    gain_two = attention_full[:, used + 1].astype(F32)

    lane = np.arange(q_heads * LANES)
    column = np.arange(q_width)
    select = jnp.asarray(
        (lane[:, None] // LANES == column[None, :] // HEAD)
        & (lane[:, None] % LANES == column[None, :] % HEAD),
        BF16,
    )
    frequency = THETA ** (-(jnp.arange(HALF, dtype=F32) * 2.0 / HEAD))
    pad = jnp.zeros((flat, LANES - HEAD), F32)
    ctx_ref = jnp.reshape(ctx, (1,)).astype(jnp.int32)

    tokens = turned(tokens, 1, HOP_AXIS)
    cotangent = turned(cotangent, 1, HOP_AXIS)
    segment_ids, parent_ids, path_pos = [
        turned(ids.reshape(-1, ctx_count, rows), 2, HOP_AXIS).reshape(ids.shape)
        for ids in (segment_ids, parent_ids, path_pos)
    ]
    state = []
    for micro in range(MICRO):
        pick = slice(micro * trees, (micro + 1) * trees)
        m = SimpleNamespace()
        state.append(m)
        m.number = micro
        m.x = tokens[pick]
        m.dy = cotangent[pick]
        seg, par, pos = segment_ids[pick], parent_ids[pick], path_pos[pick]

        def here(ids):
            return lax.dynamic_slice_in_dim(ids, ctx * rows, rows, 1)

        m.ids = (
            here(seg)[:, :, None], here(par)[:, :, None], here(pos)[:, :, None],
            seg[:, None, :], pos[:, None, :],
        )
        angles = here(pos).reshape(flat).astype(F32)[:, None] * frequency[None, :]
        cosine, sine = jnp.cos(angles), jnp.sin(angles)
        m.cos = jnp.concatenate([cosine, cosine, pad], axis=1)
        m.sin = jnp.concatenate([-sine, sine, pad], axis=1)
        x = m.x.reshape(flat, width).astype(F32)
        m.root_one = lax.rsqrt(jnp.mean(x * x, axis=-1, keepdims=True) + EPS)
        m.x_here = m.x[:, :share].astype(F32)
        m.dy_here = m.dy[:, :share].astype(F32)

    def shaped(product):
        return product.reshape(trees, rows, width)

    x_all = tokens.reshape(-1, width).astype(F32)
    root_all = jnp.concatenate([m.root_one for m in state], axis=0)
    normed_all = (x_all * root_all * gain_one).astype(BF16)
    stage = Stages()
    a, b = state

    def project(m):
        def run(root):
            at = m.number * flat
            packed = mm(normed_all[at : at + flat], attention_full)
            m.q, kv = split_heads(packed, m.cos, m.sin, q_heads, kv_heads, rows)
            m.kv = EarlierGather(kv.reshape(trees, rows, -1), "context")
            return (m.q,)

        return run

    def attend(m):
        def run(q):
            m.kv_full = m.kv.result()
            wide = attend_forward(ctx_ref, q, m.kv_full, m.ids, q_heads, kv_heads, rows)
            m.attended = mm(wide, select).astype(BF16)
            product = mm_nt(m.attended, o_full).astype(BF16)
            m.sum1 = LineSum(shaped(product), share, HOP_AXIS)
            return (product,)

        return run

    def mixed_back(m):
        def run(dy):
            m.dmixed = row_major(mm(dy.reshape(flat, width), down_full))
            return (m.dmixed,)

        return run

    def norm_two_of(m):
        middle = m.x_here + m.sum1.result()
        root = lax.rsqrt(jnp.mean(middle * middle, axis=-1, keepdims=True) + EPS)
        m.middle, m.root_two = middle, root
        m.gather1 = LineGather((middle * root * gain_two).astype(BF16), HOP_AXIS)

    def feed_forward(m):
        def run(normed_two, sends):
            m.normed_two = normed_two
            (m.mixed, m.dgate, m.dup), others = feed_forward_hidden(
                normed_two, gate_up_full, m.dmixed, sends
            )
            return (m.mixed, m.dgate, m.dup), others

        return run

    def back_of(m):
        def run(dgate, sends):
            (product, out), others = feed_back(
                dgate, m.dup, m.mixed, gate_up_full, down_full, sends
            )
            m.sum3 = LineSum(shaped(product), share, HOP_AXIS)
            m.out_part = shaped(out)
            return (product, out), others

        return run

    def norm_two_back(m):
        middle, dn2 = m.middle, m.sum3.result()
        m.gain_two_grad = jnp.sum(dn2 * middle * m.root_two, axis=(0, 1))
        m.dmiddle = m.dy_here + norm_back(dn2, middle, gain_two)
        m.gather2 = LineGather(m.dmiddle.astype(BF16), HOP_AXIS)

    def attended_back(m):
        def run(dmb, sends):
            m.dmb = dmb
            (m.do,), others = out_back(dmb, o_full, select, sends)
            return (m.do,), others

        return run

    def attend_back(m):
        def run(do_wide, sends):
            (m.dq, dk, dv), others = attend_backward(
                m.q, m.kv_full, do_wide, m.ids, q_heads, kv_heads, rows, sends
            )
            m.dkv = EarlierReturn(jnp.concatenate([dk, dv], axis=2), "context")
            return (m.dq,), others

        return run

    def norm_one_back(m):
        def run(dq, sends):
            dkv = m.dkv.result().reshape(flat, -1)
            (m.dqkv, dn1), others = pack_heads(
                dq, dkv, m.cos, m.sin, attention_full, q_heads, kv_heads, sends
            )
            x = m.x.reshape(flat, width).astype(F32)
            m.gain_one_grad = jnp.sum(dn1.astype(F32) * x * m.root_one, axis=0)
            m.sum4 = LineSum(shaped(dn1), share, HOP_AXIS)
            return (m.dqkv, dn1), others

        return run

    class WeightGrad:
        def __init__(self, lefts, *rights):
            self.lefts, self.rights = lefts, rights

        def __call__(self, sends):
            (self.grad,), others = weight_grad(self.lefts, self.rights, sends)
            return (self.grad,), others

        def scattered(self):
            return lax.psum_scatter(self.grad, WEIGHT_AXES, scatter_dimension=0, tiled=True)

    def gathered(transfer):
        return transfer.result().reshape(flat, width)

    stage([], project(a), [a.root_one])
    stage([a.kv], project(b), [b.root_one])
    stage([b.kv], attend(a), [a.q])
    stage([a.sum1], attend(b), [b.q])
    stage([a.sum1], fused=True)
    stage([a.sum1], mixed_back(a), [a.dy])
    norm_two_of(a)
    stage([a.gather1], mixed_back(b), [b.dy])
    stage([a.gather1, b.sum1], fused=True)
    stage([a.gather1, b.sum1], fused=True)
    stage([b.sum1], fused=True)
    norm_two_of(b)
    stage([b.gather1], feed_forward(a), [gathered(a.gather1)], fused=True)
    stage([b.gather1], back_of(a), [a.dgate], fused=True)
    stage([b.gather1, a.sum3], fused=True)
    stage([a.sum3], feed_forward(b), [gathered(b.gather1)], fused=True)
    dy_all = cotangent.reshape(-1, width)
    down_grad = WeightGrad([dy_all], a.mixed, b.mixed)
    stage([a.sum3], down_grad, fused=True)
    down_grad = down_grad.scattered()
    norm_two_back(a)
    a.sum2 = LineSum(a.out_part, share, HOP_AXIS)
    stage([a.gather2, a.sum2], back_of(b), [b.dgate], fused=True)
    b.sum2 = LineSum(b.out_part, share, HOP_AXIS)
    gate_grad = WeightGrad([a.normed_two, b.normed_two], a.dgate, b.dgate)
    stage([a.gather2, b.sum3], gate_grad, fused=True)
    gate_grad = gate_grad.scattered()
    up_grad = WeightGrad([a.normed_two, b.normed_two], a.dup, b.dup)
    stage([a.gather2, b.sum3], up_grad, fused=True)
    up_grad = up_grad.scattered()
    stage([b.sum3], attended_back(a), [gathered(a.gather2)], fused=True)
    norm_two_back(b)
    stage([b.gather2], attend_back(a), [a.do], fused=True)
    stage([b.gather2, b.sum2, a.dkv], fused=True)
    stage([b.gather2, a.sum2], norm_one_back(a), [a.dq], fused=True)
    stage.wait_for(down_grad)
    stage([a.sum4], attended_back(b), [gathered(b.gather2)], fused=True)
    stage.wait_for(gate_grad)
    stage([a.sum4, a.sum2], attend_back(b), [b.do], fused=True)
    stage.wait_for(up_grad)
    o_grad = WeightGrad([a.dmb, b.dmb], a.attended, b.attended)
    stage([a.sum4, b.dkv], o_grad, fused=True)
    o_grad = o_grad.scattered()
    stage([b.sum2], norm_one_back(b), [b.dq], fused=True)
    gains = jnp.stack([a.gain_one_grad + b.gain_one_grad, a.gain_two_grad + b.gain_two_grad])
    gains = SmallSum(gains, HOP_AXIS)
    attention_grad = WeightGrad([normed_all], a.dqkv, b.dqkv)
    stage([b.sum4, gains], attention_grad, fused=True)
    attention_grad = attention_grad.scattered().astype(F32)
    gains = SmallSum(gains.result(), "context")
    stage([b.sum4, b.sum2, gains], fused=True)
    stage.wait_for(o_grad)
    gains = SmallSum(gains.result(), "fsdp")
    stage([b.sum4, gains], fused=True)
    block = lax.axis_index("fsdp") * ctx_count + ctx
    gains = lax.dynamic_slice_in_dim(gains.result(), block * part, part, 1)
    for m in state:
        m.out_sum = m.sum2.result()
    for m in state:
        middle, out_sum = lax.optimization_barrier((m.middle, m.out_sum))
        m.out = (middle + out_sum.astype(F32)).astype(BF16)
        m.dx = (m.dmiddle + norm_back(m.sum4.result(), m.x_here, gain_one)).astype(BF16)

    return (
        jnp.concatenate([m.out for m in state], axis=0),
        jnp.concatenate([m.dx for m in state], axis=0),
        gains[0],
        attention_grad[:, :q_width],
        attention_grad[:, q_width : q_width + kv_width],
        attention_grad[:, q_width + kv_width : used],
        o_grad.T.astype(F32),
        gains[1],
        gate_grad[:, :hidden].astype(F32),
        up_grad[:, :hidden].astype(F32),
        down_grad[:, :hidden].T.astype(F32),
    )


def solution(mesh):
    HOP_IDS.clear()
    weights = WEIGHT_AXES
    return jax.shard_map(
        on_device,
        mesh=mesh,
        in_specs=(
            P("fsdp", "context", None),
            P(weights),
            P(weights, "tensor"),
            P(weights, "tensor"),
            P(weights, "tensor"),
            P("tensor", weights),
            P(weights),
            P(weights, "tensor"),
            P(weights, "tensor"),
            P("tensor", weights),
            P("fsdp", None),
            P("fsdp", None),
            P("fsdp", None),
            P("fsdp", "context", None),
        ),
        out_specs=(
            P("fsdp", ("context", "tensor"), None),
            P("fsdp", ("context", "tensor"), None),
            P(weights),
            P(weights, "tensor"),
            P(weights, "tensor"),
            P(weights, "tensor"),
            P("tensor", weights),
            P(weights),
            P(weights, "tensor"),
            P(weights, "tensor"),
            P("tensor", weights),
        ),
        check_vma=False,
    )
```

```python
import functools
from types import SimpleNamespace

import jax
import jax.numpy as jnp
import numpy as np
from jax import lax
from jax.experimental import pallas as pl
from jax.experimental.pallas import tpu as pltpu
from jax.experimental.layout import Layout, with_layout_constraint
from jax.sharding import PartitionSpec as P


HEAD = 80
HALF = HEAD // 2
LANES = 128
MICRO = 2
EPS = 1e-05
THETA = 10000.0
NEG = -1000000000.0
TRUNK = 512
WEIGHT_AXES = ("fsdp", "context")
BF16 = jnp.bfloat16
F32 = jnp.float32


def row_major(value):
    return with_layout_constraint(value, Layout(major_to_minor=(0, 1)))


def round_up(value, unit):
    return (value + unit - 1) // unit * unit


def mm(left, right):
    return lax.dot_general(left, right, (((1,), (0,)), ((), ())), preferred_element_type=F32)


def mm_nt(left, right):
    return lax.dot_general(left, right, (((1,), (1,)), ((), ())), preferred_element_type=F32)


def mm_tn(left, right):
    return lax.dot_general(left, right, (((0,), (0,)), ((), ())), preferred_element_type=F32)


def rotated(values, cos_table, sin_table):
    lane = lax.broadcasted_iota(jnp.int32, values.shape, 1)
    swapped = jnp.where(
        lane < HALF, pltpu.roll(values, LANES - HALF, 1), pltpu.roll(values, HALF, 1)
    )
    return values * cos_table + swapped * sin_table


def window_of(head):
    start = head * HEAD
    base = start // LANES * LANES
    return base, start - base


def split_kernel(q_heads, kv_heads, x_ref, cos_ref, sin_ref, q_ref, kv_ref):
    cos_table = cos_ref[...]
    sin_table = sin_ref[...]
    for head in range(q_heads + 2 * kv_heads):
        base, shift = window_of(head)
        window = x_ref[:, base : base + 2 * LANES]
        if shift:
            window = pltpu.roll(window, 2 * LANES - shift, 1)
        values = window[:, :LANES]
        if head < q_heads + kv_heads:
            result = rotated(values, cos_table, sin_table)
        else:
            lane = lax.broadcasted_iota(jnp.int32, values.shape, 1)
            result = jnp.where(lane < HEAD, values, 0.0)
        result = result.astype(BF16)
        if head < q_heads:
            q_ref[:, head * LANES : (head + 1) * LANES] = result
        else:
            at = (head - q_heads) * LANES
            kv_ref[:, at : at + LANES] = result


def split_heads(packed, cos_table, sin_table, q_heads, kv_heads, rows):
    total, width = packed.shape
    q_wide = q_heads * LANES
    kv_wide = 2 * kv_heads * LANES
    return pl.pallas_call(
        functools.partial(split_kernel, q_heads, kv_heads),
        grid=(total // rows,),
        in_specs=[
            pl.BlockSpec((rows, width), lambda b: (b, 0)),
            pl.BlockSpec((rows, LANES), lambda b: (b, 0)),
            pl.BlockSpec((rows, LANES), lambda b: (b, 0)),
        ],
        out_specs=[
            pl.BlockSpec((rows, q_wide), lambda b: (b, 0)),
            pl.BlockSpec((rows, kv_wide), lambda b: (b, 0)),
        ],
        out_shape=[
            jax.ShapeDtypeStruct((total, q_wide), BF16),
            jax.ShapeDtypeStruct((total, kv_wide), BF16),
        ],
        cost_estimate=pl.CostEstimate(
            flops=10 * total * width, bytes_accessed=7 * total * width, transcendentals=0
        ),
        name="split_heads",
    )(packed, cos_table, sin_table)


def fill_bias(seg_q, par_q, pos_q, seg_k, pos_k, bias_ref):
    same = (seg_k == seg_q) | (seg_k == par_q) | (seg_k == 0)
    bias_ref[...] = jnp.where(same & (pos_k <= pos_q), 0.0, NEG)


def probabilities(q_block, keys, bias):
    scores = mm_nt(q_block, keys) * HEAD ** (-0.5) + bias
    top = jnp.max(scores, axis=1, keepdims=True)
    raised = jnp.exp(scores - top)
    return raised * (1.0 / jnp.sum(raised, axis=1, keepdims=True))


def forward_kernel(
    rows, tree_len, block,
    ctx_ref, q_ref, k_ref, v_ref, seg_q, par_q, pos_q, seg_k, pos_k, out_ref, bias_ref,
):
    @pl.when(pl.program_id(1) == 0)
    def _():
        fill_bias(seg_q[0], par_q[0], pos_q[0], seg_k[0], pos_k[0], bias_ref)

    in_trunk = (ctx_ref[0] + 1) * rows <= TRUNK

    def run(keys):
        @pl.loop(0, rows // block)
        def _(step):
            at = pl.ds(pl.multiple_of(step * block, block), block)
            probs = probabilities(q_ref[at, :], k_ref[0, :keys, :], bias_ref[at, :keys])
            out_ref[at, :] = mm(probs.astype(BF16), v_ref[0, :keys, :]).astype(BF16)

    pl.when(in_trunk)(lambda: run(min(TRUNK, tree_len)))
    pl.when(jnp.logical_not(in_trunk))(lambda: run(tree_len))


def backward_kernel(
    rows, tree_len, block, group,
    q_ref, k_ref, v_ref, do_ref, seg_q, par_q, pos_q, seg_k, pos_k,
    dq_ref, dk_ref, dv_ref, bias_ref,
):
    head = pl.program_id(1)

    @pl.when(head == 0)
    def _():
        fill_bias(seg_q[0], par_q[0], pos_q[0], seg_k[0], pos_k[0], bias_ref)

    @pl.when(lax.rem(head, group) == 0)
    def _():
        dk_ref[...] = jnp.zeros_like(dk_ref)
        dv_ref[...] = jnp.zeros_like(dv_ref)

    in_trunk = (lax.axis_index("context") + 1) * rows <= TRUNK
    scale = HEAD ** (-0.5)

    def run(keys):
        @pl.loop(0, rows // block)
        def _(step):
            at = pl.ds(pl.multiple_of(step * block, block), block)
            q_block = q_ref[at, :]
            do_block = do_ref[at, :]
            k_all = k_ref[0, :keys, :]
            probs = probabilities(q_block, k_all, bias_ref[at, :keys])
            dprobs = mm_nt(do_block, v_ref[0, :keys, :])
            delta = jnp.sum(probs * dprobs, axis=1, keepdims=True)
            dscores = (probs * (dprobs - delta)).astype(BF16)
            dq_ref[at, :] = (mm(dscores, k_all) * scale).astype(BF16)
            dk_ref[0, :keys, :] += mm_tn(dscores, q_block) * scale
            dv_ref[0, :keys, :] += mm_tn(probs.astype(BF16), do_block)

    pl.when(in_trunk)(lambda: run(min(TRUNK, tree_len)))
    pl.when(jnp.logical_not(in_trunk))(lambda: run(tree_len))


def attention_specs(rows, tree_len, group, kv_heads):
    def column(b, h, *c):
        return (b, h)

    def whole(b, h, *c):
        return (b, 0, 0)

    return [
        pl.BlockSpec((rows, LANES), column),
        pl.BlockSpec((1, tree_len, LANES), lambda b, h, *c: (b, 0, h // group)),
        pl.BlockSpec((1, tree_len, LANES), lambda b, h, *c: (b, 0, kv_heads + h // group)),
    ], [
        pl.BlockSpec((1, rows, 1), whole),
        pl.BlockSpec((1, rows, 1), whole),
        pl.BlockSpec((1, rows, 1), whole),
        pl.BlockSpec((1, 1, tree_len), whole),
        pl.BlockSpec((1, 1, tree_len), whole),
    ]


def attend_forward(ctx, q_wide, kv_full, ids, q_heads, kv_heads, rows):
    trees, tree_len, _ = kv_full.shape
    group = q_heads // kv_heads
    first, last = attention_specs(rows, tree_len, group, kv_heads)
    block = min(rows, 256)
    work = trees * q_heads * rows * tree_len
    return pl.pallas_call(
        functools.partial(forward_kernel, rows, tree_len, block),
        grid_spec=pltpu.PrefetchScalarGridSpec(
            num_scalar_prefetch=1,
            grid=(trees, q_heads),
            in_specs=first + last,
            out_specs=pl.BlockSpec((rows, LANES), lambda b, h, c: (b, h)),
            scratch_shapes=[pltpu.VMEM((rows, tree_len), F32)],
        ),
        out_shape=jax.ShapeDtypeStruct(q_wide.shape, BF16),
        cost_estimate=pl.CostEstimate(
            flops=4 * LANES * work, bytes_accessed=8 * q_wide.size, transcendentals=work
        ),
        name="attend_forward",
    )(ctx, q_wide, kv_full, kv_full, *ids)


HOP_AXIS = "tensor"


def with_hops(kernel, counts, sides, *refs):
    own_in, own_out, own_scratch = counts
    sends = len(sides)
    ends_at = []
    for size in (own_in, sends, own_out, sends, own_scratch):
        ends_at.append((ends_at[-1] if ends_at else 0) + size)
    ins, sent, outs, received, scratch = (
        refs[low:high] for low, high in zip([0, *ends_at], ends_at)
    )
    send_sem, recv_sem = refs[ends_at[-1] :]
    here = lax.axis_index(HOP_AXIS)
    count = lax.axis_size(HOP_AXIS)
    has_next, has_last = here < count - 1, here > 0

    def copy(number):
        other = here + 1 - 2 * sides[number]
        return pltpu.make_async_remote_copy(
            src_ref=sent[number],
            dst_ref=received[number],
            send_sem=send_sem.at[number],
            recv_sem=recv_sem.at[number],
            device_id={HOP_AXIS: other},
            device_id_type=pl.DeviceIdType.MESH,
        )

    first, last = None, None
    if own_in:
        first, last = jnp.bool_(True), jnp.bool_(True)
        for axis in range(GRID_RANK[kernel]):
            first &= pl.program_id(axis) == 0
            last &= pl.program_id(axis) == pl.num_programs(axis) - 1

    def start():
        barrier = pltpu.get_barrier_semaphore()
        for there, step in ((has_next, 1), (has_last, -1)):

            @pl.when(there)
            def _():
                pl.semaphore_signal(
                    barrier,
                    inc=1,
                    device_id={HOP_AXIS: here + step},
                    device_id_type=pl.DeviceIdType.MESH,
                )

        pl.semaphore_wait(barrier, has_next.astype(jnp.int32) + has_last.astype(jnp.int32))
        for number, side in enumerate(sides):
            pl.when((has_next, has_last)[side])(lambda number=number: copy(number).start())

    def finish():
        for number, side in enumerate(sides):
            pl.when((has_next, has_last)[side])(lambda number=number: copy(number).wait_send())
            pl.when((has_last, has_next)[side])(lambda number=number: copy(number).wait_recv())

    if own_in:
        pl.when(first)(start)
        kernel(*ins, *outs, *scratch)
        pl.when(last)(finish)
    else:
        start()
        finish()


GRID_RANK = {}
HOP_IDS = {}


def hop_call(kernel, sends, *args, grid=(), in_specs=(), out_specs=(), out_shape=(),
             scratch_shapes=(), name="hop", cost_estimate=None):
    sides = tuple(side for _, side in sends)
    values = [value for value, _ in sends]
    anywhere = pl.BlockSpec(memory_space=pl.ANY)
    if kernel is not None:
        GRID_RANK[kernel] = len(grid)
    counts = (len(args), len(out_shape), len(scratch_shapes))
    key = (name, sides, tuple(v.shape for v in (*values, *args)))
    results = pl.pallas_call(
        functools.partial(with_hops, kernel, counts, sides),
        grid=grid,
        in_specs=[*in_specs, *[anywhere] * len(values)],
        out_specs=[*out_specs, *[anywhere] * len(values)],
        out_shape=[*out_shape, *[jax.ShapeDtypeStruct(v.shape, v.dtype) for v in values]],
        scratch_shapes=[
            *scratch_shapes,
            pltpu.SemaphoreType.DMA((len(values),)),
            pltpu.SemaphoreType.DMA((len(values),)),
        ],
        compiler_params=pltpu.CompilerParams(
            collective_id=HOP_IDS.setdefault(key, len(HOP_IDS)), has_side_effects=True
        ),
        cost_estimate=cost_estimate,
    )(*args, *values)
    return results[: len(out_shape)], results[len(out_shape) :]


def attend_backward(q_wide, kv_full, do_wide, ids, q_heads, kv_heads, rows, sends):
    trees, tree_len, _ = kv_full.shape
    group = q_heads // kv_heads
    first, last = attention_specs(rows, tree_len, group, kv_heads)
    block = min(rows, 256)
    work = trees * q_heads * rows * tree_len
    grad_spec = pl.BlockSpec((1, tree_len, LANES), lambda b, h: (b, 0, h // group))
    grad_shape = jax.ShapeDtypeStruct((trees, tree_len, kv_heads * LANES), F32)
    return hop_call(
        functools.partial(backward_kernel, rows, tree_len, block, group),
        sends,
        *(q_wide, kv_full, kv_full, do_wide, *ids),
        grid=(trees, q_heads),
        in_specs=first + [first[0]] + last,
        out_specs=[first[0], grad_spec, grad_spec],
        out_shape=[jax.ShapeDtypeStruct(q_wide.shape, BF16), grad_shape, grad_shape],
        scratch_shapes=[pltpu.VMEM((rows, tree_len), F32)],
        cost_estimate=pl.CostEstimate(
            flops=10 * LANES * work, bytes_accessed=12 * q_wide.size, transcendentals=work
        ),
        name="attend_backward",
    )


def pack_kernel(
    q_heads, kv_heads, dq_ref, dkv_ref, cos_ref, sin_ref, weight, packed_ref, product_ref, sum_ref
):
    @pl.when(pl.program_id(0) == 0)
    def _():
        cos_table = cos_ref[...]
        sin_table = -sin_ref[...]
        sum_ref[...] = jnp.zeros_like(sum_ref)
        for head in range(q_heads + 2 * kv_heads):
            base, shift = window_of(head)
            if head < q_heads:
                values = dq_ref[:, head * LANES : (head + 1) * LANES].astype(F32)
            else:
                at = (head - q_heads) * LANES
                values = dkv_ref[:, at : at + LANES].astype(BF16).astype(F32)
            if head < q_heads + kv_heads:
                values = rotated(values, cos_table, sin_table)
            wide = jnp.concatenate([values, jnp.zeros_like(values)], axis=1)
            if shift:
                wide = pltpu.roll(wide, shift, 1)
            sum_ref[:, base : base + 2 * LANES] += wide
        packed_ref[...] = sum_ref[...].astype(BF16)

    product_ref[...] = mm_nt(packed_ref[...], weight[...]).astype(BF16)


def pack_heads(dq_wide, dkv, cos_table, sin_table, weight, q_heads, kv_heads, sends):
    rows = dq_wide.shape[0]
    width, packed = weight.shape
    tile = width // 5

    def whole(values):
        return pl.BlockSpec(values.shape, lambda i: (0, 0))

    return hop_call(
        functools.partial(pack_kernel, q_heads, kv_heads),
        sends,
        *(dq_wide, dkv, cos_table, sin_table, weight),
        grid=(width // tile,),
        in_specs=[
            whole(dq_wide), whole(dkv), whole(cos_table), whole(sin_table),
            pl.BlockSpec((tile, packed), lambda i: (i, 0)),
        ],
        out_specs=[
            pl.BlockSpec((rows, packed), lambda i: (0, 0)),
            pl.BlockSpec((rows, tile), lambda i: (0, i)),
        ],
        out_shape=[
            jax.ShapeDtypeStruct((rows, packed), BF16),
            jax.ShapeDtypeStruct((rows, width), BF16),
        ],
        scratch_shapes=[pltpu.VMEM((rows, packed), F32)],
        cost_estimate=pl.CostEstimate(
            flops=2 * rows * width * packed,
            bytes_accessed=2 * width * packed + 8 * rows * packed + 2 * rows * width,
            transcendentals=0,
        ),
        name="pack_heads",
    )


def weight_grad_kernel(first_left, last_left, first_right, last_right, grad_ref):
    grad = mm_tn(first_left[...], first_right[...]) + mm_tn(last_left[...], last_right[...])
    grad_ref[...] = grad.astype(BF16)


def weight_grad(lefts, rights, sends):
    rows, columns = rights[0].shape
    if len(lefts) == 1:
        lefts, at = lefts * 2, (0, 1)
    else:
        at = (0, 0)
    width = lefts[0].shape[1]
    tile = width // 5
    right = pl.BlockSpec((rows, columns), lambda i: (0, 0))
    return hop_call(
        weight_grad_kernel,
        sends,
        *(*lefts, *rights),
        grid=(width // tile,),
        in_specs=[
            pl.BlockSpec((rows, tile), lambda i: (at[0], i)),
            pl.BlockSpec((rows, tile), lambda i: (at[1], i)),
            right,
            right,
        ],
        out_specs=[pl.BlockSpec((tile, columns), lambda i: (i, 0))],
        out_shape=[jax.ShapeDtypeStruct((width, columns), BF16)],
        cost_estimate=pl.CostEstimate(
            flops=4 * rows * width * columns,
            bytes_accessed=4 * rows * (width + columns) + 2 * width * columns,
            transcendentals=0,
        ),
        name="weight_grad",
    )


def feed_forward_kernel(normed, gate_w, up_w, dmixed, mixed_ref, dgate_ref, dup_ref):
    gate = mm(normed[...], gate_w[...])
    up = mm(normed[...], up_w[...])
    sigmoid = 1.0 / (1.0 + jnp.exp(-gate))
    silu = gate * sigmoid
    slope = sigmoid * (1.0 + gate * (1.0 - sigmoid))
    mixed_ref[...] = (silu * up).astype(BF16)
    dgate_ref[...] = (dmixed[...] * up * slope).astype(BF16)
    dup_ref[...] = (dmixed[...] * silu).astype(BF16)


def feed_forward_hidden(normed, gate_up_w, dmixed, sends):
    rows, width = normed.shape
    hidden = dmixed.shape[1]
    tile = 2 * LANES
    count = hidden // tile
    result = pl.BlockSpec((rows, tile), lambda i: (0, i))
    return hop_call(
        feed_forward_kernel,
        sends,
        *(normed, gate_up_w, gate_up_w, dmixed),
        grid=(count,),
        in_specs=[
            pl.BlockSpec((rows, width), lambda i: (0, 0)),
            pl.BlockSpec((width, tile), lambda i: (0, i)),
            pl.BlockSpec((width, tile), lambda i: (0, i + count)),
            result,
        ],
        out_specs=[result] * 3,
        out_shape=[jax.ShapeDtypeStruct((rows, hidden), BF16)] * 3,
        cost_estimate=pl.CostEstimate(
            flops=4 * rows * hidden * width,
            bytes_accessed=4 * hidden * width + 2 * rows * width + 10 * rows * hidden,
            transcendentals=rows * hidden,
        ),
        name="feed_forward",
    )


def feed_back_kernel(dgate, dup, mixed, gate_w, up_w, down_w, dn2_ref, out_ref):
    dn2 = mm_nt(dgate[...], gate_w[...]) + mm_nt(dup[...], up_w[...])
    dn2_ref[...] = dn2.astype(BF16)
    out_ref[...] = mm_nt(mixed[...], down_w[...]).astype(BF16)


def feed_back(dgate, dup, mixed, gate_up_w, down_w, sends):
    rows, hidden = mixed.shape
    width = down_w.shape[0]
    tile = width // 5
    left = pl.BlockSpec((rows, hidden), lambda i: (0, 0))
    right = pl.BlockSpec((tile, hidden), lambda i: (i, 0))
    result = pl.BlockSpec((rows, tile), lambda i: (0, i))
    return hop_call(
        feed_back_kernel,
        sends,
        *(dgate, dup, mixed, gate_up_w, gate_up_w, down_w),
        grid=(width // tile,),
        in_specs=[
            *[left] * 3,
            right,
            pl.BlockSpec((tile, hidden), lambda i: (i, 1)),
            right,
        ],
        out_specs=[result] * 2,
        out_shape=[jax.ShapeDtypeStruct((rows, width), BF16)] * 2,
        cost_estimate=pl.CostEstimate(
            flops=6 * rows * hidden * width,
            bytes_accessed=6 * hidden * (rows + width) + 4 * rows * width,
            transcendentals=0,
        ),
        name="feed_back",
    )


def out_back_kernel(grad, weight, select, result_ref):
    narrow = mm(grad[...], weight[...]).astype(BF16)
    result_ref[...] = mm_nt(narrow, select[...]).astype(BF16)


def out_back(grad, weight, select, sends):
    rows, wide = grad.shape[0], select.shape[0]

    def whole(values):
        return pl.BlockSpec(values.shape, lambda i: (0, 0))

    return hop_call(
        out_back_kernel,
        sends,
        *(grad, weight, select),
        grid=(1,),
        in_specs=[whole(grad), whole(weight), whole(select)],
        out_specs=[pl.BlockSpec((rows, wide), lambda i: (0, 0))],
        out_shape=[jax.ShapeDtypeStruct((rows, wide), BF16)],
        cost_estimate=pl.CostEstimate(
            flops=2 * rows * weight.size + 2 * rows * select.size,
            bytes_accessed=2 * (grad.size + weight.size + select.size + rows * wide),
            transcendentals=0,
        ),
        name="out_back",
    )


def piece(values, index, size):
    return lax.dynamic_slice_in_dim(values, index * size, size, 1)


class LineSum:
    def __init__(self, values, size, axis):
        self.axis = axis
        self.count = lax.axis_size(axis)
        self.pieces = [values[:, i * size : (i + 1) * size] for i in range(self.count)]
        self.step = 0
        self.got = None
        here = lax.axis_index(axis)
        self.valid = (here > 0, here < self.count - 1)

    def sends(self):
        self.step += 1
        step, count = self.step, self.count
        rights = [(i, i + 1) for i in range(step)]
        lefts = [(count - 1 - i, count - 2 - i) for i in range(step)]
        found = []
        for side, slot, pairs in ((0, step, rights), (1, count - step, lefts)):
            value = self.pieces[slot]
            if self.got is not None:
                value = (value.astype(F32) + self.arrived(side)).astype(BF16)
            found.append((value, self.axis, pairs, side))
        return found

    def arrived(self, side):
        return jnp.where(self.valid[side], self.got[side].astype(F32), 0.0)

    def loose(self):
        return self.step == 1 and self.count > 2

    def receive(self, results):
        self.got = results

    def result(self):
        assert self.step == self.count - 1
        total = self.pieces[0].astype(F32)
        for side in (0, 1) if self.got else ():
            total = total + self.arrived(side)
        return total


class LineGather:
    def __init__(self, own, axis):
        self.own, self.axis = own, axis
        self.count = lax.axis_size(axis)
        self.lefts, self.rights = [own], [own]

    def sends(self):
        step, count = len(self.lefts), self.count
        return [
            (self.lefts[-1], self.axis, [(i, i + 1) for i in range(step - 1, count - 1)], 0),
            (self.rights[-1], self.axis, [(i, i - 1) for i in range(count - step, 0, -1)], 1),
        ]

    def loose(self):
        return len(self.lefts) == self.count - 1 and self.count > 2

    def receive(self, results):
        self.lefts.append(results[0])
        self.rights.append(results[1])

    def result(self):
        count = self.count
        here = lax.axis_index(self.axis)
        assert len(self.lefts) == count
        others = [
            jnp.where(here >= step, self.lefts[step], self.rights[count - step])
            for step in range(1, count)
        ]
        return jnp.concatenate([self.own, *others], axis=1)


class EarlierGather:
    def __init__(self, own, axis):
        self.own, self.axis = own, axis
        self.count = lax.axis_size(axis)

    def sends(self):
        count = self.count
        return [
            (self.own, self.axis, [(i, i + step) for i in range(count - step)], None)
            for step in range(1, count)
        ]

    def receive(self, results):
        self.others = results

    def result(self):
        count, own = self.count, self.own
        here = lax.axis_index(self.axis)
        trees, rows, width = own.shape
        result = jnp.zeros((trees, count * rows, width), own.dtype)
        result = lax.dynamic_update_slice_in_dim(result, own, here * rows, 1)
        for step, other in enumerate(self.others, 1):
            slot = lax.rem(here - step + count, count)
            result = lax.dynamic_update_slice_in_dim(result, other, slot * rows, 1)
        return result


class EarlierReturn:
    def __init__(self, full, axis):
        self.full, self.axis = full, axis
        self.count = lax.axis_size(axis)
        self.rows = full.shape[1] // self.count

    def sends(self):
        count = self.count
        here = lax.axis_index(self.axis)
        found = []
        for step in range(1, count):
            slot = lax.rem(here - step + count, count)
            value = piece(self.full, slot, self.rows).astype(BF16)
            found.append((value, self.axis, [(i + step, i) for i in range(count - step)], None))
        return found

    def receive(self, results):
        self.others = results

    def result(self):
        total = piece(self.full, lax.axis_index(self.axis), self.rows)
        for other in self.others:
            total = total + other.astype(F32)
        return total


def ends(pairs, which):
    return {pair[which] for pair in pairs}


def disjoint(left, right):
    return not any(ends(left, which) & ends(right, which) for which in (0, 1))


def joined(sends, loose):
    groups = []
    for number, (value, axis, pairs, side) in enumerate(sends):
        for group in groups:
            if side is None or group.axis != axis or not disjoint(pairs, group.pairs):
                continue
            if group.side != side and not loose:
                continue
            here = lax.axis_index(axis)
            mine = functools.reduce(jnp.logical_or, [here == i for i in sorted(ends(pairs, 0))])
            group.value = jnp.where(mine, value, group.value)
            group.pairs = group.pairs + pairs
            group.members.append(number)
            break
        else:
            groups.append(
                SimpleNamespace(value=value, axis=axis, pairs=pairs, side=side, members=[number])
            )
    return groups


class Stages:
    def __init__(self):
        self.token = ()
        self.number = 0

    def wait_for(self, *values):
        self.token += values

    def __call__(self, transfers, compute=None, inputs=(), fused=False):
        self.number += 1
        kept = []
        for t in transfers:
            if t.count > 1:
                kept.append(t)
            else:
                t.receive([])
        transfers = kept
        sends = [t.sends() for t in transfers]
        lines = [t for t in transfers if hasattr(t, "loose")]
        loose = len(lines) == 1 and lines[0].loose() and not fused
        groups = joined([send for of_one in sends for send in of_one], loose)
        values = [group.value for group in groups]
        tied = lax.optimization_barrier((*values, *inputs, *self.token))
        results = {}
        token = []
        by_kernel = []
        for value, group in zip(tied, groups):
            if fused and group.side is not None:
                by_kernel.append((value, group))
                continue
            other = lax.ppermute(value, group.axis, group.pairs)
            token.append(other)
            results.update({number: other for number in group.members})
        given = tied[len(groups) : len(groups) + len(inputs)]
        if by_kernel:
            line_sends = [(value, group.side) for value, group in by_kernel]
            if compute is None:
                outs, others = hop_call(None, line_sends)
            else:
                outs, others = compute(*given, line_sends)
            for other, (_, group) in zip(others, by_kernel):
                token.append(other)
                results.update({number: other for number in group.members})
        else:
            outs = compute(*given) if compute else ()
        at = 0
        for transfer, of_one in zip(transfers, sends):
            transfer.receive([results[at + i] for i in range(len(of_one))])
            at += len(of_one)
        self.token = (*token, *outs)
        return outs


def turned(values, dim, axis):
    count = lax.axis_size(axis)
    here = lax.axis_index(axis)
    size = values.shape[dim] // count
    return jnp.concatenate(
        [
            lax.dynamic_slice_in_dim(
                values, lax.rem(here - i + count, count) * size, size, dim
            )
            for i in range(count)
        ],
        axis=dim,
    )


class SmallSum:
    def __init__(self, values, axis):
        self.values, self.axis = values, axis
        self.count = lax.axis_size(axis)

    def sends(self):
        count = self.count
        return [
            (self.values, self.axis, [(i, (i + step) % count) for i in range(count)], None)
            for step in range(1, count)
        ]

    def receive(self, results):
        self.others = results

    def result(self):
        return sum(self.others, self.values)


def norm_back(grad, values, gain):
    root = lax.rsqrt(jnp.mean(values * values, axis=-1, keepdims=True) + EPS)
    weighted = grad * gain
    mean = jnp.mean(weighted * values, axis=-1, keepdims=True)
    return root * weighted - values * (root * root * root) * mean


def on_device(
    tokens, norm_one, q_weight, k_weight, v_weight, o_weight, norm_two,
    gate_weight, up_weight, down_weight, segment_ids, parent_ids, path_pos, cotangent,
):
    ctx = lax.axis_index("context")
    ctx_count = lax.axis_size("context")
    ten_count = lax.axis_size(HOP_AXIS)
    tree_count, rows, width = tokens.shape
    share = rows // ten_count
    trees = tree_count // MICRO
    flat = trees * rows
    part, q_width = q_weight.shape
    kv_width = k_weight.shape[1]
    q_heads = q_width // HEAD
    kv_heads = kv_width // HEAD
    used = q_width + 2 * kv_width
    packed_width = round_up(used + 2, LANES)

    attention_block = jnp.concatenate(
        [
            q_weight, k_weight, v_weight, norm_one[:, None], norm_two[:, None],
            jnp.zeros((part, packed_width - used - 2), BF16),
        ],
        axis=1,
    )
    attention_full = lax.all_gather(attention_block, WEIGHT_AXES, axis=0, tiled=True)
    o_full = lax.all_gather(o_weight.T, WEIGHT_AXES, axis=0, tiled=True)
    hidden = gate_weight.shape[1]
    wide = round_up(hidden, LANES)

    def widened(values):
        return jnp.pad(values, ((0, 0), (0, wide - hidden)))

    down_full = lax.all_gather(widened(down_weight.T), WEIGHT_AXES, axis=0, tiled=True)
    gate_up_block = jnp.concatenate([widened(gate_weight), widened(up_weight)], axis=1)
    gate_up_full = lax.all_gather(gate_up_block, WEIGHT_AXES, axis=0, tiled=True)
    gain_one = attention_full[:, used].astype(F32)
    gain_two = attention_full[:, used + 1].astype(F32)

    lane = np.arange(q_heads * LANES)
    column = np.arange(q_width)
    select = jnp.asarray(
        (lane[:, None] // LANES == column[None, :] // HEAD)
        & (lane[:, None] % LANES == column[None, :] % HEAD),
        BF16,
    )
    frequency = THETA ** (-(jnp.arange(HALF, dtype=F32) * 2.0 / HEAD))
    pad = jnp.zeros((flat, LANES - HEAD), F32)
    ctx_ref = jnp.reshape(ctx, (1,)).astype(jnp.int32)

    tokens = turned(tokens, 1, HOP_AXIS)
    cotangent = turned(cotangent, 1, HOP_AXIS)
    segment_ids, parent_ids, path_pos = [
        turned(ids.reshape(-1, ctx_count, rows), 2, HOP_AXIS).reshape(ids.shape)
        for ids in (segment_ids, parent_ids, path_pos)
    ]
    state = []
    for micro in range(MICRO):
        pick = slice(micro * trees, (micro + 1) * trees)
        m = SimpleNamespace()
        state.append(m)
        m.number = micro
        m.x = tokens[pick]
        m.dy = cotangent[pick]
        seg, par, pos = segment_ids[pick], parent_ids[pick], path_pos[pick]

        def here(ids):
            return lax.dynamic_slice_in_dim(ids, ctx * rows, rows, 1)

        m.ids = (
            here(seg)[:, :, None], here(par)[:, :, None], here(pos)[:, :, None],
            seg[:, None, :], pos[:, None, :],
        )
        angles = here(pos).reshape(flat).astype(F32)[:, None] * frequency[None, :]
        cosine, sine = jnp.cos(angles), jnp.sin(angles)
        m.cos = jnp.concatenate([cosine, cosine, pad], axis=1)
        m.sin = jnp.concatenate([-sine, sine, pad], axis=1)
        x = m.x.reshape(flat, width).astype(F32)
        m.root_one = lax.rsqrt(jnp.mean(x * x, axis=-1, keepdims=True) + EPS)
        m.x_here = m.x[:, :share].astype(F32)
        m.dy_here = m.dy[:, :share].astype(F32)

    def shaped(product):
        return product.reshape(trees, rows, width)

    x_all = tokens.reshape(-1, width).astype(F32)
    root_all = jnp.concatenate([m.root_one for m in state], axis=0)
    normed_all = (x_all * root_all * gain_one).astype(BF16)
    stage = Stages()
    a, b = state

    def project(m):
        def run(root):
            at = m.number * flat
            packed = mm(normed_all[at : at + flat], attention_full)
            m.q, kv = split_heads(packed, m.cos, m.sin, q_heads, kv_heads, rows)
            m.kv = EarlierGather(kv.reshape(trees, rows, -1), "context")
            return (m.q,)

        return run

    def attend(m):
        def run(q):
            m.kv_full = m.kv.result()
            wide = attend_forward(ctx_ref, q, m.kv_full, m.ids, q_heads, kv_heads, rows)
            m.attended = mm(wide, select).astype(BF16)
            product = mm_nt(m.attended, o_full).astype(BF16)
            m.sum1 = LineSum(shaped(product), share, HOP_AXIS)
            return (product,)

        return run

    def mixed_back(m):
        def run(dy):
            m.dmixed = row_major(mm(dy.reshape(flat, width), down_full))
            return (m.dmixed,)

        return run

    def norm_two_of(m):
        middle = m.x_here + m.sum1.result()
        root = lax.rsqrt(jnp.mean(middle * middle, axis=-1, keepdims=True) + EPS)
        m.middle, m.root_two = middle, root
        m.gather1 = LineGather((middle * root * gain_two).astype(BF16), HOP_AXIS)

    def feed_forward(m):
        def run(normed_two, sends):
            m.normed_two = normed_two
            (m.mixed, m.dgate, m.dup), others = feed_forward_hidden(
                normed_two, gate_up_full, m.dmixed, sends
            )
            return (m.mixed, m.dgate, m.dup), others

        return run

    def back_of(m):
        def run(dgate, sends):
            (product, out), others = feed_back(
                dgate, m.dup, m.mixed, gate_up_full, down_full, sends
            )
            m.sum3 = LineSum(shaped(product), share, HOP_AXIS)
            m.out_part = shaped(out)
            return (product, out), others

        return run

    def norm_two_back(m):
        middle, dn2 = m.middle, m.sum3.result()
        m.gain_two_grad = jnp.sum(dn2 * middle * m.root_two, axis=(0, 1))
        m.dmiddle = m.dy_here + norm_back(dn2, middle, gain_two)
        m.gather2 = LineGather(m.dmiddle.astype(BF16), HOP_AXIS)

    def attended_back(m):
        def run(dmb, sends):
            m.dmb = dmb
            (m.do,), others = out_back(dmb, o_full, select, sends)
            return (m.do,), others

        return run

    def attend_back(m):
        def run(do_wide, sends):
            (m.dq, dk, dv), others = attend_backward(
                m.q, m.kv_full, do_wide, m.ids, q_heads, kv_heads, rows, sends
            )
            m.dkv = EarlierReturn(jnp.concatenate([dk, dv], axis=2), "context")
            return (m.dq,), others

        return run

    def norm_one_back(m):
        def run(dq, sends):
            dkv = m.dkv.result().reshape(flat, -1)
            (m.dqkv, dn1), others = pack_heads(
                dq, dkv, m.cos, m.sin, attention_full, q_heads, kv_heads, sends
            )
            x = m.x.reshape(flat, width).astype(F32)
            m.gain_one_grad = jnp.sum(dn1.astype(F32) * x * m.root_one, axis=0)
            m.sum4 = LineSum(shaped(dn1), share, HOP_AXIS)
            return (m.dqkv, dn1), others

        return run

    class WeightGrad:
        def __init__(self, lefts, *rights):
            self.lefts, self.rights = lefts, rights

        def __call__(self, sends):
            (self.grad,), others = weight_grad(self.lefts, self.rights, sends)
            return (self.grad,), others

        def scattered(self):
            return lax.psum_scatter(self.grad, WEIGHT_AXES, scatter_dimension=0, tiled=True)

    def gathered(transfer):
        return transfer.result().reshape(flat, width)

    stage([], project(a), [a.root_one])
    stage([a.kv], project(b), [b.root_one])
    stage([b.kv], attend(a), [a.q])
    stage([a.sum1], attend(b), [b.q])
    stage([a.sum1], fused=True)
    stage([a.sum1], mixed_back(a), [a.dy])
    norm_two_of(a)
    stage([a.gather1], mixed_back(b), [b.dy])
    stage([a.gather1, b.sum1], fused=True)
    stage([a.gather1, b.sum1], fused=True)
    stage([b.sum1], fused=True)
    norm_two_of(b)
    stage([b.gather1], feed_forward(a), [gathered(a.gather1)], fused=True)
    stage([b.gather1], back_of(a), [a.dgate], fused=True)
    stage([b.gather1, a.sum3], fused=True)
    stage([a.sum3], feed_forward(b), [gathered(b.gather1)], fused=True)
    dy_all = cotangent.reshape(-1, width)
    down_grad = WeightGrad([dy_all], a.mixed, b.mixed)
    stage([a.sum3], down_grad, fused=True)
    down_grad = down_grad.scattered()
    norm_two_back(a)
    a.sum2 = LineSum(a.out_part, share, HOP_AXIS)
    stage([a.gather2, a.sum2], back_of(b), [b.dgate], fused=True)
    b.sum2 = LineSum(b.out_part, share, HOP_AXIS)
    gate_grad = WeightGrad([a.normed_two, b.normed_two], a.dgate, b.dgate)
    stage([a.gather2, b.sum3], gate_grad, fused=True)
    gate_grad = gate_grad.scattered()
    up_grad = WeightGrad([a.normed_two, b.normed_two], a.dup, b.dup)
    stage([a.gather2, b.sum3], up_grad, fused=True)
    up_grad = up_grad.scattered()
    stage([b.sum3], attended_back(a), [gathered(a.gather2)], fused=True)
    norm_two_back(b)
    stage([b.gather2, a.sum2], attend_back(a), [a.do], fused=True)
    stage([b.gather2, b.sum2, a.dkv], fused=True)
    stage([b.gather2, b.sum2], norm_one_back(a), [a.dq], fused=True)
    stage.wait_for(down_grad)
    stage([a.sum4], attended_back(b), [gathered(b.gather2)], fused=True)
    stage.wait_for(gate_grad)
    stage([a.sum4, a.sum2], attend_back(b), [b.do], fused=True)
    stage.wait_for(up_grad)
    o_grad = WeightGrad([a.dmb, b.dmb], a.attended, b.attended)
    stage([a.sum4, b.dkv], o_grad, fused=True)
    o_grad = o_grad.scattered()
    stage([b.sum2], norm_one_back(b), [b.dq], fused=True)
    gains = jnp.stack([a.gain_one_grad + b.gain_one_grad, a.gain_two_grad + b.gain_two_grad])
    gains = SmallSum(gains, HOP_AXIS)
    attention_grad = WeightGrad([normed_all], a.dqkv, b.dqkv)
    stage([b.sum4, gains], attention_grad, fused=True)
    attention_grad = attention_grad.scattered().astype(F32)
    gains = SmallSum(gains.result(), "context")
    stage([b.sum4, gains], fused=True)
    stage.wait_for(o_grad)
    gains = SmallSum(gains.result(), "fsdp")
    stage([b.sum4, gains], fused=True)
    block = lax.axis_index("fsdp") * ctx_count + ctx
    gains = lax.dynamic_slice_in_dim(gains.result(), block * part, part, 1)
    for m in state:
        m.out_sum = m.sum2.result()
    for m in state:
        middle, out_sum = lax.optimization_barrier((m.middle, m.out_sum))
        m.out = (middle + out_sum.astype(F32)).astype(BF16)
        m.dx = (m.dmiddle + norm_back(m.sum4.result(), m.x_here, gain_one)).astype(BF16)

    return (
        jnp.concatenate([m.out for m in state], axis=0),
        jnp.concatenate([m.dx for m in state], axis=0),
        gains[0],
        attention_grad[:, :q_width],
        attention_grad[:, q_width : q_width + kv_width],
        attention_grad[:, q_width + kv_width : used],
        o_grad.T.astype(F32),
        gains[1],
        gate_grad[:, :hidden].astype(F32),
        up_grad[:, :hidden].astype(F32),
        down_grad[:, :hidden].T.astype(F32),
    )


def solution(mesh):
    HOP_IDS.clear()
    weights = WEIGHT_AXES
    return jax.shard_map(
        on_device,
        mesh=mesh,
        in_specs=(
            P("fsdp", "context", None),
            P(weights),
            P(weights, "tensor"),
            P(weights, "tensor"),
            P(weights, "tensor"),
            P("tensor", weights),
            P(weights),
            P(weights, "tensor"),
            P(weights, "tensor"),
            P("tensor", weights),
            P("fsdp", None),
            P("fsdp", None),
            P("fsdp", None),
            P("fsdp", "context", None),
        ),
        out_specs=(
            P("fsdp", ("context", "tensor"), None),
            P("fsdp", ("context", "tensor"), None),
            P(weights),
            P(weights, "tensor"),
            P(weights, "tensor"),
            P(weights, "tensor"),
            P("tensor", weights),
            P(weights),
            P(weights, "tensor"),
            P(weights, "tensor"),
            P("tensor", weights),
        ),
        check_vma=False,
    )
```
